256 devices in a mesh: line: 16 (over y, x), bus: 16 (over z, core).
Axes of the slice: x: 4, y: 4, z: 8, core: 2. Of those that a mesh axis runs over, the one named last changes fastest.
Arguments:
- primal: float32 [49152], P('line'), may hold values from 0.1 to 10
- slacks: float32 [49152], P('line'), may hold values from 0.1 to 10
- line_cost: float32 [49152], P('line'), may hold values from -6 to 6
- bus_dual: float32 [65536], P('bus'), may hold values from -6 to 6
- demand: float32 [65536], P('bus'), may hold values from -6 to 6
- endpoints: int32 [2, 49152], P(None, 'line'), may hold values from 0 to 65535, as said below
- fixed_part: float32 [256, 256, 256], P('bus'), as said below
Outputs:
- step_primal: float32 [49152], P('line')
- step_slack: float32 [49152], P('line')
- step_dual: float32 [65536], P('bus')
- step_lengths: float32 [2], replicated
The draws below stay inside these ranges and needn't reach their ends.
Inputs may be any that keep to these rules, and one draw needn't show every extreme that they name: The two endpoints of every line differ. `fixed_part`: every block is symmetric and strictly diagonally dominant with a positive diagonal.
All inputs are finite; a program needn't handle non-finite values.
Results may differ from the reference program's by a relative error of at most 0.000043.
Values sent between devices are 32-bit elements; how exact they have to be, the bound alone decides.
A program may use at most 64 MiB of HBM per device.

```python
import math
import jax
import jax.numpy as jnp
from jax import lax

BS = 256
NLINES = 49152
NBLOCKS = 256
NBUSES = 65536


line_reach = 24


def draw_endpoints(key, part):
    keys = jax.random.split(jax.random.fold_in(key, 11), 5)
    anchor = jax.random.randint(keys[0], (NLINES,), 0, NBUSES)
    reach = jax.random.randint(keys[1], (NLINES,), 1, line_reach + 1)
    direction = jax.random.randint(keys[2], (NLINES,), 0, 2) * 2 - 1
    near_target = (anchor + direction * reach) % NBUSES
    far_target = (anchor + jax.random.randint(keys[3], (NLINES,), 1, NBUSES)) % NBUSES
    distant = jax.random.randint(keys[4], (NLINES,), 0, 4) == 0
    target = jnp.where(distant, far_target, near_target)
    return jnp.stack([anchor, target]).astype(jnp.int32)


def draw_fixed_part(key, part):
    keys = jax.random.split(jax.random.fold_in(key, 23), 2)
    raw = jax.random.normal(keys[0], (NBLOCKS, BS, BS), jnp.float32)
    raw = raw * BS ** (-0.5)
    symmetric = 0.5 * (raw + jnp.swapaxes(raw, 1, 2))
    identity = jnp.eye(BS, dtype=jnp.float32)
    offdiag = symmetric * (1.0 - identity)
    margin = jnp.exp(jax.random.uniform(keys[1], (NBLOCKS, BS), jnp.float32, jnp.log(0.5), jnp.log(2.0)))
    diagonal = jnp.sum(jnp.abs(offdiag), axis=-1) + margin
    return (offdiag + identity * diagonal[:, :, None]).astype(jnp.float32)


def block_scale(stream_key, dims, cuts, smallest, top_value):
    loudness = 1.0
    for axis_at, blocks in cuts:
        draws = jax.random.uniform(jax.random.fold_in(jax.random.fold_in(stream_key, 6), axis_at), (blocks,), jnp.float32, smallest / len(cuts), top_value / len(cuts))
        loudness = loudness * jnp.repeat(jnp.exp(draws), dims[axis_at] // blocks).reshape((-1,) + (1,) * (len(dims) - 1 - axis_at))
    return loudness


def gaussian(key, dims, spread, limit, cuts=(), held_as=jnp.bfloat16):
    entries = spread * jax.random.normal(key, dims, jnp.float32)
    if cuts:
        entries = entries * block_scale(key, dims, cuts, -0.22, 0.18)
    return jnp.clip(entries, -limit, limit).astype(held_as)


def setup_inputs(seed: int = 0) -> dict:
    streams_of = jax.random.split(jax.random.key(seed), 8)
    return {
        "primal": jnp.clip(jnp.exp(math.log(10.0) - 4.6051702 * jax.random.uniform(streams_of[0], (NLINES,), jnp.float32) ** block_scale(streams_of[0], (NLINES,), ((0, 16),), -0.2, 0.2)), 0.1, 10.0),
        "slacks": jnp.clip(jnp.exp(math.log(10.0) - 4.6051702 * jax.random.uniform(streams_of[1], (NLINES,), jnp.float32) ** block_scale(streams_of[1], (NLINES,), ((0, 16),), -0.2, 0.2)), 0.1, 10.0),
        "line_cost": gaussian(streams_of[2], (NLINES,), 1.0, 6.0, ((0, 16),), jnp.float32),
        "bus_dual": gaussian(streams_of[3], (NBUSES,), 1.0, 6.0, ((0, 16),), jnp.float32),
        "demand": gaussian(streams_of[4], (NBUSES,), 1.0, 6.0, ((0, 16),), jnp.float32),
        "endpoints": draw_endpoints(jax.random.fold_in(streams_of[7], 71), 0),
        "fixed_part": draw_fixed_part(jax.random.fold_in(streams_of[7], 71), 0),
    }


damping = 0.99

def to_buses(values, endpoints):
    total = jnp.zeros((NBUSES,), jnp.float32)
    return total.at[endpoints[0]].add(values).at[endpoints[1]].add(-values)

def to_lines(vector, endpoints):
    return vector[endpoints[0]] - vector[endpoints[1]]

def normal_blocks(scaling, endpoints, fixed_part):
    block_size = fixed_part.shape[1]
    same_block = endpoints[0] // block_size == endpoints[1] // block_size
    crossing = jnp.where(same_block, -scaling, jnp.zeros_like(scaling))
    flat = jnp.zeros((NBUSES * block_size,), jnp.float32)
    flat = flat.at[endpoints[0] * block_size + endpoints[0] % block_size].add(scaling)
    flat = flat.at[endpoints[1] * block_size + endpoints[1] % block_size].add(scaling)
    flat = flat.at[endpoints[0] * block_size + endpoints[1] % block_size].add(crossing)
    flat = flat.at[endpoints[1] * block_size + endpoints[0] % block_size].add(crossing)
    return fixed_part + flat.reshape(fixed_part.shape)

def factor_solve(factor, right_side):
    lower_half = lax.linalg.triangular_solve(factor, right_side[..., None], left_side=True, lower=True)
    solved = lax.linalg.triangular_solve(factor, lower_half, left_side=True, lower=True, transpose_a=True)
    return solved[..., 0]

def reference(primal, slacks, line_cost, bus_dual, demand, endpoints, fixed_part):
    block_shape = (fixed_part.shape[0], fixed_part.shape[1])
    dual_res = line_cost - to_lines(bus_dual, endpoints) - slacks
    scaling = primal / slacks
    gap_total = jnp.sum(primal * slacks)
    first = to_buses(primal, endpoints)
    second = to_buses(scaling * dual_res + primal, endpoints)
    third = to_buses(1.0 / slacks, endpoints)
    residual_bus = demand - first
    factor = jnp.linalg.cholesky(normal_blocks(scaling, endpoints, fixed_part))
    affine_dual = factor_solve(factor, (residual_bus + second).reshape(block_shape)).reshape(-1)
    affine_slack = dual_res - to_lines(affine_dual, endpoints)
    affine_primal = -primal - scaling * affine_slack
    step_aff_p = jnp.min(primal / jnp.maximum(-affine_primal, primal))
    step_aff_d = jnp.min(slacks / jnp.maximum(-affine_slack, slacks))
    gap_affine = jnp.sum((primal + step_aff_p * affine_primal) * (slacks + step_aff_d * affine_slack))
    centering = (gap_affine / gap_total) ** 3
    gap_mean = gap_total / NLINES
    cross = affine_primal * affine_slack
    right_side = residual_bus + second - centering * gap_mean * third + to_buses(cross / slacks, endpoints)
    step_dual = factor_solve(factor, right_side.reshape(block_shape)).reshape(-1)
    step_slack = dual_res - to_lines(step_dual, endpoints)
    step_primal = (centering * gap_mean - primal * slacks - cross) / slacks - scaling * step_slack
    final_p = jnp.min(primal / jnp.maximum(-step_primal, primal))
    final_d = jnp.min(slacks / jnp.maximum(-step_slack, slacks))
    step_lengths = damping * jnp.stack([final_p, final_d])
    return (step_primal, step_slack, step_dual, step_lengths)
```

```python
import functools

import jax
import jax.numpy as jnp
from jax import lax
from jax.experimental import pallas as pl
from jax.experimental.pallas import tpu as pltpu
from jax.sharding import PartitionSpec as P

damping = 0.99

f32 = jnp.float32
bf16 = jnp.bfloat16
MESH = pl.DeviceIdType.MESH

BS = 256
PLANE = 32
DEPTH = 8
SLOTS = 32
CHUNK = 512


def position():
    li = lax.axis_index("line")
    bi = lax.axis_index("bus")
    z = bi // 2
    c = bi - 2 * z
    return li, z, c


def split3(x):
    high = x.astype(bf16).astype(f32)
    rest = x - high
    middle = rest.astype(bf16).astype(f32)
    return high, middle, rest - middle


def contract_lanes(a, b):
    return lax.dot_general(a, b, (((1,), (1,)), ((), ())), preferred_element_type=f32)


def rows_of(shape):
    return lax.broadcasted_iota(jnp.int32, shape, 0)


def build_selector(selector, place):
    for j in range(place.shape[1] // 256):
        at = slice(256 * j, 256 * (j + 1))
        selector[:, at] = jnp.where(rows_of((BS, 256)) == place[:, at], 1.0, 0.0).astype(bf16)


def to_buses(values, block, selector):
    total = None
    pieces = [piece for v in values for piece in split3(v)]
    for j in range(block.shape[1] // CHUNK):
        at = slice(CHUNK * j, CHUNK * (j + 1))
        here = rows_of((PLANE, CHUNK)) == block[:, at]
        left = jnp.concatenate([jnp.where(here, p[:, at], 0.0).astype(bf16) for p in pieces], axis=0)
        part = contract_lanes(left, selector[:, at])
        total = part if total is None else total + part
    sums = [total[PLANE * k : PLANE * (k + 1)] for k in range(len(pieces))]
    return [sums[3 * q] + sums[3 * q + 1] + sums[3 * q + 2] for q in range(len(values))]


def to_lines(table, block, selector):
    left = jnp.concatenate([p.astype(bf16) for p in split3(table)], axis=0)
    picked = []
    for j in range(block.shape[1] // CHUNK):
        at = slice(CHUNK * j, CHUNK * (j + 1))
        found = jnp.dot(left, selector[:, at], preferred_element_type=f32)
        found = found[0:PLANE] + found[PLANE : 2 * PLANE] + found[2 * PLANE : 3 * PLANE]
        here = rows_of((PLANE, CHUNK)) == block[:, at]
        picked.append(jnp.sum(jnp.where(here, found, 0.0), axis=0, keepdims=True))
    half = len(picked) // 2
    return jnp.concatenate(picked[:half], axis=1) - jnp.concatenate(picked[half:], axis=1)


def endpoint_rows(ends, c, z):
    half = ends.shape[1] // 2
    at = pl.ds(pl.multiple_of(c * half, half), half)
    start, end = ends[0:1, at], ends[1:2, at]
    both = jnp.concatenate([start, end], axis=1)
    return start, end, both & (BS - 1), (both >> 8) - PLANE * z


def greet(li, z, c):
    barrier = pltpu.get_barrier_semaphore()
    mine = 2 * li + c

    def plane(k, carry):
        s = lax.rem(mine + k, PLANE)
        pl.semaphore_signal(barrier, 1, device_id=(s // 2, 2 * z + lax.rem(s, 2)), device_id_type=MESH)
        return carry

    def depth(k, carry):
        pl.semaphore_signal(barrier, 1, device_id=(li, 2 * lax.rem(z + k, DEPTH) + c), device_id_type=MESH)
        return carry

    lax.fori_loop(1, PLANE, plane, 0)
    lax.fori_loop(1, DEPTH, depth, 0)


def greeted():
    pl.semaphore_wait(pltpu.get_barrier_semaphore(), PLANE - 1 + DEPTH - 1)


def send_plane(pick, home, slot, recv, send_sem, recv_sem, li, z, c):
    mine = 2 * li + c

    def body(k, carry):
        s = lax.rem(mine + k, PLANE)
        l2, c2 = s // 2, lax.rem(s, 2)
        pltpu.make_async_remote_copy(
            pick(c2 * 16 + l2), recv.at[slot], send_sem, recv_sem, device_id=(l2, 2 * z + c2), device_id_type=MESH
        ).start()
        return carry

    lax.fori_loop(1, PLANE, body, 0)
    pltpu.make_async_copy(home, recv.at[slot], recv_sem).start()


def send_depth(src, recv, send_sem, recv_sem, li, z, c):
    def body(k, carry):
        pltpu.make_async_remote_copy(
            src,
            recv.at[z],
            send_sem,
            recv_sem,
            device_id=(li, 2 * lax.rem(z + k, DEPTH) + c),
            device_id_type=MESH,
        ).start()
        return carry

    lax.fori_loop(1, DEPTH, body, 0)
    pltpu.make_async_copy(src, recv.at[z], recv_sem).start()


def wait_bytes(ref, sem):
    pltpu.make_async_copy(ref, ref, sem).wait()


def sum_slots(recv, at):
    total = recv[0, :, at]
    for s in range(1, recv.shape[0]):
        total = total + recv[s, :, at]
    return total


def front_kernel(
    primal, slacks, cost, ends, bus_dual, demand, fixed,
    m_out, rhs_out, third_out, dual_out, scal_out,
    selector, partner, msg, msg_in, diff, diff_in, part, part_in, block_in,
    fixed_sem, pair_sem, msg_sem, diff_sem, part_sem,
):
    li, z, c = position()
    own = pltpu.make_async_copy(fixed.at[li], block_in, fixed_sem)
    own.start()
    greet(li, z, c)
    half = primal.shape[1] // 2
    mine = pl.ds(pl.multiple_of(c * half, half), half)
    x, s = primal[:, mine], slacks[:, mine]
    start, end, place, block = endpoint_rows(ends, c, z)
    build_selector(selector, place)
    scaling = x / s
    inverse = 1.0 / s
    gap = jnp.sum(x * s, axis=1, keepdims=True)

    first = block[:, :half]
    owner = jnp.where((start >> 8) == (end >> 8), first, -1)
    order = jnp.where(rows_of((256, 256)) < lax.broadcasted_iota(jnp.int32, (256, 256), 1), 1.0, 0.0).astype(bf16)
    carry = jnp.zeros((PLANE, 1), f32)
    packed = None
    shift = (SLOTS * lax.rem(2 * li + c, 128 // SLOTS)).astype(f32)
    values = [place[:, :half].astype(f32), place[:, half:].astype(f32), *split3(scaling)]
    for j in range(half // 256):
        at = slice(256 * j, 256 * (j + 1))
        here = rows_of((PLANE, 256)) == owner[:, at]
        marks = jnp.where(here, 1.0, 0.0)
        rank = jnp.dot(marks.astype(bf16), order, preferred_element_type=f32) + carry
        carry = carry + jnp.sum(marks, axis=1, keepdims=True)
        rank = jnp.sum(jnp.where(here, rank, 0.0), axis=0, keepdims=True)
        code = jnp.where(rank < SLOTS, rank + shift, -1.0)
        slots = jnp.where(rows_of((128, 256)).astype(f32) == code, 1.0, 0.0).astype(bf16)
        left = jnp.concatenate([jnp.where(here, v[:, at], 0.0).astype(bf16) for v in values], axis=0)
        piece = contract_lanes(left, slots)
        packed = piece if packed is None else packed + piece
    most = jnp.max(carry, axis=0, keepdims=True)
    packed = [packed[PLANE * k : PLANE * (k + 1)] for k in range(5)]

    ends_sum, third = to_buses(
        [jnp.concatenate([scaling, scaling], axis=1), jnp.concatenate([inverse, -inverse], axis=1)], block, selector
    )
    whole = jnp.concatenate(
        [ends_sum, third, packed[0], packed[1], packed[2] + packed[3] + packed[4], jnp.broadcast_to(gap, (PLANE, 128))],
        axis=1,
    )
    for b in range(PLANE):
        msg[b] = whole[b : b + 1]

    greeted()
    pair = pltpu.make_async_remote_copy(
        bus_dual, partner, pair_sem.at[0], pair_sem.at[1], device_id=(li, 2 * z + 1 - c), device_id_type=MESH
    )
    pair.start()
    at_home = c * 16 + li
    send_plane(lambda b: msg.at[b], msg.at[at_home], 2 * li + c, msg_in, msg_sem.at[0], msg_sem.at[1], li, z, c)

    pair.wait()
    mine_dual = jnp.concatenate([bus_dual[:, BS * k : BS * (k + 1)] for k in range(16)], axis=0)
    other_dual = jnp.concatenate([partner[:, BS * k : BS * (k + 1)] for k in range(16)], axis=0)
    table = jnp.concatenate(
        [jnp.where(c == 0, mine_dual, other_dual), jnp.where(c == 0, other_dual, mine_dual)], axis=0
    )
    diff[:, :half] = to_lines(table, block, selector)
    diff[:, half:] = jnp.broadcast_to(most, (1, 128))
    send_depth(diff, diff_in, diff_sem.at[0], diff_sem.at[1], li, z, c)

    wait_bytes(diff_in, diff_sem.at[1])
    dual_res = cost[:, mine] - sum_slots(diff_in, slice(0, half)) - s
    dual_out[...] = dual_res
    most = diff_in[0, :, half:]
    for k in range(1, DEPTH):
        most = jnp.maximum(most, diff_in[k, :, half:])
    flow = scaling * dual_res
    (right,) = to_buses([jnp.concatenate([flow, -flow], axis=1)], block, selector)
    whole = jnp.concatenate([right, jnp.broadcast_to(most, (PLANE, 128))], axis=1)
    for b in range(PLANE):
        part[b] = whole[b : b + 1]
    send_plane(lambda b: part.at[b], part.at[at_home], 2 * li + c, part_in, part_sem.at[0], part_sem.at[1], li, z, c)

    wait_bytes(msg_in, msg_sem.at[1])
    sums = sum_slots(msg_in, slice(0, 512))
    third_out[...] = sums[:, 256:]
    group = 128 // SLOTS

    def candidates(g, at):
        return sum(msg_in[group * g + k, :, at] for k in range(1, group)) + msg_in[group * g, :, at]

    total = None
    near = rows_of((BS, 128)).astype(f32)
    for g in range(PLANE // group):
        p, q, d = (candidates(g, slice(512 + 128 * k, 640 + 128 * k)) for k in range(3))
        from_here, to_here = near == p, near == q
        right_side = jnp.concatenate(
            [jnp.where(to_here, 1.0, 0.0).astype(bf16), jnp.where(from_here, 1.0, 0.0).astype(bf16)], axis=1
        )
        for piece in split3(d):
            left = jnp.concatenate(
                [jnp.where(from_here, piece, 0.0).astype(bf16), jnp.where(to_here, piece, 0.0).astype(bf16)], axis=1
            )
            add = contract_lanes(left, right_side)
            total = add if total is None else total + add
    own.wait()
    diagonal = rows_of((BS, BS)) == lax.broadcasted_iota(jnp.int32, (BS, BS), 1)
    m_out[...] = block_in[...] + jnp.where(diagonal, sums[:, :256], 0.0) - total

    wait_bytes(part_in, part_sem.at[1])
    rhs_out[...] = demand[:, pl.ds(pl.multiple_of(li * BS, BS), BS)] + sum_slots(part_in, slice(0, 256))
    most = part_in[0, :, 256:]
    for k in range(1, PLANE):
        most = jnp.maximum(most, part_in[k, :, 256:])
    scal_out[0:1] = sum_slots(msg_in, slice(896, 1024))
    scal_out[1:2] = most
    wait_bytes(msg_in.at[pl.ds(0, PLANE - 1)], msg_sem.at[0])
    wait_bytes(diff_in.at[pl.ds(0, DEPTH - 1)], diff_sem.at[0])
    wait_bytes(part_in.at[pl.ds(0, PLANE - 1)], part_sem.at[0])


def invert_kernel(m_ref, out_ref):
    n = m_ref.shape[0]
    w = 32
    out_ref[...] = m_ref[...]
    lane = lax.broadcasted_iota(jnp.int32, (w, 128), 1)
    row = rows_of((w, 128))
    lane1 = lax.broadcasted_iota(jnp.int32, (1, 128), 1)

    def panel(_, carry):
        ra, rb = out_ref[0:w, 0:128], out_ref[0:w, 128:256]
        for sub in range(w // 8):
            cols = [jnp.broadcast_to(ra[:, j : j + 1], (w, 128)) for j in range(8 * sub, 8 * sub + 8)]
            for k in range(8):
                r = 8 * sub + k
                ck = cols[k]
                rp = 1.0 / ck[r : r + 1, :]
                pa = jnp.where(lane1 == r, 1.0, ra[r : r + 1, :]) * rp
                pb = rb[r : r + 1, :] * rp
                here = row == r
                ra = jnp.where(here, pa, jnp.where(lane == r, 0.0, ra) - ck * pa)
                rb = jnp.where(here, pb, rb - ck * pb)
                for j in range(k + 1, 8):
                    cr = cols[j][r : r + 1, :] * rp
                    cols[j] = jnp.where(here, cr, cols[j] - ck * cr)
        top = jnp.concatenate([ra, rb], axis=1)
        rest = out_ref[w:n, :]
        wide = jnp.concatenate([top, jnp.zeros((128 - w, n), f32)], axis=0)
        update = jnp.dot(rest[:, 0:128], wide, precision=lax.Precision.HIGHEST, preferred_element_type=f32)
        lanes = lax.broadcasted_iota(jnp.int32, (n - w, n), 1)
        rest = jnp.where(lanes < w, 0.0, rest) - update
        out_ref[0 : n - w, :] = pltpu.roll(rest, n - w, 1)
        out_ref[n - w : n, :] = pltpu.roll(top, n - w, 1)
        return carry

    lax.fori_loop(0, n // w, panel, 0)


def longest_step(now, step):
    return jnp.min(now / jnp.maximum(-step, now), axis=1, keepdims=True)


def back_kernel(
    total_lines,
    primal, slacks, ends, inverse, rhs, third, dual, scal,
    step_primal, step_slack, step_dual, lengths,
    selector, solved, solved_in, diff, diff_in, part, part_in,
    solved2, solved2_in, diff2, diff2_in, final, final_in, last, last_in,
    solved_sem, diff_sem, part_sem, solved2_sem, diff2_sem, last_sem, final_sem,
):
    li, z, c = position()
    greet(li, z, c)
    half = primal.shape[1] // 2
    mine = pl.ds(pl.multiple_of(c * half, half), half)
    x, s, dual_res = primal[:, mine], slacks[:, mine], dual[...]
    _, _, place, block = endpoint_rows(ends, c, z)
    build_selector(selector, place)
    scaling = x / s
    at_home = c * 16 + li
    gap_total = scal[0:1, :]

    def solve(right):
        wide = jnp.broadcast_to(right, (8, BS))
        return jnp.dot(wide, inverse[...], precision=lax.Precision.HIGHEST, preferred_element_type=f32)[0:1]

    solved[...] = solve(rhs[...])
    greeted()
    send_plane(lambda b: solved, solved, at_home, solved_in, solved_sem.at[0], solved_sem.at[1], li, z, c)
    wait_bytes(solved_in, solved_sem.at[1])
    table = jnp.concatenate([solved_in[b] for b in range(PLANE)], axis=0)
    diff[...] = to_lines(table, block, selector)
    send_depth(diff, diff_in, diff_sem.at[0], diff_sem.at[1], li, z, c)
    wait_bytes(diff_in, diff_sem.at[1])
    affine_slack = dual_res - sum_slots(diff_in, slice(0, half))
    affine_primal = -x - scaling * affine_slack
    cross = affine_primal * affine_slack
    extra = cross / s
    (sums,) = to_buses([jnp.concatenate([extra, -extra], axis=1)], block, selector)
    lane1 = lax.broadcasted_iota(jnp.int32, (1, 128), 1)
    scalars = [
        longest_step(x, affine_primal),
        longest_step(s, affine_slack),
        jnp.sum(affine_primal * s, axis=1, keepdims=True),
        jnp.sum(x * affine_slack, axis=1, keepdims=True),
        jnp.sum(cross, axis=1, keepdims=True),
    ]
    row = jnp.zeros((1, 128), f32)
    for k, value in enumerate(scalars):
        row = jnp.where(lane1 == k, value, row)
    whole = jnp.concatenate([sums, jnp.broadcast_to(row, (PLANE, 128))], axis=1)
    for b in range(PLANE):
        part[b] = whole[b : b + 1]
    send_plane(lambda b: part.at[b], part.at[at_home], 2 * li + c, part_in, part_sem.at[0], part_sem.at[1], li, z, c)
    wait_bytes(part_in, part_sem.at[1])
    added = sum_slots(part_in, slice(0, 384))
    least = part_in[0, :, 256:384]
    for k in range(1, PLANE):
        least = jnp.minimum(least, part_in[k, :, 256:384])
    take_p, take_d = least[:, 0:1], least[:, 1:2]
    tail = added[:, 256:384]
    gap0 = gap_total[:, 0:1]
    gap_affine = gap0 + take_p * tail[:, 2:3] + take_d * tail[:, 3:4] + take_p * take_d * tail[:, 4:5]
    ratio = gap_affine / gap0
    aim = ratio * ratio * ratio * (gap0 / total_lines)
    solved2[...] = solve(rhs[...] - aim * third[...] + added[:, :256])
    send_plane(lambda b: solved2, solved2, at_home, solved2_in, solved2_sem.at[0], solved2_sem.at[1], li, z, c)
    wait_bytes(solved2_in, solved2_sem.at[1])
    table = jnp.concatenate([solved2_in[b] for b in range(PLANE)], axis=0)
    diff2[...] = to_lines(table, block, selector)
    send_depth(diff2, diff2_in, diff2_sem.at[0], diff2_sem.at[1], li, z, c)
    for b in range(16):
        step_dual[:, BS * b : BS * (b + 1)] = solved2_in[16 * c + b]
    wait_bytes(diff2_in, diff2_sem.at[1])
    slack = dual_res - sum_slots(diff2_in, slice(0, half))
    primal_step = (aim - x * s - cross) / s - scaling * slack
    row = jnp.where(lane1 == 0, longest_step(x, primal_step), longest_step(s, slack))
    last[...] = row
    final[0:1] = primal_step
    final[1:2] = slack
    step_primal[:, mine] = primal_step
    step_slack[:, mine] = slack
    send_plane(lambda b: last, last, 2 * li + c, last_in, last_sem.at[0], last_sem.at[1], li, z, c)
    pair = pltpu.make_async_remote_copy(
        final, final_in, final_sem.at[0], final_sem.at[1], device_id=(li, 2 * z + 1 - c), device_id_type=MESH
    )
    pair.start()
    pair.wait()
    other = pl.ds(pl.multiple_of((1 - c) * half, half), half)
    step_primal[:, other] = final_in[0:1]
    step_slack[:, other] = final_in[1:2]
    wait_bytes(last_in, last_sem.at[1])
    least = last_in[0]
    for k in range(1, PLANE):
        least = jnp.minimum(least, last_in[k])
    lengths[...] = damping * least
    wait_bytes(solved_in.at[pl.ds(0, PLANE - 1)], solved_sem.at[0])
    wait_bytes(diff_in.at[pl.ds(0, DEPTH - 1)], diff_sem.at[0])
    wait_bytes(part_in.at[pl.ds(0, PLANE - 1)], part_sem.at[0])
    wait_bytes(solved2_in.at[pl.ds(0, PLANE - 1)], solved2_sem.at[0])
    wait_bytes(diff2_in.at[pl.ds(0, DEPTH - 1)], diff2_sem.at[0])
    wait_bytes(last_in.at[pl.ds(0, PLANE - 1)], last_sem.at[0])


def vmem(n):
    return [pl.BlockSpec(memory_space=pltpu.VMEM)] * n


def struct(*shape):
    return jax.ShapeDtypeStruct(shape, f32)


def scattered_block(primal, slacks, endpoints, fixed_part):
    blocks_here, block_size = fixed_part.shape[0], fixed_part.shape[1]
    buses_here = blocks_here * block_size
    scaling = primal / slacks
    local = endpoints - lax.axis_index("bus") * buses_here
    own_from, own_to = jnp.where((local >= 0) & (local < buses_here), local, buses_here)
    same_block = endpoints[0] // block_size == endpoints[1] // block_size
    crossing = jnp.where(same_block, -scaling, jnp.zeros_like(scaling))
    rows = jnp.concatenate([own_from, own_to, own_from, own_to])
    columns = jnp.concatenate([own_from, own_to, own_to, own_from]) % block_size
    values = jnp.concatenate([scaling, scaling, crossing, crossing])
    flat = jnp.zeros((buses_here * block_size,), f32).at[rows * block_size + columns].add(values, mode="drop")
    lines = lax.psum_scatter(flat.reshape(-1, 128), "line", tiled=True)
    mine = lax.dynamic_index_in_dim(fixed_part, lax.axis_index("line"), 0, keepdims=False)
    return mine + lines.reshape(block_size, block_size)


def per_device(primal, slacks, line_cost, bus_dual, demand, endpoints, fixed_part):
    lines_here, buses_here = primal.shape[0], bus_dual.shape[0]
    half = lines_here // 2
    total_lines = lines_here * lax.axis_size("line")
    dma = pltpu.SemaphoreType.DMA
    x, s = primal.reshape(1, -1), slacks.reshape(1, -1)
    fast, rhs, third, dual, scal = pl.pallas_call(
        front_kernel,
        out_shape=(struct(BS, BS), struct(1, BS), struct(1, BS), struct(1, half), struct(2, 128)),
        in_specs=vmem(6) + [pl.BlockSpec(memory_space=pl.ANY)],
        out_specs=tuple(vmem(5)),
        scratch_shapes=[
            pltpu.VMEM((BS, lines_here), bf16),
            pltpu.VMEM((1, buses_here), f32),
            pltpu.VMEM((PLANE, 1, 1024), f32),
            pltpu.VMEM((PLANE, 1, 1024), f32),
            pltpu.VMEM((1, half + 128), f32),
            pltpu.VMEM((DEPTH, 1, half + 128), f32),
            pltpu.VMEM((PLANE, 1, 384), f32),
            pltpu.VMEM((PLANE, 1, 384), f32),
            pltpu.VMEM((BS, BS), f32),
            dma,
            dma((2,)),
            dma((2,)),
            dma((2,)),
            dma((2,)),
        ],
        compiler_params=pltpu.CompilerParams(collective_id=0, has_side_effects=True),
        name="front",
    )(x, s, line_cost.reshape(1, -1), endpoints, bus_dual.reshape(1, -1), demand.reshape(1, -1), fixed_part)
    normal = lax.cond(
        scal[1, 0] > SLOTS,
        lambda: scattered_block(primal, slacks, endpoints, fixed_part),
        lambda: fast,
    )
    inverse = pl.pallas_call(
        invert_kernel, out_shape=struct(BS, BS), in_specs=vmem(1), out_specs=vmem(1)[0], name="invert"
    )(normal)
    step_primal, step_slack, step_dual, lengths = pl.pallas_call(
        functools.partial(back_kernel, float(total_lines)),
        out_shape=(struct(1, lines_here), struct(1, lines_here), struct(1, buses_here), struct(1, 128)),
        in_specs=vmem(8),
        out_specs=tuple(vmem(4)),
        scratch_shapes=[
            pltpu.VMEM((BS, lines_here), bf16),
            pltpu.VMEM((1, BS), f32),
            pltpu.VMEM((PLANE, 1, BS), f32),
            pltpu.VMEM((1, half), f32),
            pltpu.VMEM((DEPTH, 1, half), f32),
            pltpu.VMEM((PLANE, 1, 384), f32),
            pltpu.VMEM((PLANE, 1, 384), f32),
            pltpu.VMEM((1, BS), f32),
            pltpu.VMEM((PLANE, 1, BS), f32),
            pltpu.VMEM((1, half), f32),
            pltpu.VMEM((DEPTH, 1, half), f32),
            pltpu.VMEM((2, half), f32),
            pltpu.VMEM((2, half), f32),
            pltpu.VMEM((1, 128), f32),
            pltpu.VMEM((PLANE, 1, 128), f32),
        ]
        + [dma((2,))] * 7,
        compiler_params=pltpu.CompilerParams(collective_id=1, has_side_effects=True),
        name="back",
    )(x, s, endpoints, inverse, rhs, third, dual, scal)
    return step_primal.reshape(-1), step_slack.reshape(-1), step_dual.reshape(-1), lengths[0, :2]


def solution(mesh):
    in_specs = (P("line"), P("line"), P("line"), P("bus"), P("bus"), P(None, "line"), P("bus", None, None))
    out_specs = (P("line"), P("line"), P("bus"), P())
    return jax.shard_map(per_device, mesh=mesh, in_specs=in_specs, out_specs=out_specs, check_vma=False)
```

```python
import functools

import jax
import jax.numpy as jnp
from jax import lax
from jax.experimental import pallas as pl
from jax.experimental.pallas import tpu as pltpu
from jax.sharding import PartitionSpec as P

damping = 0.99

f32 = jnp.float32
bf16 = jnp.bfloat16
MESH = pl.DeviceIdType.MESH

BS = 256
PLANE = 32
DEPTH = 8
SLOTS = 32
CHUNK = 512


def position():
    li = lax.axis_index("line")
    bi = lax.axis_index("bus")
    z = bi // 2
    c = bi - 2 * z
    return li, z, c


def split3(x):
    high = x.astype(bf16).astype(f32)
    rest = x - high
    middle = rest.astype(bf16).astype(f32)
    return high, middle, rest - middle


def contract_lanes(a, b):
    return lax.dot_general(a, b, (((1,), (1,)), ((), ())), preferred_element_type=f32)


def rows_of(shape):
    return lax.broadcasted_iota(jnp.int32, shape, 0)


def build_selector(selector, place):
    for j in range(place.shape[1] // 256):
        at = slice(256 * j, 256 * (j + 1))
        selector[:, at] = jnp.where(rows_of((BS, 256)) == place[:, at], 1.0, 0.0).astype(bf16)


def to_buses(values, block, selector):
    total = None
    pieces = [piece for v in values for piece in split3(v)]
    for j in range(block.shape[1] // CHUNK):
        at = slice(CHUNK * j, CHUNK * (j + 1))
        here = rows_of((PLANE, CHUNK)) == block[:, at]
        left = jnp.concatenate([jnp.where(here, p[:, at], 0.0).astype(bf16) for p in pieces], axis=0)
        part = contract_lanes(left, selector[:, at])
        total = part if total is None else total + part
    sums = [total[PLANE * k : PLANE * (k + 1)] for k in range(len(pieces))]
    return [sums[3 * q] + sums[3 * q + 1] + sums[3 * q + 2] for q in range(len(values))]


def to_lines(table, block, selector):
    left = jnp.concatenate([p.astype(bf16) for p in split3(table)], axis=0)
    picked = []
    for j in range(block.shape[1] // CHUNK):
        at = slice(CHUNK * j, CHUNK * (j + 1))
        found = jnp.dot(left, selector[:, at], preferred_element_type=f32)
        found = found[0:PLANE] + found[PLANE : 2 * PLANE] + found[2 * PLANE : 3 * PLANE]
        here = rows_of((PLANE, CHUNK)) == block[:, at]
        picked.append(jnp.sum(jnp.where(here, found, 0.0), axis=0, keepdims=True))
    half = len(picked) // 2
    return jnp.concatenate(picked[:half], axis=1) - jnp.concatenate(picked[half:], axis=1)


def endpoint_rows(ends, c, z):
    half = ends.shape[1] // 2
    at = pl.ds(pl.multiple_of(c * half, half), half)
    start, end = ends[0:1, at], ends[1:2, at]
    both = jnp.concatenate([start, end], axis=1)
    return start, end, both & (BS - 1), (both >> 8) - PLANE * z


def greet(li, z, c):
    barrier = pltpu.get_barrier_semaphore()
    mine = 2 * li + c

    def plane(k, carry):
        s = lax.rem(mine + k, PLANE)
        pl.semaphore_signal(barrier, 1, device_id=(s // 2, 2 * z + lax.rem(s, 2)), device_id_type=MESH)
        return carry

    def depth(k, carry):
        pl.semaphore_signal(barrier, 1, device_id=(li, 2 * lax.rem(z + k, DEPTH) + c), device_id_type=MESH)
        return carry

    lax.fori_loop(1, PLANE, plane, 0)
    lax.fori_loop(1, DEPTH, depth, 0)


def greeted():
    pl.semaphore_wait(pltpu.get_barrier_semaphore(), PLANE - 1 + DEPTH - 1)


def send_plane(pick, home, slot, recv, send_sem, recv_sem, li, z, c):
    mine = 2 * li + c

    def body(k, carry):
        s = lax.rem(mine + k, PLANE)
        l2, c2 = s // 2, lax.rem(s, 2)
        pltpu.make_async_remote_copy(
            pick(c2 * 16 + l2), recv.at[slot], send_sem, recv_sem, device_id=(l2, 2 * z + c2), device_id_type=MESH
        ).start()
        return carry

    lax.fori_loop(1, PLANE, body, 0)
    pltpu.make_async_copy(home, recv.at[slot], recv_sem).start()


def send_depth(src, recv, send_sem, recv_sem, li, z, c):
    def body(k, carry):
        pltpu.make_async_remote_copy(
            src,
            recv.at[z],
            send_sem,
            recv_sem,
            device_id=(li, 2 * lax.rem(z + k, DEPTH) + c),
            device_id_type=MESH,
        ).start()
        return carry

    lax.fori_loop(1, DEPTH, body, 0)
    pltpu.make_async_copy(src, recv.at[z], recv_sem).start()


def wait_bytes(ref, sem):
    pltpu.make_async_copy(ref, ref, sem).wait()


def sum_slots(recv, at):
    total = recv[0, :, at]
    for s in range(1, recv.shape[0]):
        total = total + recv[s, :, at]
    return total


def front_kernel(
    primal, slacks, cost, ends, bus_dual, demand, fixed,
    m_out, rhs_out, third_out, dual_out, scal_out,
    selector, partner, msg, msg_in, diff, diff_in, part, part_in, block_in,
    fixed_sem, pair_sem, msg_sem, diff_sem, part_sem,
):
    li, z, c = position()
    own = pltpu.make_async_copy(fixed.at[li], block_in, fixed_sem)
    own.start()
    greet(li, z, c)
    half = primal.shape[1] // 2
    mine = pl.ds(pl.multiple_of(c * half, half), half)
    x, s = primal[:, mine], slacks[:, mine]
    start, end, place, block = endpoint_rows(ends, c, z)
    build_selector(selector, place)
    scaling = x / s
    inverse = 1.0 / s
    gap = jnp.sum(x * s, axis=1, keepdims=True)

    first = block[:, :half]
    owner = jnp.where((start >> 8) == (end >> 8), first, -1)
    order = jnp.where(rows_of((256, 256)) < lax.broadcasted_iota(jnp.int32, (256, 256), 1), 1.0, 0.0).astype(bf16)
    carry = jnp.zeros((PLANE, 1), f32)
    packed = None
    shift = (SLOTS * lax.rem(2 * li + c, 128 // SLOTS)).astype(f32)
    values = [place[:, :half].astype(f32), place[:, half:].astype(f32), *split3(scaling)]
    for j in range(half // 256):
        at = slice(256 * j, 256 * (j + 1))
        here = rows_of((PLANE, 256)) == owner[:, at]
        marks = jnp.where(here, 1.0, 0.0)
        rank = jnp.dot(marks.astype(bf16), order, preferred_element_type=f32) + carry
        carry = carry + jnp.sum(marks, axis=1, keepdims=True)
        rank = jnp.sum(jnp.where(here, rank, 0.0), axis=0, keepdims=True)
        code = jnp.where(rank < SLOTS, rank + shift, -1.0)
        slots = jnp.where(rows_of((128, 256)).astype(f32) == code, 1.0, 0.0).astype(bf16)
        left = jnp.concatenate([jnp.where(here, v[:, at], 0.0).astype(bf16) for v in values], axis=0)
        piece = contract_lanes(left, slots)
        packed = piece if packed is None else packed + piece
    most = jnp.max(carry, axis=0, keepdims=True)
    packed = [packed[PLANE * k : PLANE * (k + 1)] for k in range(5)]

    ends_sum, third = to_buses(
        [jnp.concatenate([scaling, scaling], axis=1), jnp.concatenate([inverse, -inverse], axis=1)], block, selector
    )
    whole = jnp.concatenate(
        [ends_sum, third, packed[0], packed[1], packed[2] + packed[3] + packed[4], jnp.broadcast_to(gap, (PLANE, 128))],
        axis=1,
    )
    for b in range(PLANE):
        msg[b] = whole[b : b + 1]

    greeted()
    pair = pltpu.make_async_remote_copy(
        bus_dual, partner, pair_sem.at[0], pair_sem.at[1], device_id=(li, 2 * z + 1 - c), device_id_type=MESH
    )
    pair.start()
    at_home = c * 16 + li
    send_plane(lambda b: msg.at[b], msg.at[at_home], 2 * li + c, msg_in, msg_sem.at[0], msg_sem.at[1], li, z, c)

    pair.wait()
    mine_dual = jnp.concatenate([bus_dual[:, BS * k : BS * (k + 1)] for k in range(16)], axis=0)
    other_dual = jnp.concatenate([partner[:, BS * k : BS * (k + 1)] for k in range(16)], axis=0)
    table = jnp.concatenate(
        [jnp.where(c == 0, mine_dual, other_dual), jnp.where(c == 0, other_dual, mine_dual)], axis=0
    )
    diff[:, :half] = to_lines(table, block, selector)
    diff[:, half:] = jnp.broadcast_to(most, (1, 128))
    send_depth(diff, diff_in, diff_sem.at[0], diff_sem.at[1], li, z, c)

    wait_bytes(diff_in, diff_sem.at[1])
    dual_res = cost[:, mine] - sum_slots(diff_in, slice(0, half)) - s
    dual_out[...] = dual_res
    most = diff_in[0, :, half:]
    for k in range(1, DEPTH):
        most = jnp.maximum(most, diff_in[k, :, half:])
    flow = scaling * dual_res
    (right,) = to_buses([jnp.concatenate([flow, -flow], axis=1)], block, selector)
    whole = jnp.concatenate([right, jnp.broadcast_to(most, (PLANE, 128))], axis=1)
    for b in range(PLANE):
        part[b] = whole[b : b + 1]
    send_plane(lambda b: part.at[b], part.at[at_home], 2 * li + c, part_in, part_sem.at[0], part_sem.at[1], li, z, c)

    wait_bytes(msg_in, msg_sem.at[1])
    sums = sum_slots(msg_in, slice(0, 512))
    third_out[...] = sums[:, 256:]
    group = 128 // SLOTS

    def candidates(g, at):
        return sum(msg_in[group * g + k, :, at] for k in range(1, group)) + msg_in[group * g, :, at]

    total = None
    near = rows_of((BS, 128)).astype(f32)
    for g in range(PLANE // group):
        p, q, d = (candidates(g, slice(512 + 128 * k, 640 + 128 * k)) for k in range(3))
        from_here, to_here = near == p, near == q
        right_side = jnp.concatenate(
            [jnp.where(to_here, 1.0, 0.0).astype(bf16), jnp.where(from_here, 1.0, 0.0).astype(bf16)], axis=1
        )
        for piece in split3(d):
            left = jnp.concatenate(
                [jnp.where(from_here, piece, 0.0).astype(bf16), jnp.where(to_here, piece, 0.0).astype(bf16)], axis=1
            )
            add = contract_lanes(left, right_side)
            total = add if total is None else total + add
    own.wait()
    diagonal = rows_of((BS, BS)) == lax.broadcasted_iota(jnp.int32, (BS, BS), 1)
    m_out[...] = block_in[...] + jnp.where(diagonal, sums[:, :256], 0.0) - total

    wait_bytes(part_in, part_sem.at[1])
    rhs_out[...] = demand[:, pl.ds(pl.multiple_of(li * BS, BS), BS)] + sum_slots(part_in, slice(0, 256))
    most = part_in[0, :, 256:]
    for k in range(1, PLANE):
        most = jnp.maximum(most, part_in[k, :, 256:])
    scal_out[0:1] = sum_slots(msg_in, slice(896, 1024))
    scal_out[1:2] = most
    wait_bytes(msg_in.at[pl.ds(0, PLANE - 1)], msg_sem.at[0])
    wait_bytes(diff_in.at[pl.ds(0, DEPTH - 1)], diff_sem.at[0])
    wait_bytes(part_in.at[pl.ds(0, PLANE - 1)], part_sem.at[0])


def invert_kernel(m_ref, out_ref):
    n = m_ref.shape[0]
    w = 32
    out_ref[...] = m_ref[...]
    lane = lax.broadcasted_iota(jnp.int32, (w, 128), 1)
    row = rows_of((w, 128))
    lane1 = lax.broadcasted_iota(jnp.int32, (1, 128), 1)

    def panel(_, carry):
        ra, rb = out_ref[0:w, 0:128], out_ref[0:w, 128:256]
        for sub in range(w // 8):
            cols = [jnp.broadcast_to(ra[:, j : j + 1], (w, 128)) for j in range(8 * sub, 8 * sub + 8)]
            for k in range(8):
                r = 8 * sub + k
                ck = cols[k]
                rp = 1.0 / ck[r : r + 1, :]
                pa = jnp.where(lane1 == r, 1.0, ra[r : r + 1, :]) * rp
                pb = rb[r : r + 1, :] * rp
                here = row == r
                ra = jnp.where(here, pa, jnp.where(lane == r, 0.0, ra) - ck * pa)
                rb = jnp.where(here, pb, rb - ck * pb)
                for j in range(k + 1, 8):
                    cr = cols[j][r : r + 1, :] * rp
                    cols[j] = jnp.where(here, cr, cols[j] - ck * cr)
        top = jnp.concatenate([ra, rb], axis=1)
        rest = out_ref[w:n, :]
        wide = jnp.concatenate([top, jnp.zeros((128 - w, n), f32)], axis=0)
        update = jnp.dot(rest[:, 0:128], wide, precision=lax.Precision.HIGHEST, preferred_element_type=f32)
        lanes = lax.broadcasted_iota(jnp.int32, (n - w, n), 1)
        rest = jnp.where(lanes < w, 0.0, rest) - update
        out_ref[0 : n - w, :] = pltpu.roll(rest, n - w, 1)
        out_ref[n - w : n, :] = pltpu.roll(top, n - w, 1)
        return carry

    lax.fori_loop(0, n // w, panel, 0)


def longest_step(now, step):
    return jnp.min(now / jnp.maximum(-step, now), axis=1, keepdims=True)


def back_kernel(
    total_lines,
    primal, slacks, ends, inverse, rhs, third, dual, scal,
    step_primal, step_slack, step_dual, lengths,
    selector, solved, solved_in, diff, diff_in, part, part_in,
    solved2, solved2_in, diff2, diff2_in, final, final_in, last, last_in,
    solved_sem, diff_sem, part_sem, solved2_sem, diff2_sem, last_sem, final_sem,
):
    li, z, c = position()
    greet(li, z, c)
    half = primal.shape[1] // 2
    mine = pl.ds(pl.multiple_of(c * half, half), half)
    x, s, dual_res = primal[:, mine], slacks[:, mine], dual[...]
    _, _, place, block = endpoint_rows(ends, c, z)
    build_selector(selector, place)
    scaling = x / s
    at_home = c * 16 + li
    gap_total = scal[0:1, :]

    def solve(right):
        wide = jnp.broadcast_to(right, (8, BS))
        return jnp.dot(wide, inverse[...], precision=lax.Precision.HIGHEST, preferred_element_type=f32)[0:1]

    solved[...] = solve(rhs[...])
    greeted()
    send_plane(lambda b: solved, solved, at_home, solved_in, solved_sem.at[0], solved_sem.at[1], li, z, c)
    wait_bytes(solved_in, solved_sem.at[1])
    table = jnp.concatenate([solved_in[b] for b in range(PLANE)], axis=0)
    diff[...] = to_lines(table, block, selector)
    send_depth(diff, diff_in, diff_sem.at[0], diff_sem.at[1], li, z, c)
    wait_bytes(diff_in, diff_sem.at[1])
    affine_slack = dual_res - sum_slots(diff_in, slice(0, half))
    affine_primal = -x - scaling * affine_slack
    cross = affine_primal * affine_slack
    extra = cross / s
    (sums,) = to_buses([jnp.concatenate([extra, -extra], axis=1)], block, selector)
    lane1 = lax.broadcasted_iota(jnp.int32, (1, 128), 1)
    scalars = [
        longest_step(x, affine_primal),
        longest_step(s, affine_slack),
        jnp.sum(affine_primal * s, axis=1, keepdims=True),
        jnp.sum(x * affine_slack, axis=1, keepdims=True),
        jnp.sum(cross, axis=1, keepdims=True),
    ]
    row = jnp.zeros((1, 128), f32)
    for k, value in enumerate(scalars):
        row = jnp.where(lane1 == k, value, row)
    whole = jnp.concatenate([sums, jnp.broadcast_to(row, (PLANE, 128))], axis=1)
    for b in range(PLANE):
        part[b] = whole[b : b + 1]
    send_plane(lambda b: part.at[b], part.at[at_home], 2 * li + c, part_in, part_sem.at[0], part_sem.at[1], li, z, c)
    wait_bytes(part_in, part_sem.at[1])
    added = sum_slots(part_in, slice(0, 384))
    least = part_in[0, :, 256:384]
    for k in range(1, PLANE):
        least = jnp.minimum(least, part_in[k, :, 256:384])
    take_p, take_d = least[:, 0:1], least[:, 1:2]
    tail = added[:, 256:384]
    gap0 = gap_total[:, 0:1]
    gap_affine = gap0 + take_p * tail[:, 2:3] + take_d * tail[:, 3:4] + take_p * take_d * tail[:, 4:5]
    ratio = gap_affine / gap0
    aim = ratio * ratio * ratio * (gap0 / total_lines)
    solved2[...] = solve(rhs[...] - aim * third[...] + added[:, :256])
    send_plane(lambda b: solved2, solved2, at_home, solved2_in, solved2_sem.at[0], solved2_sem.at[1], li, z, c)
    wait_bytes(solved2_in, solved2_sem.at[1])
    table = jnp.concatenate([solved2_in[b] for b in range(PLANE)], axis=0)
    diff2[...] = to_lines(table, block, selector)
    send_depth(diff2, diff2_in, diff2_sem.at[0], diff2_sem.at[1], li, z, c)
    for b in range(16):
        step_dual[:, BS * b : BS * (b + 1)] = solved2_in[16 * c + b]
    wait_bytes(diff2_in, diff2_sem.at[1])
    slack = dual_res - sum_slots(diff2_in, slice(0, half))
    primal_step = (aim - x * s - cross) / s - scaling * slack
    row = jnp.where(lane1 == 0, longest_step(x, primal_step), longest_step(s, slack))
    last[...] = row
    final[0:1] = primal_step
    final[1:2] = slack
    step_primal[:, mine] = primal_step
    step_slack[:, mine] = slack
    send_plane(lambda b: last, last, 2 * li + c, last_in, last_sem.at[0], last_sem.at[1], li, z, c)
    pair = pltpu.make_async_remote_copy(
        final, final_in, final_sem.at[0], final_sem.at[1], device_id=(li, 2 * z + 1 - c), device_id_type=MESH
    )
    pair.start()
    pair.wait()
    other = pl.ds(pl.multiple_of((1 - c) * half, half), half)
    step_primal[:, other] = final_in[0:1]
    step_slack[:, other] = final_in[1:2]
    wait_bytes(last_in, last_sem.at[1])
    least = last_in[0]
    for k in range(1, PLANE):
        least = jnp.minimum(least, last_in[k])
    lengths[...] = damping * least
    wait_bytes(solved_in.at[pl.ds(0, PLANE - 1)], solved_sem.at[0])
    wait_bytes(diff_in.at[pl.ds(0, DEPTH - 1)], diff_sem.at[0])
    wait_bytes(part_in.at[pl.ds(0, PLANE - 1)], part_sem.at[0])
    wait_bytes(solved2_in.at[pl.ds(0, PLANE - 1)], solved2_sem.at[0])
    wait_bytes(diff2_in.at[pl.ds(0, DEPTH - 1)], diff2_sem.at[0])
    wait_bytes(last_in.at[pl.ds(0, PLANE - 1)], last_sem.at[0])


def vmem(n):
    return [pl.BlockSpec(memory_space=pltpu.VMEM)] * n


def struct(*shape):
    return jax.ShapeDtypeStruct(shape, f32)


def scattered_block(primal, slacks, endpoints, fixed_part):
    blocks_here, block_size = fixed_part.shape[0], fixed_part.shape[1]
    buses_here = blocks_here * block_size
    scaling = primal / slacks
    local = endpoints - lax.axis_index("bus") * buses_here
    own_from, own_to = jnp.where((local >= 0) & (local < buses_here), local, buses_here)
    same_block = endpoints[0] // block_size == endpoints[1] // block_size
    crossing = jnp.where(same_block, -scaling, jnp.zeros_like(scaling))
    rows = jnp.concatenate([own_from, own_to, own_from, own_to])
    columns = jnp.concatenate([own_from, own_to, own_to, own_from]) % block_size
    values = jnp.concatenate([scaling, scaling, crossing, crossing])
    flat = jnp.zeros((buses_here * block_size,), f32).at[rows * block_size + columns].add(values, mode="drop")
    tiles = lax.all_to_all(flat.reshape(blocks_here, block_size, block_size), "line", 0, 0, tiled=True)
    mine = lax.dynamic_index_in_dim(fixed_part, lax.axis_index("line"), 0, keepdims=False)
    return mine + jnp.sum(tiles, axis=0)


def hand_over(step_primal, step_slack, step_dual, lengths, primal_out, slack_out, dual_out, lengths_out):
    primal_out[...] = step_primal[...]
    slack_out[...] = step_slack[...]
    dual_out[...] = step_dual[...]
    lengths_out[...] = lengths[:, 0:2]


def per_device(primal, slacks, line_cost, bus_dual, demand, endpoints, fixed_part):
    lines_here, buses_here = primal.shape[0], bus_dual.shape[0]
    half = lines_here // 2
    total_lines = lines_here * lax.axis_size("line")
    dma = pltpu.SemaphoreType.DMA
    x, s = primal.reshape(1, -1), slacks.reshape(1, -1)
    fast, rhs, third, dual, scal = pl.pallas_call(
        front_kernel,
        out_shape=(struct(BS, BS), struct(1, BS), struct(1, BS), struct(1, half), struct(2, 128)),
        in_specs=vmem(6) + [pl.BlockSpec(memory_space=pl.ANY)],
        out_specs=tuple(vmem(5)),
        scratch_shapes=[
            pltpu.VMEM((BS, lines_here), bf16),
            pltpu.VMEM((1, buses_here), f32),
            pltpu.VMEM((PLANE, 1, 1024), f32),
            pltpu.VMEM((PLANE, 1, 1024), f32),
            pltpu.VMEM((1, half + 128), f32),
            pltpu.VMEM((DEPTH, 1, half + 128), f32),
            pltpu.VMEM((PLANE, 1, 384), f32),
            pltpu.VMEM((PLANE, 1, 384), f32),
            pltpu.VMEM((BS, BS), f32),
            dma,
            dma((2,)),
            dma((2,)),
            dma((2,)),
            dma((2,)),
        ],
        compiler_params=pltpu.CompilerParams(collective_id=0, has_side_effects=True),
        name="front",
    )(x, s, line_cost.reshape(1, -1), endpoints, bus_dual.reshape(1, -1), demand.reshape(1, -1), fixed_part)
    normal = lax.cond(
        scal[1, 0] > SLOTS,
        lambda: scattered_block(primal, slacks, endpoints, fixed_part),
        lambda: fast,
    )
    inverse = pl.pallas_call(
        invert_kernel, out_shape=struct(BS, BS), in_specs=vmem(1), out_specs=vmem(1)[0], name="invert"
    )(normal)
    step_primal, step_slack, step_dual, lengths = pl.pallas_call(
        functools.partial(back_kernel, float(total_lines)),
        out_shape=(struct(1, lines_here), struct(1, lines_here), struct(1, buses_here), struct(1, 128)),
        in_specs=vmem(8),
        out_specs=tuple(vmem(4)),
        scratch_shapes=[
            pltpu.VMEM((BS, lines_here), bf16),
            pltpu.VMEM((1, BS), f32),
            pltpu.VMEM((PLANE, 1, BS), f32),
            pltpu.VMEM((1, half), f32),
            pltpu.VMEM((DEPTH, 1, half), f32),
            pltpu.VMEM((PLANE, 1, 384), f32),
            pltpu.VMEM((PLANE, 1, 384), f32),
            pltpu.VMEM((1, BS), f32),
            pltpu.VMEM((PLANE, 1, BS), f32),
            pltpu.VMEM((1, half), f32),
            pltpu.VMEM((DEPTH, 1, half), f32),
            pltpu.VMEM((2, half), f32),
            pltpu.VMEM((2, half), f32),
            pltpu.VMEM((1, 128), f32),
            pltpu.VMEM((PLANE, 1, 128), f32),
        ]
        + [dma((2,))] * 7,
        compiler_params=pltpu.CompilerParams(collective_id=1, has_side_effects=True),
        name="back",
    )(x, s, endpoints, inverse, rhs, third, dual, scal)
    outputs = pl.pallas_call(
        hand_over,
        out_shape=(struct(1, lines_here), struct(1, lines_here), struct(1, buses_here), struct(1, 2)),
        in_specs=vmem(4),
        out_specs=tuple(vmem(4)),
        name="hand_over",
    )(step_primal, step_slack, step_dual, lengths)
    return tuple(out.reshape(-1) for out in outputs)


def solution(mesh):
    in_specs = (P("line"), P("line"), P("line"), P("bus"), P("bus"), P(None, "line"), P("bus", None, None))
    out_specs = (P("line"), P("line"), P("bus"), P())
    return jax.shard_map(per_device, mesh=mesh, in_specs=in_specs, out_specs=out_specs, check_vma=False)
```

```python
import functools

import jax
import jax.numpy as jnp
from jax import lax
from jax.experimental import pallas as pl
from jax.experimental.pallas import tpu as pltpu
from jax.sharding import PartitionSpec as P

damping = 0.99

f32 = jnp.float32
bf16 = jnp.bfloat16
MESH = pl.DeviceIdType.MESH

BS = 256
PLANE = 32
DEPTH = 8
SLOTS = 32
CHUNK = 512


def position():
    li = lax.axis_index("line")
    bi = lax.axis_index("bus")
    z = bi // 2
    c = bi - 2 * z
    return li, z, c


def split3(x):
    high = x.astype(bf16).astype(f32)
    rest = x - high
    middle = rest.astype(bf16).astype(f32)
    return high, middle, rest - middle


def contract_lanes(a, b):
    return lax.dot_general(a, b, (((1,), (1,)), ((), ())), preferred_element_type=f32)


def rows_of(shape):
    return lax.broadcasted_iota(jnp.int32, shape, 0)


def build_selector(selector, place):
    for j in range(place.shape[1] // 256):
        at = slice(256 * j, 256 * (j + 1))
        selector[:, at] = jnp.where(rows_of((BS, 256)) == place[:, at], 1.0, 0.0).astype(bf16)


def to_buses(values, block, selector):
    total = None
    pieces = [piece for v in values for piece in split3(v)]
    for j in range(block.shape[1] // CHUNK):
        at = slice(CHUNK * j, CHUNK * (j + 1))
        here = rows_of((PLANE, CHUNK)) == block[:, at]
        left = jnp.concatenate([jnp.where(here, p[:, at], 0.0).astype(bf16) for p in pieces], axis=0)
        part = contract_lanes(left, selector[:, at])
        total = part if total is None else total + part
    sums = [total[PLANE * k : PLANE * (k + 1)] for k in range(len(pieces))]
    return [sums[3 * q] + sums[3 * q + 1] + sums[3 * q + 2] for q in range(len(values))]


def to_lines(table, block, selector):
    left = jnp.concatenate([p.astype(bf16) for p in split3(table)], axis=0)
    picked = []
    for j in range(block.shape[1] // CHUNK):
        at = slice(CHUNK * j, CHUNK * (j + 1))
        found = jnp.dot(left, selector[:, at], preferred_element_type=f32)
        found = found[0:PLANE] + found[PLANE : 2 * PLANE] + found[2 * PLANE : 3 * PLANE]
        here = rows_of((PLANE, CHUNK)) == block[:, at]
        picked.append(jnp.sum(jnp.where(here, found, 0.0), axis=0, keepdims=True))
    half = len(picked) // 2
    return jnp.concatenate(picked[:half], axis=1) - jnp.concatenate(picked[half:], axis=1)


def endpoint_rows(ends, c, z):
    half = ends.shape[1] // 2
    at = pl.ds(pl.multiple_of(c * half, half), half)
    start, end = ends[0:1, at], ends[1:2, at]
    both = jnp.concatenate([start, end], axis=1)
    return start, end, both & (BS - 1), (both >> 8) - PLANE * z


def plane_peers(li, z, c):
    y, x = li // 4, lax.rem(li, 4)
    ys = [lax.rem(y + d, 4) for d in range(4)]
    xs = [lax.rem(x + d, 4) for d in range(4)]
    cs = [c, 1 - c]
    reach = [0, 1, 2, 1]
    offsets = [(dy, dx, dc) for dy in range(4) for dx in range(4) for dc in range(2)]
    offsets.sort(key=lambda o: -reach[o[0]] - reach[o[1]])
    peers = []
    for dy, dx, dc in offsets[:-2] + [(0, 0, 1)]:
        l2, c2 = ys[dy] * 4 + xs[dx], cs[dc]
        peers.append((c2 * 16 + l2, (l2, 2 * z + c2)))
    return peers


def depth_peers(li, z, c):
    return [(li, 2 * lax.rem(z + d, DEPTH) + c) for d in (4, 3, 5, 2, 6, 1, 7)]


def greet(li, z, c):
    barrier = pltpu.get_barrier_semaphore()
    for device in [device for _, device in plane_peers(li, z, c)] + depth_peers(li, z, c):
        pl.semaphore_signal(barrier, 1, device_id=device, device_id_type=MESH)


def greeted():
    pl.semaphore_wait(pltpu.get_barrier_semaphore(), PLANE - 1 + DEPTH - 1)


def send_plane(pick, home, slot, recv, sems, li, z, c):
    for place, device in plane_peers(li, z, c):
        pltpu.make_async_remote_copy(
            pick(place), recv.at[slot], sems.at[0], sems.at[1], device_id=device, device_id_type=MESH
        ).start()
    pltpu.make_async_copy(home, recv.at[slot], sems.at[1]).start()


def send_depth(src, recv, sems, li, z, c):
    for device in depth_peers(li, z, c):
        pltpu.make_async_remote_copy(
            src, recv.at[z], sems.at[0], sems.at[1], device_id=device, device_id_type=MESH
        ).start()
    pltpu.make_async_copy(src, recv.at[z], sems.at[1]).start()


def wait_bytes(ref, sem):
    pltpu.make_async_copy(ref, ref, sem).wait()


def sum_slots(recv, at):
    total = recv[0, :, at]
    for s in range(1, recv.shape[0]):
        total = total + recv[s, :, at]
    return total


def invert(work):
    n, w = work.shape[0], 32
    lane = lax.broadcasted_iota(jnp.int32, (w, 128), 1)
    row = rows_of((w, 128))
    lane1 = lax.broadcasted_iota(jnp.int32, (1, 128), 1)

    def panel(_, carry):
        ra, rb = work[0:w, 0:128], work[0:w, 128:256]
        for sub in range(w // 8):
            cols = [jnp.broadcast_to(ra[:, j : j + 1], (w, 128)) for j in range(8 * sub, 8 * sub + 8)]
            for k in range(8):
                r = 8 * sub + k
                ck = cols[k]
                rp = 1.0 / ck[r : r + 1, :]
                pa = jnp.where(lane1 == r, 1.0, ra[r : r + 1, :]) * rp
                pb = rb[r : r + 1, :] * rp
                here = row == r
                ra = jnp.where(here, pa, jnp.where(lane == r, 0.0, ra) - ck * pa)
                rb = jnp.where(here, pb, rb - ck * pb)
                for j in range(k + 1, 8):
                    cr = cols[j][r : r + 1, :] * rp
                    cols[j] = jnp.where(here, cr, cols[j] - ck * cr)
        top = jnp.concatenate([ra, rb], axis=1)
        rest = work[w:n, :]
        wide = jnp.concatenate([top, jnp.zeros((128 - w, n), f32)], axis=0)
        update = jnp.dot(rest[:, 0:128], wide, precision=lax.Precision.HIGHEST, preferred_element_type=f32)
        lanes = lax.broadcasted_iota(jnp.int32, (n - w, n), 1)
        rest = jnp.where(lanes < w, 0.0, rest) - update
        work[0 : n - w, :] = pltpu.roll(rest, n - w, 1)
        work[n - w : n, :] = pltpu.roll(top, n - w, 1)
        return carry

    lax.fori_loop(0, n // w, panel, 0)


def longest_step(now, step):
    return jnp.min(now / jnp.maximum(-step, now), axis=1, keepdims=True)


def buckets(owner, values, shift):
    order = jnp.where(rows_of((256, 256)) < lax.broadcasted_iota(jnp.int32, (256, 256), 1), 1.0, 0.0).astype(bf16)
    carry = jnp.zeros((PLANE, 1), f32)
    packed = None
    for j in range(owner.shape[1] // 256):
        at = slice(256 * j, 256 * (j + 1))
        here = rows_of((PLANE, 256)) == owner[:, at]
        marks = jnp.where(here, 1.0, 0.0)
        rank = jnp.dot(marks.astype(bf16), order, preferred_element_type=f32) + carry
        carry = carry + jnp.sum(marks, axis=1, keepdims=True)
        rank = jnp.sum(jnp.where(here, rank, 0.0), axis=0, keepdims=True)
        code = jnp.where(rank < SLOTS, rank + shift, -1.0)
        slots = jnp.where(rows_of((128, 256)).astype(f32) == code, 1.0, 0.0).astype(bf16)
        left = jnp.concatenate([jnp.where(here, v[:, at], 0.0).astype(bf16) for v in values], axis=0)
        piece = contract_lanes(left, slots)
        packed = piece if packed is None else packed + piece
    packed = [packed[PLANE * k : PLANE * (k + 1)] for k in range(len(values))]
    return packed, jnp.max(carry, axis=0, keepdims=True)


def bucket_lines(msg_in):
    group = 128 // SLOTS

    def candidates(g, at):
        return sum(msg_in[group * g + k, :, at] for k in range(1, group)) + msg_in[group * g, :, at]

    total = None
    near = rows_of((BS, 128)).astype(f32)
    for g in range(PLANE // group):
        p, q, d = (candidates(g, slice(512 + 128 * k, 640 + 128 * k)) for k in range(3))
        from_here, to_here = near == p, near == q
        right_side = jnp.concatenate(
            [jnp.where(to_here, 1.0, 0.0).astype(bf16), jnp.where(from_here, 1.0, 0.0).astype(bf16)], axis=1
        )
        for piece in split3(d):
            left = jnp.concatenate(
                [jnp.where(from_here, piece, 0.0).astype(bf16), jnp.where(to_here, piece, 0.0).astype(bf16)], axis=1
            )
            add = contract_lanes(left, right_side)
            total = add if total is None else total + add
    return total


def step_kernel(
    total_lines, given,
    primal, slacks, cost, ends, bus_dual, demand, normal,
    step_primal, step_slack, step_dual, lengths, fullest,
    selector, partner, msg, msg_in, diff0, diff0_in, part0, part0_in, block_in, work,
    solved, solved_in, diff, diff_in, part, part_in, solved2, solved2_in, diff2, diff2_in, final, final_in, last, last_in,
    fixed_sem, pair_sem, msg_sem, diff0_sem, part0_sem,
    solved_sem, diff_sem, part_sem, solved2_sem, diff2_sem, last_sem, final_sem,
):
    li, z, c = position()
    own = pltpu.make_async_copy(normal if given else normal.at[li], block_in, fixed_sem)
    own.start()
    greet(li, z, c)
    half = primal.shape[1] // 2
    mine = pl.ds(pl.multiple_of(c * half, half), half)
    at_home = c * 16 + li
    source = 2 * li + c
    lane1 = lax.broadcasted_iota(jnp.int32, (1, 128), 1)
    x, s = primal[:, mine], slacks[:, mine]
    start, end, place, block = endpoint_rows(ends, c, z)
    build_selector(selector, place)
    scaling = x / s
    inverse = 1.0 / s
    gap = jnp.sum(x * s, axis=1, keepdims=True)
    owner = jnp.where((start >> 8) == (end >> 8), block[:, :half], -1)
    shift = (SLOTS * lax.rem(source, 128 // SLOTS)).astype(f32)
    packed, most = buckets(
        owner, [place[:, :half].astype(f32), place[:, half:].astype(f32), *split3(scaling)], shift
    )
    ends_sum, third = to_buses(
        [jnp.concatenate([scaling, scaling], axis=1), jnp.concatenate([inverse, -inverse], axis=1)], block, selector
    )
    whole = jnp.concatenate(
        [ends_sum, third, packed[0], packed[1], packed[2] + packed[3] + packed[4], jnp.broadcast_to(gap, (PLANE, 128))],
        axis=1,
    )
    for b in range(PLANE):
        msg[b] = whole[b : b + 1]

    greeted()
    pair = pltpu.make_async_remote_copy(
        bus_dual, partner, pair_sem.at[0], pair_sem.at[1], device_id=(li, 2 * z + 1 - c), device_id_type=MESH
    )
    pair.start()
    send_plane(lambda b: msg.at[b], msg.at[at_home], source, msg_in, msg_sem, li, z, c)

    pair.wait()
    mine_dual = jnp.concatenate([bus_dual[:, BS * k : BS * (k + 1)] for k in range(16)], axis=0)
    other_dual = jnp.concatenate([partner[:, BS * k : BS * (k + 1)] for k in range(16)], axis=0)
    table = jnp.concatenate(
        [jnp.where(c == 0, mine_dual, other_dual), jnp.where(c == 0, other_dual, mine_dual)], axis=0
    )
    diff0[:, :half] = to_lines(table, block, selector)
    diff0[:, half:] = jnp.broadcast_to(most, (1, 128))
    send_depth(diff0, diff0_in, diff0_sem, li, z, c)

    wait_bytes(msg_in, msg_sem.at[1])
    sums = sum_slots(msg_in, slice(0, 512))
    third = sums[:, 256:]
    gap0 = sum_slots(msg_in, slice(896, 1024))[:, 0:1]
    own.wait()
    if given:
        work[...] = block_in[...]
    else:
        diagonal = rows_of((BS, BS)) == lax.broadcasted_iota(jnp.int32, (BS, BS), 1)
        work[...] = block_in[...] + jnp.where(diagonal, sums[:, :256], 0.0) - bucket_lines(msg_in)

    wait_bytes(diff0_in, diff0_sem.at[1])
    dual_res = cost[:, mine] - sum_slots(diff0_in, slice(0, half)) - s
    most = diff0_in[0, :, half:]
    for k in range(1, DEPTH):
        most = jnp.maximum(most, diff0_in[k, :, half:])
    flow = scaling * dual_res
    (right,) = to_buses([jnp.concatenate([flow, -flow], axis=1)], block, selector)
    whole = jnp.concatenate([right, jnp.broadcast_to(most, (PLANE, 128))], axis=1)
    for b in range(PLANE):
        part0[b] = whole[b : b + 1]
    send_plane(lambda b: part0.at[b], part0.at[at_home], source, part0_in, part0_sem, li, z, c)
    invert(work)
    wait_bytes(part0_in, part0_sem.at[1])
    right = demand[:, pl.ds(pl.multiple_of(li * BS, BS), BS)] + sum_slots(part0_in, slice(0, 256))
    most = part0_in[0, :, 256:]
    for k in range(1, PLANE):
        most = jnp.maximum(most, part0_in[k, :, 256:])
    fullest[...] = most[:, 0:1]

    def solve(vector):
        wide = jnp.broadcast_to(vector, (8, BS))
        return jnp.dot(wide, work[...], precision=lax.Precision.HIGHEST, preferred_element_type=f32)[0:1]

    solved[...] = solve(right)
    send_plane(lambda b: solved, solved, at_home, solved_in, solved_sem, li, z, c)
    wait_bytes(solved_in, solved_sem.at[1])
    table = jnp.concatenate([solved_in[b] for b in range(PLANE)], axis=0)
    diff[...] = to_lines(table, block, selector)
    send_depth(diff, diff_in, diff_sem, li, z, c)
    wait_bytes(diff_in, diff_sem.at[1])
    affine_slack = dual_res - sum_slots(diff_in, slice(0, half))
    affine_primal = -x - scaling * affine_slack
    cross = affine_primal * affine_slack
    extra = cross / s
    (sums,) = to_buses([jnp.concatenate([extra, -extra], axis=1)], block, selector)
    scalars = [
        longest_step(x, affine_primal),
        longest_step(s, affine_slack),
        jnp.sum(affine_primal * s, axis=1, keepdims=True),
        jnp.sum(x * affine_slack, axis=1, keepdims=True),
        jnp.sum(cross, axis=1, keepdims=True),
    ]
    row = jnp.zeros((1, 128), f32)
    for k, value in enumerate(scalars):
        row = jnp.where(lane1 == k, value, row)
    whole = jnp.concatenate([sums, jnp.broadcast_to(row, (PLANE, 128))], axis=1)
    for b in range(PLANE):
        part[b] = whole[b : b + 1]
    send_plane(lambda b: part.at[b], part.at[at_home], source, part_in, part_sem, li, z, c)
    wait_bytes(part_in, part_sem.at[1])

    added = sum_slots(part_in, slice(0, 384))
    least = part_in[0, :, 256:384]
    for k in range(1, PLANE):
        least = jnp.minimum(least, part_in[k, :, 256:384])
    take_p, take_d = least[:, 0:1], least[:, 1:2]
    tail = added[:, 256:384]
    gap_affine = gap0 + take_p * tail[:, 2:3] + take_d * tail[:, 3:4] + take_p * take_d * tail[:, 4:5]
    ratio = gap_affine / gap0
    aim = ratio * ratio * ratio * (gap0 / total_lines)
    solved2[...] = solve(right - aim * third + added[:, :256])
    send_plane(lambda b: solved2, solved2, at_home, solved2_in, solved2_sem, li, z, c)
    wait_bytes(solved2_in, solved2_sem.at[1])
    table = jnp.concatenate([solved2_in[b] for b in range(PLANE)], axis=0)
    diff2[...] = to_lines(table, block, selector)
    send_depth(diff2, diff2_in, diff2_sem, li, z, c)
    for b in range(16):
        step_dual[:, BS * b : BS * (b + 1)] = solved2_in[16 * c + b]
    wait_bytes(diff2_in, diff2_sem.at[1])
    slack = dual_res - sum_slots(diff2_in, slice(0, half))
    primal_step = (aim - x * s - cross) / s - scaling * slack
    last[...] = jnp.where(lane1 == 0, longest_step(x, primal_step), longest_step(s, slack))
    final[0:1] = primal_step
    final[1:2] = slack
    send_plane(lambda b: last, last, source, last_in, last_sem, li, z, c)
    pair2 = pltpu.make_async_remote_copy(
        final, final_in, final_sem.at[0], final_sem.at[1], device_id=(li, 2 * z + 1 - c), device_id_type=MESH
    )
    pair2.start()
    step_primal[:, mine] = primal_step
    step_slack[:, mine] = slack
    pair2.wait()
    other = pl.ds(pl.multiple_of((1 - c) * half, half), half)
    step_primal[:, other] = final_in[0:1]
    step_slack[:, other] = final_in[1:2]
    for recv, sems in (
        (msg_in, msg_sem), (diff0_in, diff0_sem), (part0_in, part0_sem), (solved_in, solved_sem), (diff_in, diff_sem),
        (part_in, part_sem), (solved2_in, solved2_sem), (diff2_in, diff2_sem), (last_in, last_sem),
    ):
        wait_bytes(recv.at[pl.ds(0, recv.shape[0] - 1)], sems.at[0])
    wait_bytes(last_in, last_sem.at[1])
    least = last_in[0]
    for k in range(1, PLANE):
        least = jnp.minimum(least, last_in[k])
    lengths[...] = damping * least


def vmem(n):
    return [pl.BlockSpec(memory_space=pltpu.VMEM)] * n


def struct(*shape):
    return jax.ShapeDtypeStruct(shape, f32)


def scattered_block(primal, slacks, endpoints, fixed_part):
    blocks_here, block_size = fixed_part.shape[0], fixed_part.shape[1]
    buses_here = blocks_here * block_size
    scaling = primal / slacks
    local = endpoints - lax.axis_index("bus") * buses_here
    own_from, own_to = jnp.where((local >= 0) & (local < buses_here), local, buses_here)
    same_block = endpoints[0] // block_size == endpoints[1] // block_size
    crossing = jnp.where(same_block, -scaling, jnp.zeros_like(scaling))
    rows = jnp.concatenate([own_from, own_to, own_from, own_to])
    columns = jnp.concatenate([own_from, own_to, own_to, own_from]) % block_size
    values = jnp.concatenate([scaling, scaling, crossing, crossing])
    flat = jnp.zeros((buses_here * block_size,), f32).at[rows * block_size + columns].add(values, mode="drop")
    tiles = lax.all_to_all(flat.reshape(blocks_here, block_size, block_size), "line", 0, 0, tiled=True)
    mine = lax.dynamic_index_in_dim(fixed_part, lax.axis_index("line"), 0, keepdims=False)
    return mine + jnp.sum(tiles, axis=0)


def hand_over(step_primal, step_slack, step_dual, lengths, primal_out, slack_out, dual_out, lengths_out):
    primal_out[...] = step_primal[...]
    slack_out[...] = step_slack[...]
    dual_out[...] = step_dual[...]
    lengths_out[...] = lengths[:, 0:2]


def whole_step(given, args, normal):
    x, s, cost, ends, bus_dual, demand = args
    lines_here, buses_here = x.shape[1], bus_dual.shape[1]
    half = lines_here // 2
    total_lines = float(lines_here * lax.axis_size("line"))
    dma = pltpu.SemaphoreType.DMA
    exchange = lambda slots, width: [pltpu.VMEM((1, width), f32), pltpu.VMEM((slots, 1, width), f32)]
    buckets_of = lambda width: [pltpu.VMEM((PLANE, 1, width), f32)] * 2
    return pl.pallas_call(
        functools.partial(step_kernel, total_lines, given),
        out_shape=(struct(1, lines_here), struct(1, lines_here), struct(1, buses_here), struct(1, 128), struct(1, 1)),
        in_specs=vmem(6) + [pl.BlockSpec(memory_space=pl.ANY)],
        out_specs=tuple(vmem(5)),
        scratch_shapes=[pltpu.VMEM((BS, lines_here), bf16), pltpu.VMEM((1, buses_here), f32)]
        + buckets_of(1024)
        + exchange(DEPTH, half + 128)
        + buckets_of(384)
        + [pltpu.VMEM((BS, BS), f32)] * 2
        + exchange(PLANE, BS)
        + exchange(DEPTH, half)
        + buckets_of(384)
        + exchange(PLANE, BS)
        + exchange(DEPTH, half)
        + [pltpu.VMEM((2, half), f32)] * 2
        + exchange(PLANE, 128)
        + [dma]
        + [dma((2,))] * 11,
        compiler_params=pltpu.CompilerParams(collective_id=int(given), has_side_effects=True),
        name="step_given" if given else "step",
    )(*args, normal)


def per_device(primal, slacks, line_cost, bus_dual, demand, endpoints, fixed_part):
    args = tuple(a.reshape(1, -1) for a in (primal, slacks, line_cost))
    args += (endpoints, bus_dual.reshape(1, -1), demand.reshape(1, -1))
    *steps, fullest = whole_step(False, args, fixed_part)

    def out(step_primal, step_slack, step_dual, lengths):
        return pl.pallas_call(
            hand_over,
            out_shape=tuple(struct(*a.shape) for a in (step_primal, step_slack, step_dual)) + (struct(1, 2),),
            in_specs=vmem(4),
            out_specs=tuple(vmem(4)),
            name="hand_over",
        )(step_primal, step_slack, step_dual, lengths)

    def again():
        normal = scattered_block(primal, slacks, endpoints, fixed_part)
        return out(*whole_step(True, args, normal)[:4])

    outputs = lax.cond(fullest[0, 0] > SLOTS, again, lambda: out(*steps))
    return tuple(a.reshape(-1) for a in outputs)


def solution(mesh):
    in_specs = (P("line"), P("line"), P("line"), P("bus"), P("bus"), P(None, "line"), P("bus", None, None))
    out_specs = (P("line"), P("line"), P("bus"), P())
    return jax.shard_map(per_device, mesh=mesh, in_specs=in_specs, out_specs=out_specs, check_vma=False)
```

```python
import functools

import jax
import jax.numpy as jnp
from jax import lax
from jax.experimental import pallas as pl
from jax.experimental.pallas import tpu as pltpu
from jax.sharding import PartitionSpec as P

damping = 0.99

f32 = jnp.float32
bf16 = jnp.bfloat16
MESH = pl.DeviceIdType.MESH

BS = 256
PLANE = 32
DEPTH = 8
SLOTS = 32
CHUNK = 512


def position():
    li = lax.axis_index("line")
    bi = lax.axis_index("bus")
    z = bi // 2
    c = bi - 2 * z
    return li, z, c


def split3(x):
    high = x.astype(bf16).astype(f32)
    rest = x - high
    middle = rest.astype(bf16).astype(f32)
    return high, middle, rest - middle


def contract_lanes(a, b):
    return lax.dot_general(a, b, (((1,), (1,)), ((), ())), preferred_element_type=f32)


def rows_of(shape):
    return lax.broadcasted_iota(jnp.int32, shape, 0)


def build_selector(selector, place):
    for j in range(place.shape[1] // 256):
        at = slice(256 * j, 256 * (j + 1))
        selector[:, at] = jnp.where(rows_of((BS, 256)) == place[:, at], 1.0, 0.0).astype(bf16)


def to_buses(values, block, selector):
    total = None
    pieces = [piece for v in values for piece in split3(v)]
    for j in range(block.shape[1] // CHUNK):
        at = slice(CHUNK * j, CHUNK * (j + 1))
        here = rows_of((PLANE, CHUNK)) == block[:, at]
        left = jnp.concatenate([jnp.where(here, p[:, at], 0.0).astype(bf16) for p in pieces], axis=0)
        part = contract_lanes(left, selector[:, at])
        total = part if total is None else total + part
    sums = [total[PLANE * k : PLANE * (k + 1)] for k in range(len(pieces))]
    return [sums[3 * q] + sums[3 * q + 1] + sums[3 * q + 2] for q in range(len(values))]


def to_lines(table, block, selector):
    left = jnp.concatenate([p.astype(bf16) for p in split3(table)], axis=0)
    picked = []
    for j in range(block.shape[1] // CHUNK):
        at = slice(CHUNK * j, CHUNK * (j + 1))
        found = jnp.dot(left, selector[:, at], preferred_element_type=f32)
        found = found[0:PLANE] + found[PLANE : 2 * PLANE] + found[2 * PLANE : 3 * PLANE]
        here = rows_of((PLANE, CHUNK)) == block[:, at]
        picked.append(jnp.sum(jnp.where(here, found, 0.0), axis=0, keepdims=True))
    half = len(picked) // 2
    return jnp.concatenate(picked[:half], axis=1) - jnp.concatenate(picked[half:], axis=1)


def endpoint_rows(ends, z):
    start, end = ends[0:1, :], ends[1:2, :]
    both = jnp.concatenate([start, end], axis=1)
    return start, end, both & (BS - 1), (both >> 8) - PLANE * z


def plane_peers(li, z, c):
    y, x = li // 4, lax.rem(li, 4)
    ys = [lax.rem(y + d, 4) for d in range(4)]
    xs = [lax.rem(x + d, 4) for d in range(4)]
    cs = [c, 1 - c]
    reach = [0, 1, 2, 1]
    offsets = [(dy, dx, dc) for dy in range(4) for dx in range(4) for dc in range(2)]
    offsets.sort(key=lambda o: -reach[o[0]] - reach[o[1]])
    peers = []
    for dy, dx, dc in offsets[:-2] + [(0, 0, 1)]:
        l2, c2 = ys[dy] * 4 + xs[dx], cs[dc]
        peers.append((c2 * 16 + l2, (l2, 2 * z + c2)))
    return peers


def depth_peers(li, z, c):
    return [(li, 2 * lax.rem(z + d, DEPTH) + c) for d in (4, 3, 5, 2, 6, 1, 7)]


def greet(li, z, c):
    barrier = pltpu.get_barrier_semaphore()
    for device in [device for _, device in plane_peers(li, z, c)] + depth_peers(li, z, c):
        pl.semaphore_signal(barrier, 1, device_id=device, device_id_type=MESH)


def greeted():
    pl.semaphore_wait(pltpu.get_barrier_semaphore(), PLANE - 1 + DEPTH - 1)


def send_plane(pick, home, slot, recv, sems, li, z, c):
    for place, device in plane_peers(li, z, c):
        pltpu.make_async_remote_copy(
            pick(place), recv.at[slot], sems.at[0], sems.at[1], device_id=device, device_id_type=MESH
        ).start()
    pltpu.make_async_copy(home, recv.at[slot], sems.at[1]).start()


def send_depth(src, recv, sems, li, z, c):
    for device in depth_peers(li, z, c):
        pltpu.make_async_remote_copy(
            src, recv.at[z], sems.at[0], sems.at[1], device_id=device, device_id_type=MESH
        ).start()
    pltpu.make_async_copy(src, recv.at[z], sems.at[1]).start()


def wait_bytes(ref, sem):
    pltpu.make_async_copy(ref, ref, sem).wait()


def sum_slots(recv, at):
    total = recv[0, :, at]
    for s in range(1, recv.shape[0]):
        total = total + recv[s, :, at]
    return total


def eliminate(pa, pb, off):
    groups = len(pa)
    lane, row = lax.broadcasted_iota(jnp.int32, (8, 128), 1), rows_of((8, 128))

    def spread(sub):
        first = off + 8 * sub
        return [[jnp.broadcast_to(p[:, j : j + 1], (8, 128)) for p in pa] for j in range(first, first + 8)]

    columns, ahead = spread(0), None
    for sub in range(groups):
        first = off + 8 * sub
        inside = (lane >= first) & (lane < first + 8)
        unit = jnp.where(lane - first == row, 1.0, 0.0)
        pa = [jnp.where(inside, unit if g == sub else 0.0, pa[g]) for g in range(groups)]
        for k in range(8):
            if k == 3 and sub + 1 < groups:
                ahead = spread(sub + 1)
            pivot = columns[k]
            scale = 1.0 / pivot[sub][k : k + 1]
            here = row == k

            def swept(rows):
                top = rows[sub][k : k + 1] * scale
                rest = [rows[g] - pivot[g] * top for g in range(groups)]
                rest[sub] = jnp.where(here, top, rest[sub])
                return rest

            columns = columns[: k + 1] + [swept(c) for c in columns[k + 1 :]]
            if ahead is not None:
                ahead = [swept(c) for c in ahead]
            pa, pb = swept(pa), swept(pb)
        columns, ahead = ahead, None
    return pa, pb


def invert(work, between):
    n, w = work.shape[0], 32
    now = work[0:w, :]
    for i in range(n // w):
        slab, off = divmod(w * i, 128)
        a = slice(128 * slab, 128 * slab + 128)
        b = slice(128 - 128 * slab, 256 - 128 * slab)
        groups = range(0, w, 8)
        pa, pb = eliminate([now[g : g + 8, a] for g in groups], [now[g : g + 8, b] for g in groups], off)
        pa, pb = jnp.concatenate(pa, axis=0), jnp.concatenate(pb, axis=0)
        top = jnp.concatenate([pa, pb] if slab == 0 else [pb, pa], axis=1)
        parts = [jnp.zeros((off, n), f32)] * (off > 0) + [top]
        parts += [jnp.zeros((128 - w - off, n), f32)] * (off + w < 128)
        wide = jnp.concatenate(parts, axis=0)

        def take(rows):
            lanes = lax.broadcasted_iota(jnp.int32, rows.shape, 1)
            kept = jnp.where((lanes >= w * i) & (lanes < w * i + w), 0.0, rows)
            return kept - jnp.dot(rows[:, a], wide, precision=lax.Precision.HIGHEST, preferred_element_type=f32)

        low, high = w * i, w * i + w
        work[low:high, :] = top
        if high < n:
            now = take(work[high : high + w, :])
        if high + w < n:
            work[high + w : n, :] = take(work[high + w : n, :])
        if low > 0:
            work[0:low, :] = take(work[0:low, :])
        between(i)


def longest_step(now, step):
    return jnp.min(now / jnp.maximum(-step, now), axis=1, keepdims=True)


def buckets(owner, values, shift):
    order = jnp.where(rows_of((256, 256)) < lax.broadcasted_iota(jnp.int32, (256, 256), 1), 1.0, 0.0).astype(bf16)
    carry = jnp.zeros((PLANE, 1), f32)
    packed = None
    for j in range(owner.shape[1] // 256):
        at = slice(256 * j, 256 * (j + 1))
        here = rows_of((PLANE, 256)) == owner[:, at]
        marks = jnp.where(here, 1.0, 0.0)
        rank = jnp.dot(marks.astype(bf16), order, preferred_element_type=f32) + carry
        carry = carry + jnp.sum(marks, axis=1, keepdims=True)
        rank = jnp.sum(jnp.where(here, rank, 0.0), axis=0, keepdims=True)
        code = jnp.where(rank < SLOTS, rank + shift, -1.0)
        slots = jnp.where(rows_of((128, 256)).astype(f32) == code, 1.0, 0.0).astype(bf16)
        left = jnp.concatenate([jnp.where(here, v[:, at], 0.0).astype(bf16) for v in values], axis=0)
        piece = contract_lanes(left, slots)
        packed = piece if packed is None else packed + piece
    packed = [packed[PLANE * k : PLANE * (k + 1)] for k in range(len(values))]
    return packed, jnp.max(carry, axis=0, keepdims=True)


def bucket_lines(msg_in):
    group = 128 // SLOTS

    def candidates(g, at):
        return sum(msg_in[group * g + k, :, at] for k in range(1, group)) + msg_in[group * g, :, at]

    total = None
    near = rows_of((BS, 128)).astype(f32)
    for g in range(PLANE // group):
        p, q, d = (candidates(g, slice(256 + 128 * k, 384 + 128 * k)) for k in range(3))
        from_here, to_here = near == p, near == q
        right_side = jnp.concatenate(
            [jnp.where(to_here, 1.0, 0.0).astype(bf16), jnp.where(from_here, 1.0, 0.0).astype(bf16)], axis=1
        )
        for piece in split3(d):
            left = jnp.concatenate(
                [jnp.where(from_here, piece, 0.0).astype(bf16), jnp.where(to_here, piece, 0.0).astype(bf16)], axis=1
            )
            add = contract_lanes(left, right_side)
            total = add if total is None else total + add
    return total


def step_kernel(
    total_lines, given,
    primal_all, slacks_all, cost_all, ends_all, bus_dual_all, demand_all, normal,
    step_primal, step_slack, step_dual, lengths, fullest,
    primal, slacks, cost, ends, bus_dual, demand, selector, partner, msg, msg_in, diff0, diff0_in, part0, part0_in, block_in, work, dual_res,
    solved, solved_in, diff, diff_in, part, part_in, solved2, solved2_in, diff2, diff2_in, final, final_in, last, last_in,
    in_sem, fixed_sem, pair_sem, msg_sem, diff0_sem, part0_sem,
    solved_sem, diff_sem, part_sem, solved2_sem, diff2_sem, last_sem, final_sem,
):
    li, z, c = position()
    greet(li, z, c)
    half = primal.shape[1]
    mine = pl.ds(pl.multiple_of(c * half, half), half)
    own_buses = pl.ds(pl.multiple_of(li * BS, BS), BS)
    copies = [
        pltpu.make_async_copy(src, dst, in_sem.at[k])
        for k, (src, dst) in enumerate(
            (
                (ends_all.at[:, mine], ends),
                (primal_all.at[:, mine], primal),
                (slacks_all.at[:, mine], slacks),
                (bus_dual_all, bus_dual),
                (cost_all.at[:, mine], cost),
                (demand_all.at[:, own_buses], demand),
            )
        )
    ]
    for copy in copies:
        copy.start()
    own = pltpu.make_async_copy(normal if given else normal.at[li], block_in, fixed_sem)
    own.start()
    at_home = c * 16 + li
    source = 2 * li + c
    lane1 = lax.broadcasted_iota(jnp.int32, (1, 128), 1)
    copies[0].wait()
    start, end, place, block = endpoint_rows(ends, z)
    build_selector(selector, place)
    copies[1].wait()
    copies[2].wait()
    x, s = primal[...], slacks[...]
    scaling = x / s
    inverse = 1.0 / s
    gap = jnp.sum(x * s, axis=1, keepdims=True)
    owner = jnp.where((start >> 8) == (end >> 8), block[:, :half], -1)
    shift = (SLOTS * lax.rem(source, 128 // SLOTS)).astype(f32)
    packed, most = buckets(
        owner, [place[:, :half].astype(f32), place[:, half:].astype(f32), *split3(scaling)], shift
    )
    (ends_sum,) = to_buses([jnp.concatenate([scaling, scaling], axis=1)], block, selector)
    whole = jnp.concatenate(
        [ends_sum, packed[0], packed[1], packed[2] + packed[3] + packed[4], jnp.broadcast_to(gap, (PLANE, 128))],
        axis=1,
    )
    for b in range(PLANE):
        msg[b] = whole[b : b + 1]
    for copy in copies[3:]:
        copy.wait()

    greeted()
    pair = pltpu.make_async_remote_copy(
        bus_dual, partner, pair_sem.at[0], pair_sem.at[1], device_id=(li, 2 * z + 1 - c), device_id_type=MESH
    )
    pair.start()
    send_plane(lambda b: msg.at[b], msg.at[at_home], source, msg_in, msg_sem, li, z, c)

    pair.wait()
    mine_dual = jnp.concatenate([bus_dual[:, BS * k : BS * (k + 1)] for k in range(16)], axis=0)
    other_dual = jnp.concatenate([partner[:, BS * k : BS * (k + 1)] for k in range(16)], axis=0)
    table = jnp.concatenate(
        [jnp.where(c == 0, mine_dual, other_dual), jnp.where(c == 0, other_dual, mine_dual)], axis=0
    )
    diff0[:, :half] = to_lines(table, block, selector)
    diff0[:, half:] = jnp.broadcast_to(most, (1, 128))
    send_depth(diff0, diff0_in, diff0_sem, li, z, c)

    wait_bytes(msg_in, msg_sem.at[1])
    sums = sum_slots(msg_in, slice(0, 256))
    gap0 = sum_slots(msg_in, slice(640, 768))[:, 0:1]
    own.wait()
    if given:
        work[...] = block_in[...]
    else:
        diagonal = rows_of((BS, BS)) == lax.broadcasted_iota(jnp.int32, (BS, BS), 1)
        work[...] = block_in[...] + jnp.where(diagonal, sums, 0.0) - bucket_lines(msg_in)

    def first_right_side(panel):
        if panel != 1:
            return
        wait_bytes(diff0_in, diff0_sem.at[1])
        residual = cost[...] - sum_slots(diff0_in, slice(0, half)) - s
        dual_res[...] = residual
        most = diff0_in[0, :, half:]
        for k in range(1, DEPTH):
            most = jnp.maximum(most, diff0_in[k, :, half:])
        flow = scaling * residual
        sums = to_buses(
            [jnp.concatenate([flow, -flow], axis=1), jnp.concatenate([inverse, -inverse], axis=1)], block, selector
        )
        whole = jnp.concatenate([*sums, jnp.broadcast_to(most, (PLANE, 128))], axis=1)
        for b in range(PLANE):
            part0[b] = whole[b : b + 1]
        send_plane(lambda b: part0.at[b], part0.at[at_home], source, part0_in, part0_sem, li, z, c)

    invert(work, first_right_side)
    wait_bytes(part0_in, part0_sem.at[1])
    sums = sum_slots(part0_in, slice(0, 512))
    right, third = demand[...] + sums[:, :256], sums[:, 256:]

    def solve(vector):
        wide = jnp.broadcast_to(vector, (8, BS))
        return jnp.dot(wide, work[...], precision=lax.Precision.HIGHEST, preferred_element_type=f32)[0:1]

    solved[...] = solve(right)
    send_plane(lambda b: solved, solved, at_home, solved_in, solved_sem, li, z, c)
    wait_bytes(solved_in, solved_sem.at[1])
    table = jnp.concatenate([solved_in[b] for b in range(PLANE)], axis=0)
    diff[...] = to_lines(table, block, selector)
    send_depth(diff, diff_in, diff_sem, li, z, c)
    wait_bytes(diff_in, diff_sem.at[1])
    affine_slack = dual_res[...] - sum_slots(diff_in, slice(0, half))
    affine_primal = -x - scaling * affine_slack
    cross = affine_primal * affine_slack
    extra = cross / s
    (sums,) = to_buses([jnp.concatenate([extra, -extra], axis=1)], block, selector)
    scalars = [
        longest_step(x, affine_primal),
        longest_step(s, affine_slack),
        jnp.sum(affine_primal * s, axis=1, keepdims=True),
        jnp.sum(x * affine_slack, axis=1, keepdims=True),
        jnp.sum(cross, axis=1, keepdims=True),
    ]
    row = jnp.zeros((1, 128), f32)
    for k, value in enumerate(scalars):
        row = jnp.where(lane1 == k, value, row)
    whole = jnp.concatenate([sums, jnp.broadcast_to(row, (PLANE, 128))], axis=1)
    for b in range(PLANE):
        part[b] = whole[b : b + 1]
    send_plane(lambda b: part.at[b], part.at[at_home], source, part_in, part_sem, li, z, c)
    wait_bytes(part_in, part_sem.at[1])

    added = sum_slots(part_in, slice(0, 384))
    least = part_in[0, :, 256:384]
    for k in range(1, PLANE):
        least = jnp.minimum(least, part_in[k, :, 256:384])
    take_p, take_d = least[:, 0:1], least[:, 1:2]
    tail = added[:, 256:384]
    gap_affine = gap0 + take_p * tail[:, 2:3] + take_d * tail[:, 3:4] + take_p * take_d * tail[:, 4:5]
    ratio = gap_affine / gap0
    aim = ratio * ratio * ratio * (gap0 / total_lines)
    solved2[...] = solve(right - aim * third + added[:, :256])
    send_plane(lambda b: solved2, solved2, at_home, solved2_in, solved2_sem, li, z, c)
    wait_bytes(solved2_in, solved2_sem.at[1])
    table = jnp.concatenate([solved2_in[b] for b in range(PLANE)], axis=0)
    diff2[...] = to_lines(table, block, selector)
    send_depth(diff2, diff2_in, diff2_sem, li, z, c)
    for b in range(16):
        step_dual[:, BS * b : BS * (b + 1)] = solved2_in[16 * c + b]
    wait_bytes(diff2_in, diff2_sem.at[1])
    slack = dual_res[...] - sum_slots(diff2_in, slice(0, half))
    primal_step = (aim - x * s - cross) / s - scaling * slack
    last[...] = jnp.where(lane1 == 0, longest_step(x, primal_step), longest_step(s, slack))
    final[0:1] = primal_step
    final[1:2] = slack
    send_plane(lambda b: last, last, source, last_in, last_sem, li, z, c)
    pair2 = pltpu.make_async_remote_copy(
        final, final_in, final_sem.at[0], final_sem.at[1], device_id=(li, 2 * z + 1 - c), device_id_type=MESH
    )
    pair2.start()
    step_primal[:, mine] = primal_step
    step_slack[:, mine] = slack
    most = part0_in[0, :, 512:]
    for k in range(1, PLANE):
        most = jnp.maximum(most, part0_in[k, :, 512:])
    fullest[...] = most[:, 0:1]
    pair2.wait()
    other = pl.ds(pl.multiple_of((1 - c) * half, half), half)
    step_primal[:, other] = final_in[0:1]
    step_slack[:, other] = final_in[1:2]
    for recv, sems in (
        (msg_in, msg_sem), (diff0_in, diff0_sem), (part0_in, part0_sem), (solved_in, solved_sem), (diff_in, diff_sem),
        (part_in, part_sem), (solved2_in, solved2_sem), (diff2_in, diff2_sem), (last_in, last_sem),
    ):
        wait_bytes(recv.at[pl.ds(0, recv.shape[0] - 1)], sems.at[0])
    wait_bytes(last_in, last_sem.at[1])
    least = last_in[0]
    for k in range(1, PLANE):
        least = jnp.minimum(least, last_in[k])
    lengths[...] = damping * least


def vmem(n):
    return [pl.BlockSpec(memory_space=pltpu.VMEM)] * n


def struct(*shape):
    return jax.ShapeDtypeStruct(shape, f32)


def scattered_block(primal, slacks, endpoints, fixed_part):
    blocks_here, block_size = fixed_part.shape[0], fixed_part.shape[1]
    buses_here = blocks_here * block_size
    scaling = primal / slacks
    local = endpoints - lax.axis_index("bus") * buses_here
    own_from, own_to = jnp.where((local >= 0) & (local < buses_here), local, buses_here)
    same_block = endpoints[0] // block_size == endpoints[1] // block_size
    crossing = jnp.where(same_block, -scaling, jnp.zeros_like(scaling))
    rows = jnp.concatenate([own_from, own_to, own_from, own_to])
    columns = jnp.concatenate([own_from, own_to, own_to, own_from]) % block_size
    values = jnp.concatenate([scaling, scaling, crossing, crossing])
    flat = jnp.zeros((buses_here * block_size,), f32).at[rows * block_size + columns].add(values, mode="drop")
    tiles = lax.all_to_all(flat.reshape(blocks_here, block_size, block_size), "line", 0, 0, tiled=True)
    mine = lax.dynamic_index_in_dim(fixed_part, lax.axis_index("line"), 0, keepdims=False)
    return mine + jnp.sum(tiles, axis=0)


def hand_over(step_primal, step_slack, step_dual, lengths, primal_out, slack_out, dual_out, lengths_out):
    primal_out[...] = step_primal[...]
    slack_out[...] = step_slack[...]
    dual_out[...] = step_dual[...]
    lengths_out[...] = lengths[:, 0:2]


def whole_step(given, args, normal):
    x, s, cost, ends, bus_dual, demand = args
    lines_here, buses_here = x.shape[1], bus_dual.shape[1]
    half = lines_here // 2
    total_lines = float(lines_here * lax.axis_size("line"))
    dma = pltpu.SemaphoreType.DMA
    exchange = lambda slots, width: [pltpu.VMEM((1, width), f32), pltpu.VMEM((slots, 1, width), f32)]
    buckets_of = lambda width: [pltpu.VMEM((PLANE, 1, width), f32)] * 2
    return pl.pallas_call(
        functools.partial(step_kernel, total_lines, given),
        out_shape=(struct(1, lines_here), struct(1, lines_here), struct(1, buses_here), struct(1, 128), struct(1, 1)),
        in_specs=[pl.BlockSpec(memory_space=pl.ANY)] * 7,
        out_specs=tuple(vmem(5)),
        scratch_shapes=[pltpu.VMEM((1, half), f32)] * 3
        + [pltpu.VMEM((2, half), jnp.int32), pltpu.VMEM((1, buses_here), f32), pltpu.VMEM((1, BS), f32)]
        + [pltpu.VMEM((BS, lines_here), bf16), pltpu.VMEM((1, buses_here), f32)]
        + buckets_of(768)
        + exchange(DEPTH, half + 128)
        + buckets_of(640)
        + [pltpu.VMEM((BS, BS), f32)] * 2
        + [pltpu.VMEM((1, half), f32)]
        + exchange(PLANE, BS)
        + exchange(DEPTH, half)
        + buckets_of(384)
        + exchange(PLANE, BS)
        + exchange(DEPTH, half)
        + [pltpu.VMEM((2, half), f32)] * 2
        + exchange(PLANE, 128)
        + [dma((6,)), dma]
        + [dma((2,))] * 11,
        compiler_params=pltpu.CompilerParams(collective_id=int(given), has_side_effects=True),
        name="step_given" if given else "step",
    )(*args, normal)


def per_device(primal, slacks, line_cost, bus_dual, demand, endpoints, fixed_part):
    args = tuple(a.reshape(1, -1) for a in (primal, slacks, line_cost))
    args += (endpoints, bus_dual.reshape(1, -1), demand.reshape(1, -1))
    def again(steps):
        normal = scattered_block(primal, slacks, endpoints, fixed_part)
        *steps, fullest = whole_step(True, args, normal)
        return (*steps, jnp.zeros_like(fullest))

    *steps, _ = lax.while_loop(lambda steps: steps[-1][0, 0] > SLOTS, again, tuple(whole_step(False, args, fixed_part)))
    outputs = pl.pallas_call(
        hand_over,
        out_shape=tuple(struct(*a.shape) for a in steps[:3]) + (struct(1, 2),),
        in_specs=vmem(4),
        out_specs=tuple(vmem(4)),
        name="hand_over",
    )(*steps)
    return tuple(a.reshape(-1) for a in outputs)


def solution(mesh):
    in_specs = (P("line"), P("line"), P("line"), P("bus"), P("bus"), P(None, "line"), P("bus", None, None))
    out_specs = (P("line"), P("line"), P("bus"), P())
    return jax.shard_map(per_device, mesh=mesh, in_specs=in_specs, out_specs=out_specs, check_vma=False)
```

```python
import functools

import jax
import jax.numpy as jnp
from jax import lax
from jax.experimental import pallas as pl
from jax.experimental.pallas import tpu as pltpu
from jax.sharding import PartitionSpec as P

damping = 0.99

f32 = jnp.float32
bf16 = jnp.bfloat16
MESH = pl.DeviceIdType.MESH

BS = 256
PLANE = 32
DEPTH = 8
SLOTS = 20
CHUNK = 512


def position():
    li = lax.axis_index("line")
    bi = lax.axis_index("bus")
    z = bi // 2
    c = bi - 2 * z
    return li, z, c


def split3(x):
    high = x.astype(bf16).astype(f32)
    rest = x - high
    middle = rest.astype(bf16).astype(f32)
    return high, middle, rest - middle


def multiply(a, b):
    return jnp.dot(a, b, preferred_element_type=f32)


def rows_of(shape):
    return lax.broadcasted_iota(jnp.int32, shape, 0)


def lanes_of(shape):
    return lax.broadcasted_iota(jnp.int32, shape, 1)


def build_selector(selector, place):
    for j in range(place.shape[1] // 256):
        at = slice(256 * j, 256 * (j + 1))
        selector[:, at] = jnp.where(rows_of((BS, 256)) == place[:, at], 1.0, 0.0).astype(bf16)


def one_hot_rows(row, width):
    diagonal = jnp.where(rows_of((128, 128)) == lanes_of((128, 128)), row, 0.0).astype(bf16)
    value = multiply(diagonal, jnp.ones((128, width), bf16))
    return jnp.where(value == lanes_of((128, width)).astype(f32), 1.0, 0.0).astype(bf16)


def build_line_selector(selector, place):
    for j in range(place.shape[1] // 128):
        at = slice(128 * j, 128 * (j + 1))
        selector[at, :] = one_hot_rows(place[:, at].astype(f32), BS)


def to_buses(values, block, line_selector):
    total = None
    pieces = [piece for v in values for piece in split3(v)]
    for j in range(block.shape[1] // CHUNK):
        at = slice(CHUNK * j, CHUNK * (j + 1))
        here = rows_of((PLANE, CHUNK)) == block[:, at]
        left = jnp.concatenate([jnp.where(here, p[:, at], 0.0).astype(bf16) for p in pieces], axis=0)
        part = multiply(left, line_selector[at, :])
        total = part if total is None else total + part
    sums = [total[PLANE * k : PLANE * (k + 1)] for k in range(len(pieces))]
    return [sums[3 * q] + sums[3 * q + 1] + sums[3 * q + 2] for q in range(len(values))]


def to_lines(table, block, selector):
    left = jnp.concatenate([p.astype(bf16) for p in split3(table)], axis=0)
    picked = []
    for j in range(block.shape[1] // CHUNK):
        at = slice(CHUNK * j, CHUNK * (j + 1))
        found = jnp.dot(left, selector[:, at], preferred_element_type=f32)
        found = found[0:PLANE] + found[PLANE : 2 * PLANE] + found[2 * PLANE : 3 * PLANE]
        here = rows_of((PLANE, CHUNK)) == block[:, at]
        picked.append(jnp.sum(jnp.where(here, found, 0.0), axis=0, keepdims=True))
    half = len(picked) // 2
    return jnp.concatenate(picked[:half], axis=1) - jnp.concatenate(picked[half:], axis=1)


def endpoint_rows(ends, z):
    start, end = ends[0:1, :], ends[1:2, :]
    both = jnp.concatenate([start, end], axis=1)
    return start, end, both & (BS - 1), (both >> 8) - PLANE * z


def plane_peers(li, z, c):
    y, x = li // 4, lax.rem(li, 4)
    ys = [lax.rem(y + d, 4) for d in range(4)]
    xs = [lax.rem(x + d, 4) for d in range(4)]
    cs = [c, 1 - c]
    reach = [0, 1, 2, 1]
    offsets = [(dy, dx, dc) for dy in range(4) for dx in range(4) for dc in range(2)]
    offsets.sort(key=lambda o: -reach[o[0]] - reach[o[1]])
    peers = []
    for dy, dx, dc in offsets[:-2] + [(0, 0, 1)]:
        l2, c2 = ys[dy] * 4 + xs[dx], cs[dc]
        peers.append((c2 * 16 + l2, (l2, 2 * z + c2)))
    return peers


def depth_peers(li, z, c):
    return [(li, 2 * lax.rem(z + d, DEPTH) + c) for d in (4, 3, 5, 2, 6, 1, 7)]


def greet(li, z, c):
    barrier = pltpu.get_barrier_semaphore()
    for device in [device for _, device in plane_peers(li, z, c)] + depth_peers(li, z, c):
        pl.semaphore_signal(barrier, 1, device_id=device, device_id_type=MESH)


def greeted():
    pl.semaphore_wait(pltpu.get_barrier_semaphore(), PLANE - 1 + DEPTH - 1)


def send_plane(pick, home, slot, recv, sems, li, z, c):
    for place, device in plane_peers(li, z, c):
        pltpu.make_async_remote_copy(
            pick(place), recv.at[slot], sems.at[0], sems.at[1], device_id=device, device_id_type=MESH
        ).start()
    pltpu.make_async_copy(home, recv.at[slot], sems.at[1]).start()


def send_depth(src, recv, sems, li, z, c):
    for device in depth_peers(li, z, c):
        pltpu.make_async_remote_copy(
            src, recv.at[z], sems.at[0], sems.at[1], device_id=device, device_id_type=MESH
        ).start()
    pltpu.make_async_copy(src, recv.at[z], sems.at[1]).start()


def wait_bytes(ref, sem):
    pltpu.make_async_copy(ref, ref, sem).wait()


def sum_slots(recv, at):
    total = recv[0, :, at]
    for s in range(1, recv.shape[0]):
        total = total + recv[s, :, at]
    return total


def eliminate(pa, pb, off):
    groups = len(pa)
    lane, row = lax.broadcasted_iota(jnp.int32, (8, 128), 1), rows_of((8, 128))

    def spread(sub):
        first = off + 8 * sub
        return [[jnp.broadcast_to(p[:, j : j + 1], (8, 128)) for p in pa] for j in range(first, first + 8)]

    columns, ahead = spread(0), None
    for sub in range(groups):
        first = off + 8 * sub
        inside = (lane >= first) & (lane < first + 8)
        unit = jnp.where(lane - first == row, 1.0, 0.0)
        pa = [jnp.where(inside, unit if g == sub else 0.0, pa[g]) for g in range(groups)]
        for k in range(8):
            if k == 3 and sub + 1 < groups:
                ahead = spread(sub + 1)
            pivot = columns[k]
            scale = 1.0 / pivot[sub][k : k + 1]
            here = row == k

            def swept(rows):
                top = rows[sub][k : k + 1] * scale
                rest = [rows[g] - pivot[g] * top for g in range(groups)]
                rest[sub] = jnp.where(here, top, rest[sub])
                return rest

            columns = columns[: k + 1] + [swept(c) for c in columns[k + 1 :]]
            if ahead is not None:
                ahead = [swept(c) for c in ahead]
            pa, pb = swept(pa), swept(pb)
        columns, ahead = ahead, None
    return pa, pb


def invert(work, between):
    n, w = work.shape[0], 32
    now = work[0:w, :]
    for i in range(n // w):
        slab, off = divmod(w * i, 128)
        a = slice(128 * slab, 128 * slab + 128)
        b = slice(128 - 128 * slab, 256 - 128 * slab)
        groups = range(0, w, 8)
        pa, pb = eliminate([now[g : g + 8, a] for g in groups], [now[g : g + 8, b] for g in groups], off)
        pa, pb = jnp.concatenate(pa, axis=0), jnp.concatenate(pb, axis=0)
        top = jnp.concatenate([pa, pb] if slab == 0 else [pb, pa], axis=1)
        parts = [jnp.zeros((off, n), f32)] * (off > 0) + [top]
        parts += [jnp.zeros((128 - w - off, n), f32)] * (off + w < 128)
        wide = jnp.concatenate(parts, axis=0)

        def take(rows):
            lanes = lax.broadcasted_iota(jnp.int32, rows.shape, 1)
            kept = jnp.where((lanes >= w * i) & (lanes < w * i + w), 0.0, rows)
            return kept - jnp.dot(rows[:, a], wide, precision=lax.Precision.HIGHEST, preferred_element_type=f32)

        low, high = w * i, w * i + w
        work[low:high, :] = top
        if high < n:
            now = take(work[high : high + w, :])
        if high + w < n:
            work[high + w : n, :] = take(work[high + w : n, :])
        if low > 0:
            work[0:low, :] = take(work[0:low, :])
        between(i)


def longest_step(now, step):
    return jnp.min(now / jnp.maximum(-step, now), axis=1, keepdims=True)


def buckets(owner, values, shift):
    order = jnp.where(rows_of((256, 256)) < lax.broadcasted_iota(jnp.int32, (256, 256), 1), 1.0, 0.0).astype(bf16)
    carry = jnp.zeros((PLANE, 1), f32)
    packed = None
    for j in range(owner.shape[1] // 256):
        at = slice(256 * j, 256 * (j + 1))
        here = rows_of((PLANE, 256)) == owner[:, at]
        marks = jnp.where(here, 1.0, 0.0)
        rank = jnp.dot(marks.astype(bf16), order, preferred_element_type=f32) + carry
        carry = carry + jnp.sum(marks, axis=1, keepdims=True)
        rank = jnp.sum(jnp.where(here, rank, 0.0), axis=0, keepdims=True)
        code = jnp.where(rank < SLOTS, rank + shift, -1.0)
        slots = jnp.where(rows_of((128, 256)).astype(f32) == code, 1.0, 0.0).astype(bf16)
        left = jnp.concatenate([jnp.where(here, v[:, at], 0.0).astype(bf16) for v in values], axis=0)
        piece = lax.dot_general(left, slots, (((1,), (1,)), ((), ())), preferred_element_type=f32)
        packed = piece if packed is None else packed + piece
    packed = [packed[PLANE * k : PLANE * (k + 1)] for k in range(len(values))]
    return packed, jnp.max(carry, axis=0, keepdims=True)


def bucket_lines(msg_in):
    group = 128 // SLOTS
    near = rows_of((BS, 128)).astype(f32)
    sides = []
    for first in range(0, PLANE, group):
        rows = msg_in[first, :, 256:640]
        for k in range(first + 1, min(first + group, PLANE)):
            rows = rows + msg_in[k, :, 256:640]
        p, q, d = rows[:, 0:128], rows[:, 128:256], rows[:, 256:384]
        here = near == p
        left = [jnp.where(here, piece, 0.0).astype(bf16) for piece in split3(d)]
        sides.append((left, one_hot_rows(q, BS)))
    total = None
    for g in range(0, len(sides), 2):
        right = jnp.concatenate([side[1] for side in sides[g : g + 2]], axis=0)
        for k in range(3):
            add = multiply(jnp.concatenate([side[0][k] for side in sides[g : g + 2]], axis=1), right)
            total = add if total is None else total + add
    return total + total.T


def step_kernel(
    total_lines, given,
    primal_all, slacks_all, cost_all, ends_all, bus_dual_all, demand_all, normal,
    step_primal, step_slack, step_dual, lengths, fullest,
    primal, slacks, cost, ends, bus_dual, demand, selector, line_selector, partner, msg, msg_in, diff0, diff0_in, part0, part0_in, block_in, work, dual_res, split,
    solved, solved_in, diff, diff_in, part, part_in, solved2, solved2_in, diff2, diff2_in, final, final_in, last, last_in,
    in_sem, fixed_sem, pair_sem, msg_sem, diff0_sem, part0_sem,
    solved_sem, diff_sem, part_sem, solved2_sem, diff2_sem, last_sem, final_sem,
):
    li, z, c = position()
    greet(li, z, c)
    half = primal.shape[1]
    mine = pl.ds(pl.multiple_of(c * half, half), half)
    own_buses = pl.ds(pl.multiple_of(li * BS, BS), BS)
    copies = [
        pltpu.make_async_copy(src, dst, in_sem.at[k])
        for k, (src, dst) in enumerate(
            (
                (ends_all.at[:, mine], ends),
                (primal_all.at[:, mine], primal),
                (slacks_all.at[:, mine], slacks),
                (bus_dual_all, bus_dual),
                (cost_all.at[:, mine], cost),
                (demand_all.at[:, own_buses], demand),
            )
        )
    ]
    for copy in copies:
        copy.start()
    own = pltpu.make_async_copy(normal if given else normal.at[li], block_in, fixed_sem)
    own.start()
    at_home = c * 16 + li
    source = 2 * li + c
    lane1 = lax.broadcasted_iota(jnp.int32, (1, 128), 1)
    copies[0].wait()
    start, end, place, block = endpoint_rows(ends, z)
    build_line_selector(line_selector, place)
    copies[1].wait()
    copies[2].wait()
    x, s = primal[...], slacks[...]
    scaling = x / s
    inverse = 1.0 / s
    gap = jnp.sum(x * s, axis=1, keepdims=True)
    owner = jnp.where((start >> 8) == (end >> 8), block[:, :half], -1)
    shift = (SLOTS * lax.rem(source, 128 // SLOTS)).astype(f32)
    packed, most = buckets(
        owner, [place[:, :half].astype(f32), place[:, half:].astype(f32), *split3(scaling)], shift
    )
    (ends_sum,) = to_buses([jnp.concatenate([scaling, scaling], axis=1)], block, line_selector)
    whole = jnp.concatenate(
        [ends_sum, packed[0], packed[1], packed[2] + packed[3] + packed[4], jnp.broadcast_to(gap, (PLANE, 128))],
        axis=1,
    )
    for b in range(PLANE):
        msg[b] = whole[b : b + 1]
    for copy in copies[3:]:
        copy.wait()

    greeted()
    pair = pltpu.make_async_remote_copy(
        bus_dual, partner, pair_sem.at[0], pair_sem.at[1], device_id=(li, 2 * z + 1 - c), device_id_type=MESH
    )
    pair.start()
    send_plane(lambda b: msg.at[b], msg.at[at_home], source, msg_in, msg_sem, li, z, c)

    build_selector(selector, place)
    pair.wait()
    mine_dual = jnp.concatenate([bus_dual[:, BS * k : BS * (k + 1)] for k in range(16)], axis=0)
    other_dual = jnp.concatenate([partner[:, BS * k : BS * (k + 1)] for k in range(16)], axis=0)
    table = jnp.concatenate(
        [jnp.where(c == 0, mine_dual, other_dual), jnp.where(c == 0, other_dual, mine_dual)], axis=0
    )
    diff0[:, :half] = to_lines(table, block, selector)
    diff0[:, half:] = jnp.broadcast_to(most, (1, 128))
    send_depth(diff0, diff0_in, diff0_sem, li, z, c)

    (sums,) = to_buses([jnp.concatenate([inverse, -inverse], axis=1)], block, line_selector)
    for b in range(PLANE):
        part0[b, :, 256:512] = sums[b : b + 1]
    wait_bytes(msg_in, msg_sem.at[1])
    sums = sum_slots(msg_in, slice(0, 256))
    gap0 = sum_slots(msg_in, slice(640, 768))[:, 0:1]
    own.wait()
    if given:
        work[...] = block_in[...]
    else:
        diagonal = rows_of((BS, BS)) == lax.broadcasted_iota(jnp.int32, (BS, BS), 1)
        work[...] = block_in[...] + jnp.where(diagonal, sums, 0.0) - bucket_lines(msg_in)

    def first_right_side(panel):
        if panel != 1:
            return
        wait_bytes(diff0_in, diff0_sem.at[1])
        residual = cost[...] - sum_slots(diff0_in, slice(0, half)) - s
        dual_res[...] = residual
        most = diff0_in[0, :, half:]
        for k in range(1, DEPTH):
            most = jnp.maximum(most, diff0_in[k, :, half:])
        flow = scaling * residual
        (sums,) = to_buses([jnp.concatenate([flow, -flow], axis=1)], block, line_selector)
        for b in range(PLANE):
            part0[b, :, 0:256] = sums[b : b + 1]
            part0[b, :, 512:640] = most
        send_plane(lambda b: part0.at[b], part0.at[at_home], source, part0_in, part0_sem, li, z, c)

    invert(work, first_right_side)
    wait_bytes(part0_in, part0_sem.at[1])
    sums = sum_slots(part0_in, slice(0, 512))
    right, third = demand[...] + sums[:, :256], sums[:, 256:]

    def solve(vector):
        wide = jnp.broadcast_to(vector, (8, BS))
        return jnp.dot(wide, work[...], precision=lax.Precision.HIGHEST, preferred_element_type=f32)[0:1]

    solved[...] = solve(right)
    send_plane(lambda b: solved, solved, at_home, solved_in, solved_sem, li, z, c)
    for k, piece in enumerate(split3(work[...])):
        split[k] = piece.astype(bf16)
    wait_bytes(solved_in, solved_sem.at[1])
    table = jnp.concatenate([solved_in[b] for b in range(PLANE)], axis=0)
    diff[...] = to_lines(table, block, selector)
    send_depth(diff, diff_in, diff_sem, li, z, c)
    wait_bytes(diff_in, diff_sem.at[1])
    affine_slack = dual_res[...] - sum_slots(diff_in, slice(0, half))
    affine_primal = -x - scaling * affine_slack
    cross = affine_primal * affine_slack
    extra = cross / s
    (sums,) = to_buses([jnp.concatenate([extra, -extra], axis=1)], block, line_selector)
    scalars = [
        longest_step(x, affine_primal),
        longest_step(s, affine_slack),
        jnp.sum(affine_primal * s, axis=1, keepdims=True),
        jnp.sum(x * affine_slack, axis=1, keepdims=True),
        jnp.sum(cross, axis=1, keepdims=True),
    ]
    row = jnp.zeros((1, 128), f32)
    for k, value in enumerate(scalars):
        row = jnp.where(lane1 == k, value, row)
    whole = jnp.concatenate([sums, jnp.broadcast_to(row, (PLANE, 128))], axis=1)
    for b in range(PLANE):
        part[b] = whole[b : b + 1]
    send_plane(lambda b: part.at[b], part.at[at_home], source, part_in, part_sem, li, z, c)
    wait_bytes(part_in, part_sem.at[1])

    added = sum_slots(part_in, slice(0, 384))
    least = part_in[0, :, 256:384]
    for k in range(1, PLANE):
        least = jnp.minimum(least, part_in[k, :, 256:384])
    take_p, take_d = least[:, 0:1], least[:, 1:2]
    tail = added[:, 256:384]
    gap_affine = gap0 + take_p * tail[:, 2:3] + take_d * tail[:, 3:4] + take_p * take_d * tail[:, 4:5]
    ratio = gap_affine / gap0
    aim = ratio * ratio * ratio * (gap0 / total_lines)
    right = right - aim * third + added[:, :256]
    high, middle, low = split3(jnp.broadcast_to(right, (8, BS)))
    three = jnp.concatenate([high, middle, low], axis=0).astype(bf16)
    by_high, by_middle, by_low = multiply(three, split[0]), multiply(three[0:16], split[1]), multiply(three[0:8], split[2])
    solved2[...] = (
        by_high[0:1] + (by_high[8:9] + by_middle[0:1]) + (by_high[16:17] + by_middle[8:9] + by_low[0:1])
    )
    send_plane(lambda b: solved2, solved2, at_home, solved2_in, solved2_sem, li, z, c)
    wait_bytes(solved2_in, solved2_sem.at[1])
    table = jnp.concatenate([solved2_in[b] for b in range(PLANE)], axis=0)
    diff2[...] = to_lines(table, block, selector)
    send_depth(diff2, diff2_in, diff2_sem, li, z, c)
    for b in range(16):
        step_dual[:, BS * b : BS * (b + 1)] = solved2_in[16 * c + b]
    wait_bytes(diff2_in, diff2_sem.at[1])
    slack = dual_res[...] - sum_slots(diff2_in, slice(0, half))
    primal_step = (aim - x * s - cross) / s - scaling * slack
    last[...] = jnp.where(lane1 == 0, longest_step(x, primal_step), longest_step(s, slack))
    final[0:1] = primal_step
    final[1:2] = slack
    send_plane(lambda b: last, last, source, last_in, last_sem, li, z, c)
    pair2 = pltpu.make_async_remote_copy(
        final, final_in, final_sem.at[0], final_sem.at[1], device_id=(li, 2 * z + 1 - c), device_id_type=MESH
    )
    pair2.start()
    step_primal[:, mine] = primal_step
    step_slack[:, mine] = slack
    most = part0_in[0, :, 512:]
    for k in range(1, PLANE):
        most = jnp.maximum(most, part0_in[k, :, 512:])
    fullest[...] = most[:, 0:1]
    pair2.wait()
    other = pl.ds(pl.multiple_of((1 - c) * half, half), half)
    step_primal[:, other] = final_in[0:1]
    step_slack[:, other] = final_in[1:2]
    for recv, sems in (
        (msg_in, msg_sem), (diff0_in, diff0_sem), (part0_in, part0_sem), (solved_in, solved_sem), (diff_in, diff_sem),
        (part_in, part_sem), (solved2_in, solved2_sem), (diff2_in, diff2_sem), (last_in, last_sem),
    ):
        wait_bytes(recv.at[pl.ds(0, recv.shape[0] - 1)], sems.at[0])
    wait_bytes(last_in, last_sem.at[1])
    least = last_in[0]
    for k in range(1, PLANE):
        least = jnp.minimum(least, last_in[k])
    lengths[...] = damping * least


def vmem(n):
    return [pl.BlockSpec(memory_space=pltpu.VMEM)] * n


def struct(*shape):
    return jax.ShapeDtypeStruct(shape, f32)


def scattered_block(primal, slacks, endpoints, fixed_part):
    blocks_here, block_size = fixed_part.shape[0], fixed_part.shape[1]
    buses_here = blocks_here * block_size
    scaling = primal / slacks
    local = endpoints - lax.axis_index("bus") * buses_here
    own_from, own_to = jnp.where((local >= 0) & (local < buses_here), local, buses_here)
    same_block = endpoints[0] // block_size == endpoints[1] // block_size
    crossing = jnp.where(same_block, -scaling, jnp.zeros_like(scaling))
    rows = jnp.concatenate([own_from, own_to, own_from, own_to])
    columns = jnp.concatenate([own_from, own_to, own_to, own_from]) % block_size
    values = jnp.concatenate([scaling, scaling, crossing, crossing])
    flat = jnp.zeros((buses_here * block_size,), f32).at[rows * block_size + columns].add(values, mode="drop")
    tiles = lax.all_to_all(flat.reshape(blocks_here, block_size, block_size), "line", 0, 0, tiled=True)
    mine = lax.dynamic_index_in_dim(fixed_part, lax.axis_index("line"), 0, keepdims=False)
    return mine + jnp.sum(tiles, axis=0)


def hand_over(step_primal, step_slack, step_dual, lengths, primal_out, slack_out, dual_out, lengths_out):
    primal_out[...] = step_primal[...]
    slack_out[...] = step_slack[...]
    dual_out[...] = step_dual[...]
    lengths_out[...] = lengths[:, 0:2]


def whole_step(given, args, normal):
    x, s, cost, ends, bus_dual, demand = args
    lines_here, buses_here = x.shape[1], bus_dual.shape[1]
    half = lines_here // 2
    total_lines = float(lines_here * lax.axis_size("line"))
    dma = pltpu.SemaphoreType.DMA
    exchange = lambda slots, width: [pltpu.VMEM((1, width), f32), pltpu.VMEM((slots, 1, width), f32)]
    buckets_of = lambda width: [pltpu.VMEM((PLANE, 1, width), f32)] * 2
    return pl.pallas_call(
        functools.partial(step_kernel, total_lines, given),
        out_shape=(struct(1, lines_here), struct(1, lines_here), struct(1, buses_here), struct(1, 128), struct(1, 1)),
        in_specs=[pl.BlockSpec(memory_space=pl.ANY)] * 7,
        out_specs=tuple(vmem(5)),
        scratch_shapes=[pltpu.VMEM((1, half), f32)] * 3
        + [pltpu.VMEM((2, half), jnp.int32), pltpu.VMEM((1, buses_here), f32), pltpu.VMEM((1, BS), f32)]
        + [pltpu.VMEM((BS, lines_here), bf16), pltpu.VMEM((lines_here, BS), bf16), pltpu.VMEM((1, buses_here), f32)]
        + buckets_of(768)
        + exchange(DEPTH, half + 128)
        + buckets_of(640)
        + [pltpu.VMEM((BS, BS), f32)] * 2
        + [pltpu.VMEM((1, half), f32), pltpu.VMEM((3, BS, BS), bf16)]
        + exchange(PLANE, BS)
        + exchange(DEPTH, half)
        + buckets_of(384)
        + exchange(PLANE, BS)
        + exchange(DEPTH, half)
        + [pltpu.VMEM((2, half), f32)] * 2
        + exchange(PLANE, 128)
        + [dma((6,)), dma]
        + [dma((2,))] * 11,
        compiler_params=pltpu.CompilerParams(collective_id=int(given), has_side_effects=True),
        name="step_given" if given else "step",
    )(*args, normal)


def per_device(primal, slacks, line_cost, bus_dual, demand, endpoints, fixed_part):
    args = tuple(a.reshape(1, -1) for a in (primal, slacks, line_cost))
    args += (endpoints, bus_dual.reshape(1, -1), demand.reshape(1, -1))
    def again(steps):
        normal = scattered_block(primal, slacks, endpoints, fixed_part)
        *steps, fullest = whole_step(True, args, normal)
        return (*steps, jnp.zeros_like(fullest))

    *steps, _ = lax.while_loop(lambda steps: steps[-1][0, 0] > SLOTS, again, tuple(whole_step(False, args, fixed_part)))
    outputs = pl.pallas_call(
        hand_over,
        out_shape=tuple(struct(*a.shape) for a in steps[:3]) + (struct(1, 2),),
        in_specs=vmem(4),
        out_specs=tuple(vmem(4)),
        name="hand_over",
    )(*steps)
    return tuple(a.reshape(-1) for a in outputs)


def solution(mesh):
    in_specs = (P("line"), P("line"), P("line"), P("bus"), P("bus"), P(None, "line"), P("bus", None, None))
    out_specs = (P("line"), P("line"), P("bus"), P())
    return jax.shard_map(per_device, mesh=mesh, in_specs=in_specs, out_specs=out_specs, check_vma=False)
```

```python
import functools

import jax
import jax.numpy as jnp
from jax import lax
from jax.experimental import pallas as pl
from jax.experimental.pallas import tpu as pltpu
from jax.sharding import PartitionSpec as P

damping = 0.99

f32 = jnp.float32
bf16 = jnp.bfloat16
MESH = pl.DeviceIdType.MESH

BS = 256
PLANE = 32
DEPTH = 8
LANE_STEP = 42
SLOTS = 20
CHUNK = 512


def position():
    li = lax.axis_index("line")
    bi = lax.axis_index("bus")
    z = bi // 2
    c = bi - 2 * z
    return li, z, c


def split3(x):
    high = x.astype(bf16).astype(f32)
    rest = x - high
    middle = rest.astype(bf16).astype(f32)
    return high, middle, rest - middle


def multiply(a, b):
    return jnp.dot(a, b, preferred_element_type=f32)


def rows_of(shape):
    return lax.broadcasted_iota(jnp.int32, shape, 0)


def lanes_of(shape):
    return lax.broadcasted_iota(jnp.int32, shape, 1)


def build_selector(selector, place):
    for j in range(place.shape[1] // 256):
        at = slice(256 * j, 256 * (j + 1))
        selector[:, at] = jnp.where(rows_of((BS, 256)) == place[:, at], 1.0, 0.0).astype(bf16)


def one_hot_rows(row, width):
    diagonal = jnp.where(rows_of((128, 128)) == lanes_of((128, 128)), row, 0.0).astype(bf16)
    value = multiply(diagonal, jnp.ones((128, width), bf16))
    return jnp.where(value == lanes_of((128, width)).astype(f32), 1.0, 0.0).astype(bf16)


def build_line_selector(selector, place):
    for j in range(place.shape[1] // 128):
        at = slice(128 * j, 128 * (j + 1))
        selector[at, :] = one_hot_rows(place[:, at].astype(f32), BS)


def to_buses(values, block, line_selector):
    total = None
    pieces = [piece for v in values for piece in split3(v)]
    for j in range(block.shape[1] // CHUNK):
        at = slice(CHUNK * j, CHUNK * (j + 1))
        here = rows_of((PLANE, CHUNK)) == block[:, at]
        left = jnp.concatenate([jnp.where(here, p[:, at], 0.0).astype(bf16) for p in pieces], axis=0)
        part = multiply(left, line_selector[at, :])
        total = part if total is None else total + part
    sums = [total[PLANE * k : PLANE * (k + 1)] for k in range(len(pieces))]
    return [sums[3 * q] + sums[3 * q + 1] + sums[3 * q + 2] for q in range(len(values))]


def to_lines(table, block, selector):
    left = jnp.concatenate([p.astype(bf16) for p in split3(table)], axis=0)
    picked = []
    for j in range(block.shape[1] // CHUNK):
        at = slice(CHUNK * j, CHUNK * (j + 1))
        found = jnp.dot(left, selector[:, at], preferred_element_type=f32)
        found = found[0:PLANE] + found[PLANE : 2 * PLANE] + found[2 * PLANE : 3 * PLANE]
        here = rows_of((PLANE, CHUNK)) == block[:, at]
        picked.append(jnp.sum(jnp.where(here, found, 0.0), axis=0, keepdims=True))
    half = len(picked) // 2
    return jnp.concatenate(picked[:half], axis=1) - jnp.concatenate(picked[half:], axis=1)


def endpoint_rows(ends, z):
    start, end = ends[0:1, :], ends[1:2, :]
    both = jnp.concatenate([start, end], axis=1)
    return start, end, both & (BS - 1), (both >> 8) - PLANE * z


def plane_peers(li, z, c):
    y, x = li // 4, lax.rem(li, 4)
    ys = [lax.rem(y + d, 4) for d in range(4)]
    xs = [lax.rem(x + d, 4) for d in range(4)]
    cs = [c, 1 - c]
    reach = [0, 1, 2, 1]
    offsets = [(dy, dx, dc) for dy in range(4) for dx in range(4) for dc in range(2)]
    offsets.sort(key=lambda o: -reach[o[0]] - reach[o[1]])
    peers = []
    for dy, dx, dc in offsets[:-2] + [(0, 0, 1)]:
        l2, c2 = ys[dy] * 4 + xs[dx], cs[dc]
        peers.append((c2 * 16 + l2, (l2, 2 * z + c2)))
    return peers


def depth_peers(li, z, c):
    return [(li, 2 * lax.rem(z + d, DEPTH) + c) for d in (4, 3, 5, 2, 6, 1, 7)]


def greet(li, z, c):
    barrier = pltpu.get_barrier_semaphore()
    for device in [device for _, device in plane_peers(li, z, c)] + depth_peers(li, z, c):
        pl.semaphore_signal(barrier, 1, device_id=device, device_id_type=MESH)


def greeted():
    pl.semaphore_wait(pltpu.get_barrier_semaphore(), PLANE - 1 + DEPTH - 1)


def send_plane(pick, home, slot, recv, sems, li, z, c):
    for place, device in plane_peers(li, z, c):
        pltpu.make_async_remote_copy(
            pick(place), recv.at[slot], sems.at[0], sems.at[1], device_id=device, device_id_type=MESH
        ).start()
    pltpu.make_async_copy(home, recv.at[slot], sems.at[1]).start()


def send_depth(src, recv, sems, li, z, c):
    for device in depth_peers(li, z, c):
        pltpu.make_async_remote_copy(
            src, recv.at[z], sems.at[0], sems.at[1], device_id=device, device_id_type=MESH
        ).start()
    pltpu.make_async_copy(src, recv.at[z], sems.at[1]).start()


def wait_bytes(ref, sem):
    pltpu.make_async_copy(ref, ref, sem).wait()


def sum_slots(recv, at):
    total = recv[0, :, at]
    for s in range(1, recv.shape[0]):
        total = total + recv[s, :, at]
    return total


def eliminate(pa, pb, off):
    groups = len(pa)
    lane, row = lax.broadcasted_iota(jnp.int32, (8, 128), 1), rows_of((8, 128))

    def spread(sub):
        first = off + 8 * sub
        return [[jnp.broadcast_to(p[:, j : j + 1], (8, 128)) for p in pa] for j in range(first, first + 8)]

    columns, ahead = spread(0), None
    for sub in range(groups):
        first = off + 8 * sub
        inside = (lane >= first) & (lane < first + 8)
        unit = jnp.where(lane - first == row, 1.0, 0.0)
        pa = [jnp.where(inside, unit if g == sub else 0.0, pa[g]) for g in range(groups)]
        for k in range(8):
            if k == 3 and sub + 1 < groups:
                ahead = spread(sub + 1)
            pivot = columns[k]
            scale = 1.0 / pivot[sub][k : k + 1]
            here = row == k

            def swept(rows):
                top = rows[sub][k : k + 1] * scale
                rest = [rows[g] - pivot[g] * top for g in range(groups)]
                rest[sub] = jnp.where(here, top, rest[sub])
                return rest

            columns = columns[: k + 1] + [swept(c) for c in columns[k + 1 :]]
            if ahead is not None:
                ahead = [swept(c) for c in ahead]
            pa, pb = swept(pa), swept(pb)
        columns, ahead = ahead, None
    return pa, pb


def invert(work, between):
    n, w = work.shape[0], 32
    now = work[0:w, :]
    for i in range(n // w):
        slab, off = divmod(w * i, 128)
        a = slice(128 * slab, 128 * slab + 128)
        b = slice(128 - 128 * slab, 256 - 128 * slab)
        groups = range(0, w, 8)
        pa, pb = eliminate([now[g : g + 8, a] for g in groups], [now[g : g + 8, b] for g in groups], off)
        pa, pb = jnp.concatenate(pa, axis=0), jnp.concatenate(pb, axis=0)
        top = jnp.concatenate([pa, pb] if slab == 0 else [pb, pa], axis=1)
        parts = [jnp.zeros((off, n), f32)] * (off > 0) + [top]
        parts += [jnp.zeros((128 - w - off, n), f32)] * (off + w < 128)
        wide = jnp.concatenate(parts, axis=0)

        def take(rows):
            lanes = lax.broadcasted_iota(jnp.int32, rows.shape, 1)
            kept = jnp.where((lanes >= w * i) & (lanes < w * i + w), 0.0, rows)
            return kept - jnp.dot(rows[:, a], wide, precision=lax.Precision.HIGHEST, preferred_element_type=f32)

        low, high = w * i, w * i + w
        work[low:high, :] = top
        if high < n:
            now = take(work[high : high + w, :])
        if high + w < n:
            work[high + w : n, :] = take(work[high + w : n, :])
        if low > 0:
            work[0:low, :] = take(work[0:low, :])
        between(i)


def longest_step(now, step):
    return jnp.min(now / jnp.maximum(-step, now), axis=1, keepdims=True)


def buckets(owner, values, shift):
    order = jnp.where(rows_of((256, 256)) < lax.broadcasted_iota(jnp.int32, (256, 256), 1), 1.0, 0.0).astype(bf16)
    carry = jnp.zeros((PLANE, 1), f32)
    packed = None
    for j in range(owner.shape[1] // 256):
        at = slice(256 * j, 256 * (j + 1))
        here = rows_of((PLANE, 256)) == owner[:, at]
        marks = jnp.where(here, 1.0, 0.0)
        rank = jnp.dot(marks.astype(bf16), order, preferred_element_type=f32) + carry
        carry = carry + jnp.sum(marks, axis=1, keepdims=True)
        rank = jnp.sum(jnp.where(here, rank, 0.0), axis=0, keepdims=True)
        code = jnp.where(rank < SLOTS, rank + shift, -1.0)
        slots = jnp.where(rows_of((128, 256)).astype(f32) == code, 1.0, 0.0).astype(bf16)
        left = jnp.concatenate([jnp.where(here, v[:, at], 0.0).astype(bf16) for v in values], axis=0)
        piece = lax.dot_general(left, slots, (((1,), (1,)), ((), ())), preferred_element_type=f32)
        packed = piece if packed is None else packed + piece
    packed = [packed[PLANE * k : PLANE * (k + 1)] for k in range(len(values))]
    return packed, jnp.max(carry, axis=0, keepdims=True)


def bucket_lines(msg_in):
    near = rows_of((BS, 128)).astype(f32)
    rows = [msg_in[k, :, 256:384] + msg_in[k + 1, :, 256:384] for k in range(0, PLANE, 2)]
    here = jnp.concatenate(rows, axis=0)
    up, up2 = pltpu.roll(here, LANE_STEP, 1), pltpu.roll(here, 2 * LANE_STEP, 1)
    down, down2 = pltpu.roll(here, 128 - LANE_STEP, 1), pltpu.roll(here, 128 - 2 * LANE_STEP, 1)
    lane = lanes_of((1, 128))

    def joined(parts, first):
        row = jnp.zeros((1, 128), f32)
        for k in (2, 1, 0):
            if first + k < len(rows):
                row = jnp.where(lane < LANE_STEP * (k + 1), parts[k][first + k : first + k + 1], row)
            else:
                row = jnp.where(lane < LANE_STEP * (k + 1), 0.0, row)
        return row

    sides = []
    for first in range(0, len(rows), 3):
        p, q, d = joined((here, up, up2), first), joined((down, here, up), first), joined((down2, down, here), first)
        mark = near == p
        left = [jnp.where(mark, piece, 0.0).astype(bf16) for piece in split3(d)]
        sides.append((left, one_hot_rows(q, BS)))
    total = None
    for g in range(0, len(sides), 2):
        right = jnp.concatenate([side[1] for side in sides[g : g + 2]], axis=0)
        for k in range(3):
            add = multiply(jnp.concatenate([side[0][k] for side in sides[g : g + 2]], axis=1), right)
            total = add if total is None else total + add
    return total + total.T


def step_kernel(
    total_lines, given,
    primal_all, slacks_all, cost_all, ends_all, bus_dual_all, demand_all, normal,
    step_primal, step_slack, step_dual, lengths, fullest,
    primal, slacks, cost, ends, bus_dual, demand, selector, line_selector, partner, msg, msg_in, diff0, diff0_in, part0, part0_in, block_in, work, dual_res, split,
    solved, solved_in, diff, diff_in, part, part_in, solved2, solved2_in, diff2, diff2_in, final, final_in, last, last_in,
    in_sem, fixed_sem, pair_sem, msg_sem, diff0_sem, part0_sem,
    solved_sem, diff_sem, part_sem, solved2_sem, diff2_sem, last_sem, final_sem, out_sem,
):
    li, z, c = position()
    half = primal.shape[1]
    mine = pl.ds(pl.multiple_of(c * half, half), half)
    own_buses = pl.ds(pl.multiple_of(li * BS, BS), BS)
    copies = [
        pltpu.make_async_copy(src, dst, in_sem.at[k])
        for k, (src, dst) in enumerate(
            (
                (ends_all.at[:, mine], ends),
                (primal_all.at[:, mine], primal),
                (slacks_all.at[:, mine], slacks),
                (bus_dual_all, bus_dual),
                (cost_all.at[:, mine], cost),
                (demand_all.at[:, own_buses], demand),
            )
        )
    ]
    for copy in copies:
        copy.start()
    own = pltpu.make_async_copy(normal if given else normal.at[li], block_in, fixed_sem)
    own.start()
    greet(li, z, c)
    at_home = c * 16 + li
    source = 2 * li + c
    lane1 = lax.broadcasted_iota(jnp.int32, (1, 128), 1)
    copies[0].wait()
    start, end, place, block = endpoint_rows(ends, z)
    build_line_selector(line_selector, place)
    copies[1].wait()
    copies[2].wait()
    x, s = primal[...], slacks[...]
    scaling = x / s
    inverse = 1.0 / s
    gap = jnp.sum(x * s, axis=1, keepdims=True)
    owner = jnp.where((start >> 8) == (end >> 8), block[:, :half], -1)
    shift = (SLOTS * lax.rem(source, 2)).astype(f32)
    packed, most = buckets(
        owner, [place[:, :half].astype(f32), place[:, half:].astype(f32), *split3(scaling)], shift
    )
    (ends_sum,) = to_buses([jnp.concatenate([scaling, scaling], axis=1)], block, line_selector)
    row = packed[0] + pltpu.roll(packed[1], LANE_STEP, 1)
    row = row + pltpu.roll(packed[2] + packed[3] + packed[4], 2 * LANE_STEP, 1)
    row = jnp.where(lane1 == 127, gap, row)
    whole = jnp.concatenate([ends_sum, row], axis=1)
    for b in range(PLANE):
        msg[b] = whole[b : b + 1]
    for copy in copies[3:]:
        copy.wait()

    greeted()
    pair = pltpu.make_async_remote_copy(
        bus_dual, partner, pair_sem.at[0], pair_sem.at[1], device_id=(li, 2 * z + 1 - c), device_id_type=MESH
    )
    pair.start()
    send_plane(lambda b: msg.at[b], msg.at[at_home], source, msg_in, msg_sem, li, z, c)

    build_selector(selector, place)
    pair.wait()
    mine_dual = jnp.concatenate([bus_dual[:, BS * k : BS * (k + 1)] for k in range(16)], axis=0)
    other_dual = jnp.concatenate([partner[:, BS * k : BS * (k + 1)] for k in range(16)], axis=0)
    table = jnp.concatenate(
        [jnp.where(c == 0, mine_dual, other_dual), jnp.where(c == 0, other_dual, mine_dual)], axis=0
    )
    diff0[:, :half] = to_lines(table, block, selector)
    diff0[:, half:] = jnp.broadcast_to(most, (1, 128))
    send_depth(diff0, diff0_in, diff0_sem, li, z, c)

    (sums,) = to_buses([jnp.concatenate([inverse, -inverse], axis=1)], block, line_selector)
    for b in range(PLANE):
        part0[b, :, 256:512] = sums[b : b + 1]
    wait_bytes(msg_in, msg_sem.at[1])
    sums = sum_slots(msg_in, slice(0, 256))
    gap0 = sum_slots(msg_in, slice(256, 384))[:, 127:128]
    own.wait()
    if given:
        work[...] = block_in[...]
    else:
        diagonal = rows_of((BS, BS)) == lax.broadcasted_iota(jnp.int32, (BS, BS), 1)
        work[...] = block_in[...] + jnp.where(diagonal, sums, 0.0) - bucket_lines(msg_in)

    def first_right_side(panel):
        if panel != 1:
            return
        wait_bytes(diff0_in, diff0_sem.at[1])
        residual = cost[...] - sum_slots(diff0_in, slice(0, half)) - s
        dual_res[...] = residual
        most = diff0_in[0, :, half:]
        for k in range(1, DEPTH):
            most = jnp.maximum(most, diff0_in[k, :, half:])
        flow = scaling * residual
        (sums,) = to_buses([jnp.concatenate([flow, -flow], axis=1)], block, line_selector)
        for b in range(PLANE):
            part0[b, :, 0:256] = sums[b : b + 1]
            part0[b, :, 512:640] = most
        send_plane(lambda b: part0.at[b], part0.at[at_home], source, part0_in, part0_sem, li, z, c)

    invert(work, first_right_side)
    wait_bytes(part0_in, part0_sem.at[1])
    sums = sum_slots(part0_in, slice(0, 512))
    right, third = demand[...] + sums[:, :256], sums[:, 256:]

    def solve(vector):
        wide = jnp.broadcast_to(vector, (8, BS))
        return jnp.dot(wide, work[...], precision=lax.Precision.HIGHEST, preferred_element_type=f32)[0:1]

    solved[...] = solve(right)
    send_plane(lambda b: solved, solved, at_home, solved_in, solved_sem, li, z, c)
    for k, piece in enumerate(split3(work[...])):
        split[k] = piece.astype(bf16)
    wait_bytes(solved_in, solved_sem.at[1])
    table = jnp.concatenate([solved_in[b] for b in range(PLANE)], axis=0)
    diff[...] = to_lines(table, block, selector)
    send_depth(diff, diff_in, diff_sem, li, z, c)
    wait_bytes(diff_in, diff_sem.at[1])
    affine_slack = dual_res[...] - sum_slots(diff_in, slice(0, half))
    affine_primal = -x - scaling * affine_slack
    cross = affine_primal * affine_slack
    extra = cross / s
    (sums,) = to_buses([jnp.concatenate([extra, -extra], axis=1)], block, line_selector)
    scalars = [
        longest_step(x, affine_primal),
        longest_step(s, affine_slack),
        jnp.sum(affine_primal * s, axis=1, keepdims=True),
        jnp.sum(x * affine_slack, axis=1, keepdims=True),
        jnp.sum(cross, axis=1, keepdims=True),
    ]
    row = jnp.zeros((1, 128), f32)
    for k, value in enumerate(scalars):
        row = jnp.where(lane1 == k, value, row)
    whole = jnp.concatenate([sums, jnp.broadcast_to(row, (PLANE, 128))], axis=1)
    for b in range(PLANE):
        part[b] = whole[b : b + 1]
    send_plane(lambda b: part.at[b], part.at[at_home], source, part_in, part_sem, li, z, c)
    wait_bytes(part_in, part_sem.at[1])

    added = sum_slots(part_in, slice(0, 384))
    least = part_in[0, :, 256:384]
    for k in range(1, PLANE):
        least = jnp.minimum(least, part_in[k, :, 256:384])
    take_p, take_d = least[:, 0:1], least[:, 1:2]
    tail = added[:, 256:384]
    gap_affine = gap0 + take_p * tail[:, 2:3] + take_d * tail[:, 3:4] + take_p * take_d * tail[:, 4:5]
    ratio = gap_affine / gap0
    aim = ratio * ratio * ratio * (gap0 / total_lines)
    right = right - aim * third + added[:, :256]
    high, middle, low = split3(jnp.broadcast_to(right, (8, BS)))
    three = jnp.concatenate([high, middle, low], axis=0).astype(bf16)
    by_high, by_middle, by_low = multiply(three, split[0]), multiply(three[0:16], split[1]), multiply(three[0:8], split[2])
    solved2[...] = (
        by_high[0:1] + (by_high[8:9] + by_middle[0:1]) + (by_high[16:17] + by_middle[8:9] + by_low[0:1])
    )
    send_plane(lambda b: solved2, solved2, at_home, solved2_in, solved2_sem, li, z, c)
    wait_bytes(solved2_in, solved2_sem.at[1])
    table = jnp.concatenate([solved2_in[b] for b in range(PLANE)], axis=0)
    diff2[...] = to_lines(table, block, selector)
    send_depth(diff2, diff2_in, diff2_sem, li, z, c)
    for b in range(16):
        pltpu.make_async_copy(solved2_in.at[16 * c + b], step_dual.at[:, pl.ds(BS * b, BS)], out_sem.at[2]).start()
    wait_bytes(diff2_in, diff2_sem.at[1])
    slack = dual_res[...] - sum_slots(diff2_in, slice(0, half))
    primal_step = (aim - x * s - cross) / s - scaling * slack
    last[...] = jnp.where(lane1 == 0, longest_step(x, primal_step), longest_step(s, slack))
    final[0] = primal_step
    final[1] = slack
    send_plane(lambda b: last, last, source, last_in, last_sem, li, z, c)
    pair2 = pltpu.make_async_remote_copy(
        final, final_in, final_sem.at[0], final_sem.at[1], device_id=(li, 2 * z + 1 - c), device_id_type=MESH
    )
    pair2.start()
    for k, out in enumerate((step_primal, step_slack)):
        pltpu.make_async_copy(final.at[k], out.at[:, mine], out_sem.at[k]).start()
    most = part0_in[0, :, 512:]
    for k in range(1, PLANE):
        most = jnp.maximum(most, part0_in[k, :, 512:])
    fullest[...] = most[:, 0:1]
    pair2.wait()
    other = pl.ds(pl.multiple_of((1 - c) * half, half), half)
    for k, out in enumerate((step_primal, step_slack)):
        pltpu.make_async_copy(final_in.at[k], out.at[:, other], out_sem.at[k]).start()
    for recv, sems in (
        (msg_in, msg_sem), (diff0_in, diff0_sem), (part0_in, part0_sem), (solved_in, solved_sem), (diff_in, diff_sem),
        (part_in, part_sem), (solved2_in, solved2_sem), (diff2_in, diff2_sem), (last_in, last_sem),
    ):
        wait_bytes(recv.at[pl.ds(0, recv.shape[0] - 1)], sems.at[0])
    for k, out in enumerate((step_primal, step_slack, step_dual)):
        wait_bytes(out, out_sem.at[k])
    wait_bytes(last_in, last_sem.at[1])
    least = last_in[0]
    for k in range(1, PLANE):
        least = jnp.minimum(least, last_in[k])
    lengths[...] = damping * least


def vmem(n):
    return [pl.BlockSpec(memory_space=pltpu.VMEM)] * n


def struct(*shape):
    return jax.ShapeDtypeStruct(shape, f32)


def scattered_block(primal, slacks, endpoints, fixed_part):
    blocks_here, block_size = fixed_part.shape[0], fixed_part.shape[1]
    buses_here = blocks_here * block_size
    scaling = primal / slacks
    local = endpoints - lax.axis_index("bus") * buses_here
    own_from, own_to = jnp.where((local >= 0) & (local < buses_here), local, buses_here)
    same_block = endpoints[0] // block_size == endpoints[1] // block_size
    crossing = jnp.where(same_block, -scaling, jnp.zeros_like(scaling))
    rows = jnp.concatenate([own_from, own_to, own_from, own_to])
    columns = jnp.concatenate([own_from, own_to, own_to, own_from]) % block_size
    values = jnp.concatenate([scaling, scaling, crossing, crossing])
    flat = jnp.zeros((buses_here * block_size,), f32).at[rows * block_size + columns].add(values, mode="drop")
    tiles = lax.all_to_all(flat.reshape(blocks_here, block_size, block_size), "line", 0, 0, tiled=True)
    mine = lax.dynamic_index_in_dim(fixed_part, lax.axis_index("line"), 0, keepdims=False)
    return mine + jnp.sum(tiles, axis=0)


def hand_over(step_primal, step_slack, step_dual, lengths, primal_out, slack_out, dual_out, lengths_out):
    primal_out[...] = step_primal[...]
    slack_out[...] = step_slack[...]
    dual_out[...] = step_dual[...]
    lengths_out[...] = lengths[:, 0:2]


def whole_step(given, args, normal):
    x, s, cost, ends, bus_dual, demand = args
    lines_here, buses_here = x.shape[1], bus_dual.shape[1]
    half = lines_here // 2
    total_lines = float(lines_here * lax.axis_size("line"))
    dma = pltpu.SemaphoreType.DMA
    exchange = lambda slots, width: [pltpu.VMEM((1, width), f32), pltpu.VMEM((slots, 1, width), f32)]
    buckets_of = lambda width: [pltpu.VMEM((PLANE, 1, width), f32)] * 2
    return pl.pallas_call(
        functools.partial(step_kernel, total_lines, given),
        out_shape=(struct(1, lines_here), struct(1, lines_here), struct(1, buses_here), struct(1, 128), struct(1, 1)),
        in_specs=[pl.BlockSpec(memory_space=pl.ANY)] * 7,
        out_specs=(pl.BlockSpec(memory_space=pl.ANY),) * 3 + tuple(vmem(2)),
        scratch_shapes=[pltpu.VMEM((1, half), f32)] * 3
        + [pltpu.VMEM((2, half), jnp.int32), pltpu.VMEM((1, buses_here), f32), pltpu.VMEM((1, BS), f32)]
        + [pltpu.VMEM((BS, lines_here), bf16), pltpu.VMEM((lines_here, BS), bf16), pltpu.VMEM((1, buses_here), f32)]
        + buckets_of(384)
        + exchange(DEPTH, half + 128)
        + buckets_of(640)
        + [pltpu.VMEM((BS, BS), f32)] * 2
        + [pltpu.VMEM((1, half), f32), pltpu.VMEM((3, BS, BS), bf16)]
        + exchange(PLANE, BS)
        + exchange(DEPTH, half)
        + buckets_of(384)
        + exchange(PLANE, BS)
        + exchange(DEPTH, half)
        + [pltpu.VMEM((2, 1, half), f32)] * 2
        + exchange(PLANE, 128)
        + [dma((6,)), dma]
        + [dma((2,))] * 11
        + [dma((3,))],
        compiler_params=pltpu.CompilerParams(collective_id=int(given), has_side_effects=True),
        name="step_given" if given else "step",
    )(*args, normal)


def per_device(primal, slacks, line_cost, bus_dual, demand, endpoints, fixed_part):
    args = tuple(a.reshape(1, -1) for a in (primal, slacks, line_cost))
    args += (endpoints, bus_dual.reshape(1, -1), demand.reshape(1, -1))
    def again(steps):
        normal = scattered_block(primal, slacks, endpoints, fixed_part)
        *steps, fullest = whole_step(True, args, normal)
        return (*steps, jnp.zeros_like(fullest))

    *steps, _ = lax.while_loop(lambda steps: steps[-1][0, 0] > SLOTS, again, tuple(whole_step(False, args, fixed_part)))
    outputs = pl.pallas_call(
        hand_over,
        out_shape=tuple(struct(*a.shape) for a in steps[:3]) + (struct(1, 2),),
        in_specs=vmem(4),
        out_specs=tuple(vmem(4)),
        name="hand_over",
    )(*steps)
    return tuple(a.reshape(-1) for a in outputs)


def solution(mesh):
    in_specs = (P("line"), P("line"), P("line"), P("bus"), P("bus"), P(None, "line"), P("bus", None, None))
    out_specs = (P("line"), P("line"), P("bus"), P())
    return jax.shard_map(per_device, mesh=mesh, in_specs=in_specs, out_specs=out_specs, check_vma=False)
```

```python
import functools

import jax
import jax.numpy as jnp
from jax import lax
from jax.experimental import pallas as pl
from jax.experimental.pallas import tpu as pltpu
from jax.sharding import PartitionSpec as P

damping = 0.99

f32 = jnp.float32
bf16 = jnp.bfloat16
MESH = pl.DeviceIdType.MESH

BS = 256
PLANE = 32
DEPTH = 8
LANE_STEP = 42
SLOTS = 20
CHUNK = 512


def position():
    li = lax.axis_index("line")
    bi = lax.axis_index("bus")
    z = bi // 2
    c = bi - 2 * z
    return li, z, c


def split3(x):
    high = x.astype(bf16).astype(f32)
    rest = x - high
    middle = rest.astype(bf16).astype(f32)
    return high, middle, rest - middle


def multiply(a, b):
    return jnp.dot(a, b, preferred_element_type=f32)


def rows_of(shape):
    return lax.broadcasted_iota(jnp.int32, shape, 0)


def lanes_of(shape):
    return lax.broadcasted_iota(jnp.int32, shape, 1)


def build_selector(selector, place):
    for j in range(place.shape[1] // 256):
        at = slice(256 * j, 256 * (j + 1))
        selector[:, at] = jnp.where(rows_of((BS, 256)) == place[:, at], 1.0, 0.0).astype(bf16)


def one_hot_rows(row, width):
    diagonal = jnp.where(rows_of((128, 128)) == lanes_of((128, 128)), row, 0.0).astype(bf16)
    value = multiply(diagonal, jnp.ones((128, width), bf16))
    return jnp.where(value == lanes_of((128, width)).astype(f32), 1.0, 0.0).astype(bf16)


def build_line_selector(selector, place):
    for j in range(place.shape[1] // 128):
        at = slice(128 * j, 128 * (j + 1))
        selector[at, :] = one_hot_rows(place[:, at].astype(f32), BS)


def to_buses(values, block, line_selector):
    total = None
    pieces = [piece for v in values for piece in split3(v)]
    for j in range(block.shape[1] // CHUNK):
        at = slice(CHUNK * j, CHUNK * (j + 1))
        here = rows_of((PLANE, CHUNK)) == block[:, at]
        left = jnp.concatenate([jnp.where(here, p[:, at], 0.0).astype(bf16) for p in pieces], axis=0)
        part = multiply(left, line_selector[at, :])
        total = part if total is None else total + part
    sums = [total[PLANE * k : PLANE * (k + 1)] for k in range(len(pieces))]
    return [sums[3 * q] + sums[3 * q + 1] + sums[3 * q + 2] for q in range(len(values))]


def to_lines(table, block, selector):
    left = jnp.concatenate([p.astype(bf16) for p in split3(table)], axis=0)
    picked = []
    for j in range(block.shape[1] // CHUNK):
        at = slice(CHUNK * j, CHUNK * (j + 1))
        found = jnp.dot(left, selector[:, at], preferred_element_type=f32)
        found = found[0:PLANE] + found[PLANE : 2 * PLANE] + found[2 * PLANE : 3 * PLANE]
        here = rows_of((PLANE, CHUNK)) == block[:, at]
        picked.append(jnp.sum(jnp.where(here, found, 0.0), axis=0, keepdims=True))
    half = len(picked) // 2
    return jnp.concatenate(picked[:half], axis=1) - jnp.concatenate(picked[half:], axis=1)


def endpoint_rows(ends, z):
    start, end = ends[0:1, :], ends[1:2, :]
    both = jnp.concatenate([start, end], axis=1)
    return start, end, both & (BS - 1), (both >> 8) - PLANE * z


def plane_peers(li, z, c):
    y, x = li // 4, lax.rem(li, 4)
    ys = [lax.rem(y + d, 4) for d in range(4)]
    xs = [lax.rem(x + d, 4) for d in range(4)]
    cs = [c, 1 - c]
    reach = [0, 1, 2, 1]
    offsets = [(dy, dx, dc) for dy in range(4) for dx in range(4) for dc in range(2)]
    offsets.sort(key=lambda o: -reach[o[0]] - reach[o[1]])
    peers = []
    for dy, dx, dc in offsets[:-2] + [(0, 0, 1)]:
        l2, c2 = ys[dy] * 4 + xs[dx], cs[dc]
        peers.append((c2 * 16 + l2, (l2, 2 * z + c2)))
    return peers


def depth_peers(li, z, c):
    return [(li, 2 * lax.rem(z + d, DEPTH) + c) for d in (4, 3, 5, 2, 6, 1, 7)]


def greet(li, z, c):
    barrier = pltpu.get_barrier_semaphore()
    for device in [device for _, device in plane_peers(li, z, c)] + depth_peers(li, z, c):
        pl.semaphore_signal(barrier, 1, device_id=device, device_id_type=MESH)


def greeted():
    pl.semaphore_wait(pltpu.get_barrier_semaphore(), PLANE - 1 + DEPTH - 1)


def send_plane(pick, home, slot, recv, sems, li, z, c):
    for place, device in plane_peers(li, z, c):
        pltpu.make_async_remote_copy(
            pick(place), recv.at[slot], sems.at[0], sems.at[1], device_id=device, device_id_type=MESH
        ).start()
    pltpu.make_async_copy(home, recv.at[slot], sems.at[1]).start()


def send_depth(src, recv, sems, li, z, c):
    for device in depth_peers(li, z, c):
        pltpu.make_async_remote_copy(
            src, recv.at[z], sems.at[0], sems.at[1], device_id=device, device_id_type=MESH
        ).start()
    pltpu.make_async_copy(src, recv.at[z], sems.at[1]).start()


def wait_bytes(ref, sem):
    pltpu.make_async_copy(ref, ref, sem).wait()


def sum_slots(recv, at):
    total = recv[0, :, at]
    for s in range(1, recv.shape[0]):
        total = total + recv[s, :, at]
    return total


def eliminate(pa, pb, off):
    groups = len(pa)
    lane, row = lax.broadcasted_iota(jnp.int32, (8, 128), 1), rows_of((8, 128))

    def spread(sub):
        first = off + 8 * sub
        return [[jnp.broadcast_to(p[:, j : j + 1], (8, 128)) for p in pa] for j in range(first, first + 8)]

    columns, ahead = spread(0), None
    for sub in range(groups):
        first = off + 8 * sub
        inside = (lane >= first) & (lane < first + 8)
        unit = jnp.where(lane - first == row, 1.0, 0.0)
        pa = [jnp.where(inside, unit if g == sub else 0.0, pa[g]) for g in range(groups)]
        for k in range(8):
            if k == 3 and sub + 1 < groups:
                ahead = spread(sub + 1)
            pivot = columns[k]
            scale = 1.0 / pivot[sub][k : k + 1]
            here = row == k

            def swept(rows):
                top = rows[sub][k : k + 1] * scale
                rest = [rows[g] - pivot[g] * top for g in range(groups)]
                rest[sub] = jnp.where(here, top, rest[sub])
                return rest

            columns = columns[: k + 1] + [swept(c) for c in columns[k + 1 :]]
            if ahead is not None:
                ahead = [swept(c) for c in ahead]
            pa, pb = swept(pa), swept(pb)
        columns, ahead = ahead, None
    return pa, pb


def invert(work, between):
    n, w = work.shape[0], 32
    now = work[0:w, :]
    for i in range(n // w):
        slab, off = divmod(w * i, 128)
        a = slice(128 * slab, 128 * slab + 128)
        b = slice(128 - 128 * slab, 256 - 128 * slab)
        groups = range(0, w, 8)
        pa, pb = eliminate([now[g : g + 8, a] for g in groups], [now[g : g + 8, b] for g in groups], off)
        pa, pb = jnp.concatenate(pa, axis=0), jnp.concatenate(pb, axis=0)
        top = jnp.concatenate([pa, pb] if slab == 0 else [pb, pa], axis=1)
        parts = [jnp.zeros((off, n), f32)] * (off > 0) + [top]
        parts += [jnp.zeros((128 - w - off, n), f32)] * (off + w < 128)
        wide = jnp.concatenate(parts, axis=0)

        def take(rows):
            lanes = lax.broadcasted_iota(jnp.int32, rows.shape, 1)
            kept = jnp.where((lanes >= w * i) & (lanes < w * i + w), 0.0, rows)
            return kept - jnp.dot(rows[:, a], wide, precision=lax.Precision.HIGHEST, preferred_element_type=f32)

        low, high = w * i, w * i + w
        work[low:high, :] = top
        if high < n:
            now = take(work[high : high + w, :])
        if high + w < n:
            work[high + w : n, :] = take(work[high + w : n, :])
        if low > 0:
            work[0:low, :] = take(work[0:low, :])
        between(i)


def longest_step(now, step):
    return jnp.min(now / jnp.maximum(-step, now), axis=1, keepdims=True)


def buckets(owner, values, shift):
    order = jnp.where(rows_of((256, 256)) < lax.broadcasted_iota(jnp.int32, (256, 256), 1), 1.0, 0.0).astype(bf16)
    carry = jnp.zeros((PLANE, 1), f32)
    packed = None
    for j in range(owner.shape[1] // 256):
        at = slice(256 * j, 256 * (j + 1))
        here = rows_of((PLANE, 256)) == owner[:, at]
        marks = jnp.where(here, 1.0, 0.0)
        rank = jnp.dot(marks.astype(bf16), order, preferred_element_type=f32) + carry
        carry = carry + jnp.sum(marks, axis=1, keepdims=True)
        rank = jnp.sum(jnp.where(here, rank, 0.0), axis=0, keepdims=True)
        code = jnp.where(rank < SLOTS, rank + shift, -1.0)
        slots = jnp.where(rows_of((128, 256)).astype(f32) == code, 1.0, 0.0).astype(bf16)
        left = jnp.concatenate([jnp.where(here, v[:, at], 0.0).astype(bf16) for v in values], axis=0)
        piece = lax.dot_general(left, slots, (((1,), (1,)), ((), ())), preferred_element_type=f32)
        packed = piece if packed is None else packed + piece
    packed = [packed[PLANE * k : PLANE * (k + 1)] for k in range(len(values))]
    return packed, jnp.max(carry, axis=0, keepdims=True)


def bucket_lines(msg_in):
    near = rows_of((BS, 128)).astype(f32)
    rows = [msg_in[k, :, 256:384] + msg_in[k + 1, :, 256:384] for k in range(0, PLANE, 2)]
    here = jnp.concatenate(rows, axis=0)
    up, up2 = pltpu.roll(here, LANE_STEP, 1), pltpu.roll(here, 2 * LANE_STEP, 1)
    down, down2 = pltpu.roll(here, 128 - LANE_STEP, 1), pltpu.roll(here, 128 - 2 * LANE_STEP, 1)
    lane = lanes_of((1, 128))

    def joined(parts, first):
        row = jnp.zeros((1, 128), f32)
        for k in (2, 1, 0):
            if first + k < len(rows):
                row = jnp.where(lane < LANE_STEP * (k + 1), parts[k][first + k : first + k + 1], row)
            else:
                row = jnp.where(lane < LANE_STEP * (k + 1), 0.0, row)
        return row

    sides = []
    for first in range(0, len(rows), 3):
        p, q, d = joined((here, up, up2), first), joined((down, here, up), first), joined((down2, down, here), first)
        mark = near == p
        left = [jnp.where(mark, piece, 0.0).astype(bf16) for piece in split3(d)]
        sides.append((left, one_hot_rows(q, BS)))
    total = None
    for g in range(0, len(sides), 2):
        right = jnp.concatenate([side[1] for side in sides[g : g + 2]], axis=0)
        for k in range(3):
            add = multiply(jnp.concatenate([side[0][k] for side in sides[g : g + 2]], axis=1), right)
            total = add if total is None else total + add
    return total + total.T


def step_kernel(
    total_lines, given,
    primal_all, slacks_all, cost_all, ends_all, bus_dual_all, demand_all, normal,
    step_primal, step_slack, step_dual, lengths, fullest,
    primal, slacks, cost, ends, bus_dual, demand, selector, line_selector, partner, msg, msg_in, diff0, diff0_in, part0, part0_in, block_in, work, dual_res, split,
    solved, solved_in, diff, diff_in, part, part_in, solved2, solved2_in, diff2, diff2_in, final, final_in, last, last_in,
    in_sem, fixed_sem, pair_sem, msg_sem, diff0_sem, part0_sem,
    solved_sem, diff_sem, part_sem, solved2_sem, diff2_sem, last_sem, final_sem, out_sem,
):
    li, z, c = position()
    half = primal.shape[1]
    mine = pl.ds(pl.multiple_of(c * half, half), half)
    own_buses = pl.ds(pl.multiple_of(li * BS, BS), BS)
    copies = [
        pltpu.make_async_copy(src, dst, in_sem.at[k])
        for k, (src, dst) in enumerate(
            (
                (ends_all.at[:, mine], ends),
                (primal_all.at[:, mine], primal),
                (slacks_all.at[:, mine], slacks),
                (bus_dual_all, bus_dual),
                (cost_all.at[:, mine], cost),
                (demand_all.at[:, own_buses], demand),
            )
        )
    ]
    for copy in copies:
        copy.start()
    own = pltpu.make_async_copy(normal if given else normal.at[li], block_in, fixed_sem)
    own.start()
    greet(li, z, c)
    at_home = c * 16 + li
    source = 2 * li + c
    lane1 = lax.broadcasted_iota(jnp.int32, (1, 128), 1)
    copies[0].wait()
    start, end, place, block = endpoint_rows(ends, z)
    build_line_selector(line_selector, place)
    copies[1].wait()
    copies[2].wait()
    x, s = primal[...], slacks[...]
    scaling = x / s
    inverse = 1.0 / s
    gap = jnp.sum(x * s, axis=1, keepdims=True)
    owner = jnp.where((start >> 8) == (end >> 8), block[:, :half], -1)
    shift = (SLOTS * lax.rem(source, 2)).astype(f32)
    packed, most = buckets(
        owner, [place[:, :half].astype(f32), place[:, half:].astype(f32), *split3(scaling)], shift
    )
    (ends_sum,) = to_buses([jnp.concatenate([scaling, scaling], axis=1)], block, line_selector)
    row = packed[0] + pltpu.roll(packed[1], LANE_STEP, 1)
    row = row + pltpu.roll(packed[2] + packed[3] + packed[4], 2 * LANE_STEP, 1)
    row = jnp.where(lane1 == 127, gap, row)
    whole = jnp.concatenate([ends_sum, row], axis=1)
    for b in range(PLANE):
        msg[b] = whole[b : b + 1]
    for copy in copies[3:]:
        copy.wait()

    greeted()
    pair = pltpu.make_async_remote_copy(
        bus_dual, partner, pair_sem.at[0], pair_sem.at[1], device_id=(li, 2 * z + 1 - c), device_id_type=MESH
    )
    pair.start()
    send_plane(lambda b: msg.at[b], msg.at[at_home], source, msg_in, msg_sem, li, z, c)

    build_selector(selector, place)
    pair.wait()
    mine_dual = jnp.concatenate([bus_dual[:, BS * k : BS * (k + 1)] for k in range(16)], axis=0)
    other_dual = jnp.concatenate([partner[:, BS * k : BS * (k + 1)] for k in range(16)], axis=0)
    table = jnp.concatenate(
        [jnp.where(c == 0, mine_dual, other_dual), jnp.where(c == 0, other_dual, mine_dual)], axis=0
    )
    diff0[:, :half] = to_lines(table, block, selector)
    diff0[:, half:] = jnp.broadcast_to(most, (1, 128))
    send_depth(diff0, diff0_in, diff0_sem, li, z, c)

    (sums,) = to_buses([jnp.concatenate([inverse, -inverse], axis=1)], block, line_selector)
    for b in range(PLANE):
        part0[b, :, 256:512] = sums[b : b + 1]
    wait_bytes(msg_in, msg_sem.at[1])
    sums = sum_slots(msg_in, slice(0, 256))
    gap0 = sum_slots(msg_in, slice(256, 384))[:, 127:128]
    own.wait()
    if given:
        work[...] = block_in[...]
    else:
        diagonal = rows_of((BS, BS)) == lax.broadcasted_iota(jnp.int32, (BS, BS), 1)
        work[...] = block_in[...] + jnp.where(diagonal, sums, 0.0) - bucket_lines(msg_in)

    def first_right_side(panel):
        if panel == 1:
            send_plane(
                lambda b: part0.at[b], part0.at[at_home], source, part0_in, part0_sem, li, z, c
            )
        if panel != 0:
            return
        residual = cost[...] - sum_slots(diff0_in, slice(0, half)) - s
        dual_res[...] = residual
        most = diff0_in[0, :, half:]
        for k in range(1, DEPTH):
            most = jnp.maximum(most, diff0_in[k, :, half:])
        flow = scaling * residual
        (sums,) = to_buses([jnp.concatenate([flow, -flow], axis=1)], block, line_selector)
        for b in range(PLANE):
            part0[b, :, 0:256] = sums[b : b + 1]
            part0[b, :, 512:640] = most

    wait_bytes(diff0_in, diff0_sem.at[1])
    invert(work, first_right_side)
    wait_bytes(part0_in, part0_sem.at[1])
    right = demand[...] + sum_slots(part0_in, slice(0, 256))

    def solve(vector):
        wide = jnp.broadcast_to(vector, (8, BS))
        return jnp.dot(wide, work[...], precision=lax.Precision.HIGHEST, preferred_element_type=f32)[0:1]

    solved[...] = solve(right)
    send_plane(lambda b: solved, solved, at_home, solved_in, solved_sem, li, z, c)
    for k, piece in enumerate(split3(work[...])):
        split[k] = piece.astype(bf16)
    third = sum_slots(part0_in, slice(256, 512))
    wait_bytes(solved_in, solved_sem.at[1])
    table = jnp.concatenate([solved_in[b] for b in range(PLANE)], axis=0)
    diff[...] = to_lines(table, block, selector)
    send_depth(diff, diff_in, diff_sem, li, z, c)
    wait_bytes(diff_in, diff_sem.at[1])
    affine_slack = dual_res[...] - sum_slots(diff_in, slice(0, half))
    affine_primal = -x - scaling * affine_slack
    cross = affine_primal * affine_slack
    extra = cross / s
    (sums,) = to_buses([jnp.concatenate([extra, -extra], axis=1)], block, line_selector)
    scalars = [
        longest_step(x, affine_primal),
        longest_step(s, affine_slack),
        jnp.sum(affine_primal * s, axis=1, keepdims=True),
        jnp.sum(x * affine_slack, axis=1, keepdims=True),
        jnp.sum(cross, axis=1, keepdims=True),
    ]
    row = jnp.zeros((1, 128), f32)
    for k, value in enumerate(scalars):
        row = jnp.where(lane1 == k, value, row)
    whole = jnp.concatenate([sums, jnp.broadcast_to(row, (PLANE, 128))], axis=1)
    for b in range(PLANE):
        part[b] = whole[b : b + 1]
    send_plane(lambda b: part.at[b], part.at[at_home], source, part_in, part_sem, li, z, c)
    wait_bytes(part_in, part_sem.at[1])

    added = sum_slots(part_in, slice(0, 384))
    least = part_in[0, :, 256:384]
    for k in range(1, PLANE):
        least = jnp.minimum(least, part_in[k, :, 256:384])
    take_p, take_d = least[:, 0:1], least[:, 1:2]
    tail = added[:, 256:384]
    gap_affine = gap0 + take_p * tail[:, 2:3] + take_d * tail[:, 3:4] + take_p * take_d * tail[:, 4:5]
    ratio = gap_affine / gap0
    aim = ratio * ratio * ratio * (gap0 / total_lines)
    right = right - aim * third + added[:, :256]
    high, middle, low = split3(jnp.broadcast_to(right, (8, BS)))
    three = jnp.concatenate([high, middle, low], axis=0).astype(bf16)
    by_high, by_middle, by_low = multiply(three, split[0]), multiply(three[0:16], split[1]), multiply(three[0:8], split[2])
    solved2[...] = (
        by_high[0:1] + (by_high[8:9] + by_middle[0:1]) + (by_high[16:17] + by_middle[8:9] + by_low[0:1])
    )
    send_plane(lambda b: solved2, solved2, at_home, solved2_in, solved2_sem, li, z, c)
    wait_bytes(solved2_in, solved2_sem.at[1])
    table = jnp.concatenate([solved2_in[b] for b in range(PLANE)], axis=0)
    diff2[...] = to_lines(table, block, selector)
    send_depth(diff2, diff2_in, diff2_sem, li, z, c)
    for b in range(16):
        pltpu.make_async_copy(solved2_in.at[16 * c + b], step_dual.at[:, pl.ds(BS * b, BS)], out_sem.at[2]).start()
    wait_bytes(diff2_in, diff2_sem.at[1])
    slack = dual_res[...] - sum_slots(diff2_in, slice(0, half))
    primal_step = (aim - x * s - cross) / s - scaling * slack
    last[...] = jnp.where(lane1 == 0, longest_step(x, primal_step), longest_step(s, slack))
    final[0] = primal_step
    final[1] = slack
    send_plane(lambda b: last, last, source, last_in, last_sem, li, z, c)
    pair2 = pltpu.make_async_remote_copy(
        final, final_in, final_sem.at[0], final_sem.at[1], device_id=(li, 2 * z + 1 - c), device_id_type=MESH
    )
    pair2.start()
    for k, out in enumerate((step_primal, step_slack)):
        pltpu.make_async_copy(final.at[k], out.at[:, mine], out_sem.at[k]).start()
    most = part0_in[0, :, 512:]
    for k in range(1, PLANE):
        most = jnp.maximum(most, part0_in[k, :, 512:])
    fullest[...] = most[:, 0:1]
    pair2.wait()
    other = pl.ds(pl.multiple_of((1 - c) * half, half), half)
    for k, out in enumerate((step_primal, step_slack)):
        pltpu.make_async_copy(final_in.at[k], out.at[:, other], out_sem.at[k]).start()
    for recv, sems in (
        (msg_in, msg_sem), (diff0_in, diff0_sem), (part0_in, part0_sem), (solved_in, solved_sem), (diff_in, diff_sem),
        (part_in, part_sem), (solved2_in, solved2_sem), (diff2_in, diff2_sem), (last_in, last_sem),
    ):
        wait_bytes(recv.at[pl.ds(0, recv.shape[0] - 1)], sems.at[0])
    for k, out in enumerate((step_primal, step_slack, step_dual)):
        wait_bytes(out, out_sem.at[k])
    wait_bytes(last_in, last_sem.at[1])
    least = last_in[0]
    for k in range(1, PLANE):
        least = jnp.minimum(least, last_in[k])
    lengths[...] = damping * least


def vmem(n):
    return [pl.BlockSpec(memory_space=pltpu.VMEM)] * n


def struct(*shape):
    return jax.ShapeDtypeStruct(shape, f32)


def scattered_block(primal, slacks, endpoints, fixed_part):
    blocks_here, block_size = fixed_part.shape[0], fixed_part.shape[1]
    buses_here = blocks_here * block_size
    scaling = primal / slacks
    local = endpoints - lax.axis_index("bus") * buses_here
    own_from, own_to = jnp.where((local >= 0) & (local < buses_here), local, buses_here)
    same_block = endpoints[0] // block_size == endpoints[1] // block_size
    crossing = jnp.where(same_block, -scaling, jnp.zeros_like(scaling))
    rows = jnp.concatenate([own_from, own_to, own_from, own_to])
    columns = jnp.concatenate([own_from, own_to, own_to, own_from]) % block_size
    values = jnp.concatenate([scaling, scaling, crossing, crossing])
    flat = jnp.zeros((buses_here * block_size,), f32).at[rows * block_size + columns].add(values, mode="drop")
    tiles = lax.all_to_all(flat.reshape(blocks_here, block_size, block_size), "line", 0, 0, tiled=True)
    mine = lax.dynamic_index_in_dim(fixed_part, lax.axis_index("line"), 0, keepdims=False)
    return mine + jnp.sum(tiles, axis=0)


def hand_over(step_primal, step_slack, step_dual, lengths, primal_out, slack_out, dual_out, lengths_out):
    primal_out[...] = step_primal[...]
    slack_out[...] = step_slack[...]
    dual_out[...] = step_dual[...]
    lengths_out[...] = lengths[:, 0:2]


def whole_step(given, args, normal):
    x, s, cost, ends, bus_dual, demand = args
    lines_here, buses_here = x.shape[1], bus_dual.shape[1]
    half = lines_here // 2
    total_lines = float(lines_here * lax.axis_size("line"))
    dma = pltpu.SemaphoreType.DMA
    exchange = lambda slots, width: [pltpu.VMEM((1, width), f32), pltpu.VMEM((slots, 1, width), f32)]
    buckets_of = lambda width: [pltpu.VMEM((PLANE, 1, width), f32)] * 2
    return pl.pallas_call(
        functools.partial(step_kernel, total_lines, given),
        out_shape=tuple(pltpu.VMEM((1, n), f32) for n in (lines_here, lines_here, buses_here, 128, 1)),
        in_specs=[pl.BlockSpec(memory_space=pl.ANY)] * 7,
        out_specs=tuple(vmem(5)),
        scratch_shapes=[pltpu.VMEM((1, half), f32)] * 3
        + [pltpu.VMEM((2, half), jnp.int32), pltpu.VMEM((1, buses_here), f32), pltpu.VMEM((1, BS), f32)]
        + [pltpu.VMEM((BS, lines_here), bf16), pltpu.VMEM((lines_here, BS), bf16), pltpu.VMEM((1, buses_here), f32)]
        + buckets_of(384)
        + exchange(DEPTH, half + 128)
        + buckets_of(640)
        + [pltpu.VMEM((BS, BS), f32)] * 2
        + [pltpu.VMEM((1, half), f32), pltpu.VMEM((3, BS, BS), bf16)]
        + exchange(PLANE, BS)
        + exchange(DEPTH, half)
        + buckets_of(384)
        + exchange(PLANE, BS)
        + exchange(DEPTH, half)
        + [pltpu.VMEM((2, 1, half), f32)] * 2
        + exchange(PLANE, 128)
        + [dma((6,)), dma]
        + [dma((2,))] * 11
        + [dma((3,))],
        compiler_params=pltpu.CompilerParams(collective_id=int(given), has_side_effects=True),
        name="step_given" if given else "step",
    )(*args, normal)


def per_device(primal, slacks, line_cost, bus_dual, demand, endpoints, fixed_part):
    args = tuple(a.reshape(1, -1) for a in (primal, slacks, line_cost))
    args += (endpoints, bus_dual.reshape(1, -1), demand.reshape(1, -1))
    def again(steps):
        normal = scattered_block(primal, slacks, endpoints, fixed_part)
        *steps, fullest = whole_step(True, args, normal)
        return (*steps, jnp.zeros_like(fullest))

    *steps, _ = lax.while_loop(lambda steps: steps[-1][0, 0] > SLOTS, again, tuple(whole_step(False, args, fixed_part)))
    outputs = pl.pallas_call(
        hand_over,
        out_shape=tuple(struct(*a.shape) for a in steps[:3]) + (struct(1, 2),),
        in_specs=vmem(4),
        out_specs=tuple(vmem(4)),
        name="hand_over",
    )(*steps)
    return tuple(a.reshape(-1) for a in outputs)


def solution(mesh):
    in_specs = (P("line"), P("line"), P("line"), P("bus"), P("bus"), P(None, "line"), P("bus", None, None))
    out_specs = (P("line"), P("line"), P("bus"), P())
    return jax.shard_map(per_device, mesh=mesh, in_specs=in_specs, out_specs=out_specs, check_vma=False)
```

```python
import functools

import jax
import jax.numpy as jnp
from jax import lax
from jax.experimental import pallas as pl
from jax.experimental.pallas import tpu as pltpu
from jax.sharding import PartitionSpec as P

damping = 0.99

f32 = jnp.float32
bf16 = jnp.bfloat16
MESH = pl.DeviceIdType.MESH

BS = 256
PLANE = 32
DEPTH = 8
LANE_STEP = 42
SLOTS = 20
CHUNK = 512


def position():
    li = lax.axis_index("line")
    bi = lax.axis_index("bus")
    z = bi // 2
    c = bi - 2 * z
    return li, z, c


def split3(x):
    high = x.astype(bf16).astype(f32)
    rest = x - high
    middle = rest.astype(bf16).astype(f32)
    return high, middle, rest - middle


def multiply(a, b):
    return jnp.dot(a, b, preferred_element_type=f32)


def rows_of(shape):
    return lax.broadcasted_iota(jnp.int32, shape, 0)


def lanes_of(shape):
    return lax.broadcasted_iota(jnp.int32, shape, 1)


def build_selector(selector, place):
    for j in range(place.shape[1] // 256):
        at = slice(256 * j, 256 * (j + 1))
        selector[:, at] = jnp.where(rows_of((BS, 256)) == place[:, at], 1.0, 0.0).astype(bf16)


def one_hot_rows(row, width):
    diagonal = jnp.where(rows_of((128, 128)) == lanes_of((128, 128)), row, 0.0).astype(bf16)
    value = multiply(diagonal, jnp.ones((128, width), bf16))
    return jnp.where(value == lanes_of((128, width)).astype(f32), 1.0, 0.0).astype(bf16)


def build_line_selector(selector, place):
    for j in range(place.shape[1] // 128):
        at = slice(128 * j, 128 * (j + 1))
        selector[at, :] = one_hot_rows(place[:, at].astype(f32), BS)


def to_buses(values, block, line_selector):
    total = None
    pieces = [piece for v in values for piece in split3(v)]
    for j in range(block.shape[1] // CHUNK):
        at = slice(CHUNK * j, CHUNK * (j + 1))
        here = rows_of((PLANE, CHUNK)) == block[:, at]
        left = jnp.concatenate([jnp.where(here, p[:, at], 0.0).astype(bf16) for p in pieces], axis=0)
        part = multiply(left, line_selector[at, :])
        total = part if total is None else total + part
    sums = [total[PLANE * k : PLANE * (k + 1)] for k in range(len(pieces))]
    return [sums[3 * q] + sums[3 * q + 1] + sums[3 * q + 2] for q in range(len(values))]


def to_lines(table, block, selector):
    left = jnp.concatenate([p.astype(bf16) for p in split3(table)], axis=0)
    picked = []
    for j in range(block.shape[1] // CHUNK):
        at = slice(CHUNK * j, CHUNK * (j + 1))
        found = jnp.dot(left, selector[:, at], preferred_element_type=f32)
        found = found[0:PLANE] + found[PLANE : 2 * PLANE] + found[2 * PLANE : 3 * PLANE]
        here = rows_of((PLANE, CHUNK)) == block[:, at]
        picked.append(jnp.sum(jnp.where(here, found, 0.0), axis=0, keepdims=True))
    half = len(picked) // 2
    return jnp.concatenate(picked[:half], axis=1) - jnp.concatenate(picked[half:], axis=1)


def endpoint_rows(ends, z):
    start, end = ends[0:1, :], ends[1:2, :]
    both = jnp.concatenate([start, end], axis=1)
    return start, end, both & (BS - 1), (both >> 8) - PLANE * z


def plane_peers(li, z, c):
    y, x = li // 4, lax.rem(li, 4)
    ys = [lax.rem(y + d, 4) for d in range(4)]
    xs = [lax.rem(x + d, 4) for d in range(4)]
    cs = [c, 1 - c]
    reach = [0, 1, 2, 1]
    offsets = [(dy, dx, dc) for dy in range(4) for dx in range(4) for dc in range(2)]
    offsets.sort(key=lambda o: -reach[o[0]] - reach[o[1]])
    peers = []
    for dy, dx, dc in offsets[:-2] + [(0, 0, 1)]:
        l2, c2 = ys[dy] * 4 + xs[dx], cs[dc]
        peers.append((c2 * 16 + l2, (l2, 2 * z + c2)))
    return peers


def depth_peers(li, z, c):
    return [(li, 2 * lax.rem(z + d, DEPTH) + c) for d in (4, 3, 5, 2, 6, 1, 7)]


def greet(li, z, c):
    barrier = pltpu.get_barrier_semaphore()
    for device in [device for _, device in plane_peers(li, z, c)] + depth_peers(li, z, c):
        pl.semaphore_signal(barrier, 1, device_id=device, device_id_type=MESH)


def greeted():
    pl.semaphore_wait(pltpu.get_barrier_semaphore(), PLANE - 1 + DEPTH - 1)


def send_plane(pick, home, slot, recv, sems, li, z, c):
    for place, device in plane_peers(li, z, c):
        pltpu.make_async_remote_copy(
            pick(place), recv.at[slot], sems.at[0], sems.at[1], device_id=device, device_id_type=MESH
        ).start()
    pltpu.make_async_copy(home, recv.at[slot], sems.at[1]).start()


def send_depth(src, recv, sems, li, z, c):
    for device in depth_peers(li, z, c):
        pltpu.make_async_remote_copy(
            src, recv.at[z], sems.at[0], sems.at[1], device_id=device, device_id_type=MESH
        ).start()
    pltpu.make_async_copy(src, recv.at[z], sems.at[1]).start()


def wait_bytes(ref, sem):
    pltpu.make_async_copy(ref, ref, sem).wait()


def over_slots(combine, recv, at):
    rows = [recv[k, :, at] for k in range(recv.shape[0])]
    while len(rows) > 1:
        rows = [combine(rows[k], rows[k + 1]) for k in range(0, len(rows), 2)]
    return rows[0]


def sum_slots(recv, at):
    return over_slots(jnp.add, recv, at)


def eliminate(pa, pb, off):
    groups = len(pa)
    lane, row = lax.broadcasted_iota(jnp.int32, (8, 128), 1), rows_of((8, 128))

    def spread(sub):
        first = off + 8 * sub
        return [[jnp.broadcast_to(p[:, j : j + 1], (8, 128)) for p in pa] for j in range(first, first + 8)]

    columns, ahead = spread(0), None
    for sub in range(groups):
        first = off + 8 * sub
        inside = (lane >= first) & (lane < first + 8)
        unit = jnp.where(lane - first == row, 1.0, 0.0)
        pa = [jnp.where(inside, unit if g == sub else 0.0, pa[g]) for g in range(groups)]
        for k in range(8):
            if k == 3 and sub + 1 < groups:
                ahead = spread(sub + 1)
            pivot = columns[k]
            scale = 1.0 / pivot[sub][k : k + 1]
            here = row == k

            def swept(rows):
                top = rows[sub][k : k + 1] * scale
                rest = [rows[g] - pivot[g] * top for g in range(groups)]
                rest[sub] = jnp.where(here, top, rest[sub])
                return rest

            columns = columns[: k + 1] + [swept(c) for c in columns[k + 1 :]]
            if ahead is not None:
                ahead = [swept(c) for c in ahead]
            pa, pb = swept(pa), swept(pb)
        columns, ahead = ahead, None
    return pa, pb


def invert(work, between):
    n, w = work.shape[0], 32
    now = work[0:w, :]
    for i in range(n // w):
        slab, off = divmod(w * i, 128)
        a = slice(128 * slab, 128 * slab + 128)
        b = slice(128 - 128 * slab, 256 - 128 * slab)
        groups = range(0, w, 8)
        pa, pb = eliminate([now[g : g + 8, a] for g in groups], [now[g : g + 8, b] for g in groups], off)
        pa, pb = jnp.concatenate(pa, axis=0), jnp.concatenate(pb, axis=0)
        top = jnp.concatenate([pa, pb] if slab == 0 else [pb, pa], axis=1)
        parts = [jnp.zeros((off, n), f32)] * (off > 0) + [top]
        parts += [jnp.zeros((128 - w - off, n), f32)] * (off + w < 128)
        wide = jnp.concatenate(parts, axis=0)

        def take(rows):
            lanes = lax.broadcasted_iota(jnp.int32, rows.shape, 1)
            kept = jnp.where((lanes >= w * i) & (lanes < w * i + w), 0.0, rows)
            return kept - jnp.dot(rows[:, a], wide, precision=lax.Precision.HIGHEST, preferred_element_type=f32)

        low, high = w * i, w * i + w
        work[low:high, :] = top
        if high < n:
            now = take(work[high : high + w, :])
        if high + w < n:
            work[high + w : n, :] = take(work[high + w : n, :])
        if low > 0:
            work[0:low, :] = take(work[0:low, :])
        between(i)


def longest_step(now, step):
    return jnp.min(now / jnp.maximum(-step, now), axis=1, keepdims=True)


def buckets(owner, values, shift):
    order = jnp.where(rows_of((256, 256)) < lax.broadcasted_iota(jnp.int32, (256, 256), 1), 1.0, 0.0).astype(bf16)
    carry = jnp.zeros((PLANE, 1), f32)
    packed = None
    for j in range(owner.shape[1] // 256):
        at = slice(256 * j, 256 * (j + 1))
        here = rows_of((PLANE, 256)) == owner[:, at]
        marks = jnp.where(here, 1.0, 0.0)
        rank = jnp.dot(marks.astype(bf16), order, preferred_element_type=f32) + carry
        carry = carry + jnp.sum(marks, axis=1, keepdims=True)
        rank = jnp.sum(jnp.where(here, rank, 0.0), axis=0, keepdims=True)
        code = jnp.where(rank < SLOTS, rank + shift, -1.0)
        slots = jnp.where(rows_of((128, 256)).astype(f32) == code, 1.0, 0.0).astype(bf16)
        left = jnp.concatenate([jnp.where(here, v[:, at], 0.0).astype(bf16) for v in values], axis=0)
        piece = lax.dot_general(left, slots, (((1,), (1,)), ((), ())), preferred_element_type=f32)
        packed = piece if packed is None else packed + piece
    packed = [packed[PLANE * k : PLANE * (k + 1)] for k in range(len(values))]
    return packed, jnp.max(carry, axis=0, keepdims=True)


def bucket_lines(msg_in):
    near = rows_of((BS, 128)).astype(f32)
    rows = [msg_in[k, :, 256:384] + msg_in[k + 1, :, 256:384] for k in range(0, PLANE, 2)]
    here = jnp.concatenate(rows, axis=0)
    up, up2 = pltpu.roll(here, LANE_STEP, 1), pltpu.roll(here, 2 * LANE_STEP, 1)
    down, down2 = pltpu.roll(here, 128 - LANE_STEP, 1), pltpu.roll(here, 128 - 2 * LANE_STEP, 1)
    lane = lanes_of((1, 128))

    def joined(parts, first):
        row = jnp.zeros((1, 128), f32)
        for k in (2, 1, 0):
            if first + k < len(rows):
                row = jnp.where(lane < LANE_STEP * (k + 1), parts[k][first + k : first + k + 1], row)
            else:
                row = jnp.where(lane < LANE_STEP * (k + 1), 0.0, row)
        return row

    sides = []
    for first in range(0, len(rows), 3):
        p, q, d = joined((here, up, up2), first), joined((down, here, up), first), joined((down2, down, here), first)
        mark = near == p
        left = [jnp.where(mark, piece, 0.0).astype(bf16) for piece in split3(d)]
        sides.append((left, one_hot_rows(q, BS)))
    total = None
    for g in range(0, len(sides), 2):
        right = jnp.concatenate([side[1] for side in sides[g : g + 2]], axis=0)
        for k in range(3):
            add = multiply(jnp.concatenate([side[0][k] for side in sides[g : g + 2]], axis=1), right)
            total = add if total is None else total + add
    return total + total.T


def step_kernel(
    total_lines, given,
    primal_all, slacks_all, cost_all, ends_all, bus_dual_all, demand_all, normal,
    step_primal, step_slack, step_dual, lengths, fullest,
    primal, slacks, cost, ends, bus_dual, demand, selector, line_selector, partner, msg, msg_in, diff0, diff0_in, part0, part0_in, block_in, work, dual_res, split,
    solved, solved_in, diff, diff_in, part, part_in, solved2, solved2_in, diff2, diff2_in, final, final_in, last, last_in,
    in_sem, fixed_sem, pair_sem, msg_sem, diff0_sem, part0_sem,
    solved_sem, diff_sem, part_sem, solved2_sem, diff2_sem, last_sem, final_sem, out_sem,
):
    li, z, c = position()
    half = primal.shape[1]
    mine = pl.ds(pl.multiple_of(c * half, half), half)
    own_buses = pl.ds(pl.multiple_of(li * BS, BS), BS)
    copies = [
        pltpu.make_async_copy(src, dst, in_sem.at[k])
        for k, (src, dst) in enumerate(
            (
                (ends_all.at[:, mine], ends),
                (primal_all.at[:, mine], primal),
                (slacks_all.at[:, mine], slacks),
                (bus_dual_all, bus_dual),
                (cost_all.at[:, mine], cost),
                (demand_all.at[:, own_buses], demand),
            )
        )
    ]
    for copy in copies:
        copy.start()
    own = pltpu.make_async_copy(normal if given else normal.at[li], block_in, fixed_sem)
    own.start()
    greet(li, z, c)
    at_home = c * 16 + li
    source = 2 * li + c
    lane1 = lax.broadcasted_iota(jnp.int32, (1, 128), 1)
    copies[0].wait()
    start, end, place, block = endpoint_rows(ends, z)
    build_line_selector(line_selector, place)
    copies[1].wait()
    copies[2].wait()
    x, s = primal[...], slacks[...]
    scaling = x / s
    inverse = 1.0 / s
    gap = jnp.sum(x * s, axis=1, keepdims=True)
    owner = jnp.where((start >> 8) == (end >> 8), block[:, :half], -1)
    shift = (SLOTS * lax.rem(source, 2)).astype(f32)
    packed, most = buckets(
        owner, [place[:, :half].astype(f32), place[:, half:].astype(f32), *split3(scaling)], shift
    )
    (ends_sum,) = to_buses([jnp.concatenate([scaling, scaling], axis=1)], block, line_selector)
    row = packed[0] + pltpu.roll(packed[1], LANE_STEP, 1)
    row = row + pltpu.roll(packed[2] + packed[3] + packed[4], 2 * LANE_STEP, 1)
    row = jnp.where(lane1 == 127, gap, row)
    whole = jnp.concatenate([ends_sum, row], axis=1)
    for b in range(PLANE):
        msg[b] = whole[b : b + 1]
    for copy in copies[3:]:
        copy.wait()

    greeted()
    pair = pltpu.make_async_remote_copy(
        bus_dual, partner, pair_sem.at[0], pair_sem.at[1], device_id=(li, 2 * z + 1 - c), device_id_type=MESH
    )
    pair.start()
    send_plane(lambda b: msg.at[b], msg.at[at_home], source, msg_in, msg_sem, li, z, c)

    build_selector(selector, place)
    pair.wait()
    mine_dual = jnp.concatenate([bus_dual[:, BS * k : BS * (k + 1)] for k in range(16)], axis=0)
    other_dual = jnp.concatenate([partner[:, BS * k : BS * (k + 1)] for k in range(16)], axis=0)
    table = jnp.concatenate(
        [jnp.where(c == 0, mine_dual, other_dual), jnp.where(c == 0, other_dual, mine_dual)], axis=0
    )
    diff0[:, :half] = to_lines(table, block, selector)
    diff0[:, half:] = jnp.broadcast_to(most, (1, 128))
    send_depth(diff0, diff0_in, diff0_sem, li, z, c)

    (sums,) = to_buses([jnp.concatenate([inverse, -inverse], axis=1)], block, line_selector)
    for b in range(PLANE):
        part0[b, :, 256:512] = sums[b : b + 1]
    wait_bytes(msg_in, msg_sem.at[1])
    sums = sum_slots(msg_in, slice(0, 256))
    gap0 = sum_slots(msg_in, slice(256, 384))[:, 127:128]
    own.wait()
    if given:
        work[...] = block_in[...]
    else:
        diagonal = rows_of((BS, BS)) == lax.broadcasted_iota(jnp.int32, (BS, BS), 1)
        work[...] = block_in[...] + jnp.where(diagonal, sums, 0.0) - bucket_lines(msg_in)

    def first_right_side(panel):
        if panel == 1:
            send_plane(
                lambda b: part0.at[b], part0.at[at_home], source, part0_in, part0_sem, li, z, c
            )
        if panel != 0:
            return
        residual = cost[...] - sum_slots(diff0_in, slice(0, half)) - s
        dual_res[...] = residual
        most = diff0_in[0, :, half:]
        for k in range(1, DEPTH):
            most = jnp.maximum(most, diff0_in[k, :, half:])
        flow = scaling * residual
        (sums,) = to_buses([jnp.concatenate([flow, -flow], axis=1)], block, line_selector)
        for b in range(PLANE):
            part0[b, :, 0:256] = sums[b : b + 1]
            part0[b, :, 512:640] = most

    wait_bytes(diff0_in, diff0_sem.at[1])
    invert(work, first_right_side)
    wait_bytes(part0_in, part0_sem.at[1])
    right = demand[...] + sum_slots(part0_in, slice(0, 256))

    def solve(vector):
        wide = jnp.broadcast_to(vector, (8, BS))
        return jnp.dot(wide, work[...], precision=lax.Precision.HIGHEST, preferred_element_type=f32)[0:1]

    solved[...] = solve(right)
    send_plane(lambda b: solved, solved, at_home, solved_in, solved_sem, li, z, c)
    for k, piece in enumerate(split3(work[...])):
        split[k] = piece.astype(bf16)
    third = sum_slots(part0_in, slice(256, 512))
    wait_bytes(solved_in, solved_sem.at[1])
    table = jnp.concatenate([solved_in[b] for b in range(PLANE)], axis=0)
    diff[...] = to_lines(table, block, selector)
    send_depth(diff, diff_in, diff_sem, li, z, c)
    wait_bytes(diff_in, diff_sem.at[1])
    affine_slack = dual_res[...] - sum_slots(diff_in, slice(0, half))
    affine_primal = -x - scaling * affine_slack
    cross = affine_primal * affine_slack
    extra = cross / s
    (sums,) = to_buses([jnp.concatenate([extra, -extra], axis=1)], block, line_selector)
    scalars = [
        longest_step(x, affine_primal),
        longest_step(s, affine_slack),
        jnp.sum(affine_primal * s, axis=1, keepdims=True),
        jnp.sum(x * affine_slack, axis=1, keepdims=True),
        jnp.sum(cross, axis=1, keepdims=True),
    ]
    row = jnp.zeros((1, 128), f32)
    for k, value in enumerate(scalars):
        row = jnp.where(lane1 == k, value, row)
    whole = jnp.concatenate([sums, jnp.broadcast_to(row, (PLANE, 128))], axis=1)
    for b in range(PLANE):
        part[b] = whole[b : b + 1]
    send_plane(lambda b: part.at[b], part.at[at_home], source, part_in, part_sem, li, z, c)
    wait_bytes(part_in, part_sem.at[1])

    added = sum_slots(part_in, slice(0, 384))
    least = over_slots(jnp.minimum, part_in, slice(256, 384))
    take_p, take_d = least[:, 0:1], least[:, 1:2]
    tail = added[:, 256:384]
    gap_affine = gap0 + take_p * tail[:, 2:3] + take_d * tail[:, 3:4] + take_p * take_d * tail[:, 4:5]
    ratio = gap_affine / gap0
    aim = ratio * ratio * ratio * (gap0 / total_lines)
    right = right - aim * third + added[:, :256]
    high, middle, low = split3(jnp.broadcast_to(right, (8, BS)))
    three = jnp.concatenate([high, middle, low], axis=0).astype(bf16)
    by_high, by_middle, by_low = multiply(three, split[0]), multiply(three[0:16], split[1]), multiply(three[0:8], split[2])
    solved2[...] = (
        by_high[0:1] + (by_high[8:9] + by_middle[0:1]) + (by_high[16:17] + by_middle[8:9] + by_low[0:1])
    )
    send_plane(lambda b: solved2, solved2, at_home, solved2_in, solved2_sem, li, z, c)
    wait_bytes(solved2_in, solved2_sem.at[1])
    table = jnp.concatenate([solved2_in[b] for b in range(PLANE)], axis=0)
    diff2[...] = to_lines(table, block, selector)
    send_depth(diff2, diff2_in, diff2_sem, li, z, c)
    for b in range(16):
        pltpu.make_async_copy(solved2_in.at[16 * c + b], step_dual.at[:, pl.ds(BS * b, BS)], out_sem.at[2]).start()
    wait_bytes(diff2_in, diff2_sem.at[1])
    slack = dual_res[...] - sum_slots(diff2_in, slice(0, half))
    primal_step = (aim - x * s - cross) / s - scaling * slack
    last[...] = jnp.where(lane1 == 0, longest_step(x, primal_step), longest_step(s, slack))
    final[0] = primal_step
    final[1] = slack
    send_plane(lambda b: last, last, source, last_in, last_sem, li, z, c)
    pair2 = pltpu.make_async_remote_copy(
        final, final_in, final_sem.at[0], final_sem.at[1], device_id=(li, 2 * z + 1 - c), device_id_type=MESH
    )
    pair2.start()
    for k, out in enumerate((step_primal, step_slack)):
        pltpu.make_async_copy(final.at[k], out.at[:, mine], out_sem.at[k]).start()
    most = part0_in[0, :, 512:]
    for k in range(1, PLANE):
        most = jnp.maximum(most, part0_in[k, :, 512:])
    fullest[...] = most[:, 0:1]
    pair2.wait()
    other = pl.ds(pl.multiple_of((1 - c) * half, half), half)
    for k, out in enumerate((step_primal, step_slack)):
        pltpu.make_async_copy(final_in.at[k], out.at[:, other], out_sem.at[k]).start()
    for recv, sems in (
        (msg_in, msg_sem), (diff0_in, diff0_sem), (part0_in, part0_sem), (solved_in, solved_sem), (diff_in, diff_sem),
        (part_in, part_sem), (solved2_in, solved2_sem), (diff2_in, diff2_sem), (last_in, last_sem),
    ):
        wait_bytes(recv.at[pl.ds(0, recv.shape[0] - 1)], sems.at[0])
    for k, out in enumerate((step_primal, step_slack, step_dual)):
        wait_bytes(out, out_sem.at[k])
    wait_bytes(last_in, last_sem.at[1])
    least = over_slots(jnp.minimum, last_in, slice(0, 128))
    lengths[...] = damping * least


def vmem(n):
    return [pl.BlockSpec(memory_space=pltpu.VMEM)] * n


def struct(*shape):
    return jax.ShapeDtypeStruct(shape, f32)


def scattered_block(primal, slacks, endpoints, fixed_part):
    blocks_here, block_size = fixed_part.shape[0], fixed_part.shape[1]
    buses_here = blocks_here * block_size
    scaling = primal / slacks
    local = endpoints - lax.axis_index("bus") * buses_here
    own_from, own_to = jnp.where((local >= 0) & (local < buses_here), local, buses_here)
    same_block = endpoints[0] // block_size == endpoints[1] // block_size
    crossing = jnp.where(same_block, -scaling, jnp.zeros_like(scaling))
    rows = jnp.concatenate([own_from, own_to, own_from, own_to])
    columns = jnp.concatenate([own_from, own_to, own_to, own_from]) % block_size
    values = jnp.concatenate([scaling, scaling, crossing, crossing])
    flat = jnp.zeros((buses_here * block_size,), f32).at[rows * block_size + columns].add(values, mode="drop")
    tiles = lax.all_to_all(flat.reshape(blocks_here, block_size, block_size), "line", 0, 0, tiled=True)
    mine = lax.dynamic_index_in_dim(fixed_part, lax.axis_index("line"), 0, keepdims=False)
    return mine + jnp.sum(tiles, axis=0)


def hand_over(step_primal, step_slack, step_dual, lengths, primal_out, slack_out, dual_out, lengths_out):
    primal_out[...] = step_primal[...]
    slack_out[...] = step_slack[...]
    dual_out[...] = step_dual[...]
    lengths_out[...] = lengths[:, 0:2]


def whole_step(given, args, normal):
    x, s, cost, ends, bus_dual, demand = args
    lines_here, buses_here = x.shape[1], bus_dual.shape[1]
    half = lines_here // 2
    total_lines = float(lines_here * lax.axis_size("line"))
    dma = pltpu.SemaphoreType.DMA
    exchange = lambda slots, width: [pltpu.VMEM((1, width), f32), pltpu.VMEM((slots, 1, width), f32)]
    buckets_of = lambda width: [pltpu.VMEM((PLANE, 1, width), f32)] * 2
    return pl.pallas_call(
        functools.partial(step_kernel, total_lines, given),
        out_shape=tuple(pltpu.VMEM((1, n), f32) for n in (lines_here, lines_here, buses_here, 128, 1)),
        in_specs=[pl.BlockSpec(memory_space=pl.ANY)] * 7,
        out_specs=tuple(vmem(5)),
        scratch_shapes=[pltpu.VMEM((1, half), f32)] * 3
        + [pltpu.VMEM((2, half), jnp.int32), pltpu.VMEM((1, buses_here), f32), pltpu.VMEM((1, BS), f32)]
        + [pltpu.VMEM((BS, lines_here), bf16), pltpu.VMEM((lines_here, BS), bf16), pltpu.VMEM((1, buses_here), f32)]
        + buckets_of(384)
        + exchange(DEPTH, half + 128)
        + buckets_of(640)
        + [pltpu.VMEM((BS, BS), f32)] * 2
        + [pltpu.VMEM((1, half), f32), pltpu.VMEM((3, BS, BS), bf16)]
        + exchange(PLANE, BS)
        + exchange(DEPTH, half)
        + buckets_of(384)
        + exchange(PLANE, BS)
        + exchange(DEPTH, half)
        + [pltpu.VMEM((2, 1, half), f32)] * 2
        + exchange(PLANE, 128)
        + [dma((6,)), dma]
        + [dma((2,))] * 11
        + [dma((3,))],
        compiler_params=pltpu.CompilerParams(collective_id=int(given), has_side_effects=True),
        name="step_given" if given else "step",
    )(*args, normal)


def per_device(primal, slacks, line_cost, bus_dual, demand, endpoints, fixed_part):
    args = tuple(a.reshape(1, -1) for a in (primal, slacks, line_cost))
    args += (endpoints, bus_dual.reshape(1, -1), demand.reshape(1, -1))
    def again(steps):
        normal = scattered_block(primal, slacks, endpoints, fixed_part)
        *steps, fullest = whole_step(True, args, normal)
        return (*steps, jnp.zeros_like(fullest))

    *steps, _ = lax.while_loop(lambda steps: steps[-1][0, 0] > SLOTS, again, tuple(whole_step(False, args, fixed_part)))
    outputs = pl.pallas_call(
        hand_over,
        out_shape=tuple(struct(*a.shape) for a in steps[:3]) + (struct(1, 2),),
        in_specs=vmem(4),
        out_specs=tuple(vmem(4)),
        name="hand_over",
    )(*steps)
    return tuple(a.reshape(-1) for a in outputs)


def solution(mesh):
    in_specs = (P("line"), P("line"), P("line"), P("bus"), P("bus"), P(None, "line"), P("bus", None, None))
    out_specs = (P("line"), P("line"), P("bus"), P())
    return jax.shard_map(per_device, mesh=mesh, in_specs=in_specs, out_specs=out_specs, check_vma=False)
```
